64 devices in a mesh: dp: 4 (over x, y), tp: 16 (over z, core).
Axes of the slice: x: 2, y: 2, z: 8, core: 2. Of those that a mesh axis runs over, the one named last changes fastest.
The devices are a block of a 4x4x8 slice.
Arguments:
- x_in: bfloat16 [32, 256, 1408], P('dp', 'tp'), parts along dimension 0
- y_text: bfloat16 [32, 256, 1408], P('dp', 'tp'), parts along dimension 0
- t_emb: bfloat16 [32, 8448], P('dp'), parts along dimension 0
- text_len: int32 [32], P('dp'), parts along dimension 0
- mod_table: bfloat16 [6, 1408], replicated
- w_qkv: bfloat16 [1408, 16, 264], P(None, 'tp')
- b_qkv: bfloat16 [16, 264], P('tp')
- w_o: bfloat16 [16, 88, 1408], P('tp')
- b_o: bfloat16 [1408], replicated
- w_q: bfloat16 [1408, 16, 88], P(None, 'tp')
- b_q: bfloat16 [16, 88], P('tp')
- w_kv: bfloat16 [1408, 16, 176], P(None, 'tp')
- b_kv: bfloat16 [16, 176], P('tp')
- w_co: bfloat16 [16, 88, 1408], P('tp')
- b_co: bfloat16 [1408], replicated
- w_1: bfloat16 [1408, 6144], P(None, 'tp')
- b_1: bfloat16 [6144], P('tp')
- w_2: bfloat16 [6144, 1408], P('tp')
- b_2: bfloat16 [1408], replicated
- g_out: bfloat16 [32, 256, 1408], P('dp', 'tp'), parts along dimension 0
Outputs:
- output 1: bfloat16 [32, 256, 1408], P('dp', 'tp'), parts along dimension 0
- output 2: bfloat16 [32, 256, 1408], P('dp', 'tp'), parts along dimension 0
- output 3: bfloat16 [32, 256, 1408], P('dp', 'tp'), parts along dimension 0
- output 4: float32 [24, 1408], P('dp'), parts along dimension 0
- output 5: bfloat16 [5632, 16, 264], P('dp', 'tp'), parts along dimension 0
- output 6: bfloat16 [64, 264], P(('dp', 'tp')), parts along dimension 0
- output 7: bfloat16 [64, 88, 1408], P(('dp', 'tp')), parts along dimension 0
- output 8: bfloat16 [5632], P('dp'), parts along dimension 0
- output 9: bfloat16 [5632, 16, 88], P('dp', 'tp'), parts along dimension 0
- output 10: bfloat16 [64, 88], P(('dp', 'tp')), parts along dimension 0
- output 11: bfloat16 [5632, 16, 176], P('dp', 'tp'), parts along dimension 0
- output 12: bfloat16 [64, 176], P(('dp', 'tp')), parts along dimension 0
- output 13: bfloat16 [64, 88, 1408], P(('dp', 'tp')), parts along dimension 0
- output 14: bfloat16 [5632], P('dp'), parts along dimension 0
- output 15: bfloat16 [5632, 6144], P('dp', 'tp'), parts along dimension 0
- output 16: bfloat16 [24576], P(('dp', 'tp')), parts along dimension 0
- output 17: bfloat16 [24576, 1408], P(('dp', 'tp')), parts along dimension 0
- output 18: bfloat16 [5632], P('dp'), parts along dimension 0
There are 4 independent parts. The reference program is written for one: setup_inputs(seed, part) draws one part's arguments, and reference() takes and returns one part's arrays. A program takes and returns all parts, laid end to end along the dimension named above; an argument that names none is the same for every part.
All inputs are finite; a program needn't handle non-finite values.
Results may differ from the reference program's by a relative error of at most 0.02.
Values are sent between devices in bfloat16 or wider.
A program may use at most 768 MiB of HBM per device.

```python
import jax
import jax.numpy as jnp
from jax import lax

BATCH_SIZE = 8
IMG_TOKENS = 256
TEXT_SLOTS = 256
TEXT_LEN = 256
WIDTH = 1408
NUM_HEADS = 16
HEAD_DIM = 88
FFN_DIM = 6144
LN_EPS = 1e-6


def setup_inputs(seed: int = 0, part: int = 0) -> dict:
    part_keys = jax.random.split(jax.random.fold_in(jax.random.key(seed), part), 5)
    weight_keys = jax.random.split(jax.random.key(seed + 1), 15)
    width_scale = WIDTH ** -0.5

    def draw_normal(rng_key, shape, scale):
        return (scale * jax.random.normal(rng_key, shape, jnp.float32)).astype(jnp.bfloat16)

    lengths = jax.random.randint(part_keys[3], (BATCH_SIZE,), 1, TEXT_LEN + 1)
    lengths = jnp.where(jnp.arange(BATCH_SIZE) == 0, TEXT_LEN, lengths).astype(jnp.int32)
    return {
        'x_in': draw_normal(part_keys[0], (BATCH_SIZE, IMG_TOKENS, WIDTH), 1.0),
        'y_text': draw_normal(part_keys[1], (BATCH_SIZE, TEXT_SLOTS, WIDTH), 1.0),
        't_emb': draw_normal(part_keys[2], (BATCH_SIZE, 6 * WIDTH), 0.3),
        'text_len': lengths,
        'mod_table': draw_normal(weight_keys[0], (6, WIDTH), 0.3),
        'w_qkv': draw_normal(weight_keys[1], (WIDTH, NUM_HEADS, 3 * HEAD_DIM), width_scale),
        'b_qkv': draw_normal(weight_keys[2], (NUM_HEADS, 3 * HEAD_DIM), 0.2),
        'w_o': draw_normal(weight_keys[3], (NUM_HEADS, HEAD_DIM, WIDTH), width_scale),
        'b_o': draw_normal(weight_keys[4], (WIDTH,), 0.2),
        'w_q': draw_normal(weight_keys[5], (WIDTH, NUM_HEADS, HEAD_DIM), width_scale),
        'b_q': draw_normal(weight_keys[6], (NUM_HEADS, HEAD_DIM), 0.2),
        'w_kv': draw_normal(weight_keys[7], (WIDTH, NUM_HEADS, 2 * HEAD_DIM), width_scale),
        'b_kv': draw_normal(weight_keys[8], (NUM_HEADS, 2 * HEAD_DIM), 0.2),
        'w_co': draw_normal(weight_keys[9], (NUM_HEADS, HEAD_DIM, WIDTH), 2.0 * width_scale),
        'b_co': draw_normal(weight_keys[10], (WIDTH,), 0.2),
        'w_1': draw_normal(weight_keys[11], (WIDTH, FFN_DIM), width_scale),
        'b_1': draw_normal(weight_keys[12], (FFN_DIM,), 0.2),
        'w_2': draw_normal(weight_keys[13], (FFN_DIM, WIDTH), FFN_DIM ** -0.5),
        'b_2': draw_normal(weight_keys[14], (WIDTH,), 0.2),
        'g_out': draw_normal(part_keys[4], (BATCH_SIZE, IMG_TOKENS, WIDTH), 1.0),
    }


def as_bf16(tensor):
    return tensor.astype(jnp.bfloat16).astype(jnp.float32)


def layer_norm(tensor):
    centered = tensor - jnp.mean(tensor, axis=-1, keepdims=True)
    variance = jnp.mean(centered * centered, axis=-1, keepdims=True)
    return centered * lax.rsqrt(variance + LN_EPS)


def split_heads(tensor):
    batch, length = tensor.shape[0], tensor.shape[1]
    return tensor.transpose(0, 2, 1, 3).reshape(batch * NUM_HEADS, length, HEAD_DIM)


def merge_heads(tensor, batch):
    length = tensor.shape[1]
    return tensor.reshape(batch, NUM_HEADS, length, HEAD_DIM).transpose(0, 2, 1, 3)


def attention(q_heads, k_heads, v_heads, key_ok):
    def one_head(operands):
        q_blk, k_blk, v_blk, ok_row = operands
        scores = jnp.dot(q_blk, k_blk.T, preferred_element_type=jnp.float32) * HEAD_DIM ** -0.5
        scores = jnp.where(ok_row[None, :], scores, -1e30)
        weights = jax.nn.softmax(scores, axis=-1)
        return jnp.dot(weights, v_blk, preferred_element_type=jnp.float32)
    return lax.map(jax.checkpoint(one_head), (q_heads, k_heads, v_heads, key_ok))


def block_forward(x_val, y_val, params, t_val, text_len):
    (mod_table, w_qkv, b_qkv, w_o, b_o, w_q, b_q, w_kv, b_kv, w_co, b_co, w_1, b_1, w_2, b_2) = params
    batch = x_val.shape[0]
    mod_rows = mod_table[None] + t_val.reshape(batch, 6, WIDTH)
    shift1 = mod_rows[:, 0, None, :]
    scale1 = mod_rows[:, 1, None, :]
    gate1 = mod_rows[:, 2, None, :]
    shift2 = mod_rows[:, 3, None, :]
    scale2 = mod_rows[:, 4, None, :]
    gate2 = mod_rows[:, 5, None, :]
    h_one = as_bf16(layer_norm(x_val) * (1.0 + scale1) + shift1)
    qkv_all = as_bf16(jnp.einsum('bnd,dhe->bnhe', h_one, w_qkv) + b_qkv)
    self_ok = jnp.ones((batch * NUM_HEADS, IMG_TOKENS), dtype=jnp.bool_)
    attn_val = attention(split_heads(qkv_all[..., :HEAD_DIM]), split_heads(qkv_all[..., HEAD_DIM:2 * HEAD_DIM]), split_heads(qkv_all[..., 2 * HEAD_DIM:]), self_ok)
    attn_val = as_bf16(merge_heads(attn_val, batch))
    x_one = as_bf16(x_val + gate1 * (jnp.einsum('bnhe,hed->bnd', attn_val, w_o) + b_o))
    q_cross = as_bf16(jnp.einsum('bnd,dhe->bnhe', x_one, w_q) + b_q)
    kv_cross = as_bf16(jnp.einsum('bsd,dhe->bshe', y_val, w_kv) + b_kv)
    slot_ok = jnp.arange(TEXT_SLOTS)[None, :] < text_len[:, None]
    cross_ok = jnp.broadcast_to(slot_ok[:, None, :], (batch, NUM_HEADS, TEXT_SLOTS)).reshape(batch * NUM_HEADS, TEXT_SLOTS)
    cross_val = attention(split_heads(q_cross), split_heads(kv_cross[..., :HEAD_DIM]), split_heads(kv_cross[..., HEAD_DIM:]), cross_ok)
    cross_val = as_bf16(merge_heads(cross_val, batch))
    x_two = as_bf16(x_one + jnp.einsum('bnhe,hed->bnd', cross_val, w_co) + b_co)
    h_two = as_bf16(layer_norm(x_two) * (1.0 + scale2) + shift2)
    hidden = jnp.einsum('bnd,df->bnf', h_two, w_1) + b_1
    gelu_out = as_bf16(jax.nn.gelu(hidden, approximate=True))
    return x_two + gate2 * (jnp.einsum('bnf,fd->bnd', gelu_out, w_2) + b_2)


def reference(x_in, y_text, t_emb, text_len, mod_table, w_qkv, b_qkv, w_o, b_o, w_q, b_q, w_kv, b_kv, w_co, b_co, w_1, b_1, w_2, b_2, g_out):
    params = tuple(weight.astype(jnp.float32) for weight in (mod_table, w_qkv, b_qkv, w_o, b_o, w_q, b_q, w_kv, b_kv, w_co, b_co, w_1, b_1, w_2, b_2))
    t_val = t_emb.astype(jnp.float32)

    def forward(x_val, y_val, param_set):
        return block_forward(x_val, y_val, param_set, t_val, text_len)

    x_out, back = jax.vjp(forward, x_in.astype(jnp.float32), y_text.astype(jnp.float32), params)
    g_x, g_y, g_par = back(g_out.astype(jnp.float32))
    return (x_out.astype(jnp.bfloat16), g_x.astype(jnp.bfloat16), g_y.astype(jnp.bfloat16), g_par[0], g_par[1].astype(jnp.bfloat16), g_par[2].astype(jnp.bfloat16), g_par[3].astype(jnp.bfloat16), g_par[4].astype(jnp.bfloat16), g_par[5].astype(jnp.bfloat16), g_par[6].astype(jnp.bfloat16), g_par[7].astype(jnp.bfloat16), g_par[8].astype(jnp.bfloat16), g_par[9].astype(jnp.bfloat16), g_par[10].astype(jnp.bfloat16), g_par[11].astype(jnp.bfloat16), g_par[12].astype(jnp.bfloat16), g_par[13].astype(jnp.bfloat16), g_par[14].astype(jnp.bfloat16))
```

```python
import functools

import jax
import jax.numpy as jnp
from jax import lax
from jax.experimental import pallas as pl
from jax.experimental.pallas import tpu as pltpu
from jax.sharding import PartitionSpec as P

LN_EPS = 1e-6
MASK_FILL = -1e30
LANES = 128
MESH = pl.DeviceIdType.MESH
BF16 = jnp.bfloat16
F32 = jnp.float32
VMEM_LIMIT = 66 * 1000 * 1000
NN = (((1,), (0,)), ((), ()))
NT = (((1,), (1,)), ((), ()))
TN = (((0,), (0,)), ((), ()))
UP, DOWN = 0, 1


def dot(lhs, rhs, dims=NN):
    return lax.dot_general(lhs, rhs, dims, preferred_element_type=F32)


def place(tp_size):
    me = lax.axis_index('tp')
    return tp_size // 2, me // 2, lax.rem(me, 2)


def greet(ring, chip, core):
    barrier = pltpu.get_barrier_semaphore()
    for zz, cc in ((lax.rem(chip + 1, ring), core), (lax.rem(chip + ring - 1, ring), core), (chip, 1 - core)):
        pl.semaphore_signal(barrier, inc=1, device_id={'tp': zz * 2 + cc}, device_id_type=MESH)
    pl.semaphore_wait(barrier, 3)


def gather_body(tp_size, n_src, n_in, saves, n_acc, compute, *refs):
    ring, chip, core = place(tp_size)
    half = ring // 2
    srcs, refs = refs[:n_src], refs[n_src:]
    ins, refs = refs[:n_in], refs[n_in:]
    n_save = len(saves)
    full, rsend, rrecv, ssend, srecv, save_sem = refs[-6:]
    outs = refs[:-6]
    saved, outs = outs[:n_save], outs[n_save:]
    batch, n_loc = srcs[0].shape[0], srcs[0].shape[1]
    hb = batch * n_src // 2

    for acc in outs[len(outs) - n_acc:]:
        acc[...] = jnp.zeros_like(acc)

    def wrap(zz):
        return lax.rem(zz + ring, ring)

    def part(zz, cc, ch):
        row = pl.multiple_of((zz * 2 + cc) * n_loc, n_loc)
        return full.at[pl.ds(ch * hb, hb), pl.ds(row, n_loc), :]

    def own(ch):
        return srcs[ch] if n_src == 2 else srcs[0].at[pl.ds(ch * hb, hb)]

    def ring_copy(way, k, ch, sending):
        sign = -1 if way == UP else 1
        zb = wrap(chip + sign * (k - 1 if sending else k))
        src = own(ch) if (sending and k == 1) else part(zb, core, ch)
        return pltpu.make_async_remote_copy(
            src_ref=src, dst_ref=part(zb, core, ch),
            send_sem=rsend.at[way, k - 1, ch], recv_sem=rrecv.at[way, k - 1, ch],
            device_id={'tp': wrap(chip - sign) * 2 + core}, device_id_type=MESH)

    def chip_at(slot):
        k = (slot + 1) // 2
        return wrap(chip - k) if slot % 2 else wrap(chip + k)

    def sib_copy(slot, ch, sending):
        zb = chip_at(slot)
        cc = core if sending else 1 - core
        src = own(ch) if (sending and slot == 0) else part(zb, cc, ch)
        return pltpu.make_async_remote_copy(
            src_ref=src, dst_ref=part(zb, cc, ch),
            send_sem=ssend.at[slot, ch], recv_sem=srecv.at[slot, ch],
            device_id={'tp': chip * 2 + 1 - core}, device_id_type=MESH)

    def carries(way, k, ch):
        return k < half or (k == half and ch == way)

    def slot_of(way, k):
        return 2 * half - 1 if k == half else (2 * k - 1 if way == UP else 2 * k)

    greet(ring, chip, core)
    ring_copy(UP, 1, 0, True).start()
    ring_copy(DOWN, 1, 1, True).start()
    ring_copy(UP, 1, 1, True).start()
    ring_copy(DOWN, 1, 0, True).start()
    sib_copy(0, 0, True).start()
    sib_copy(0, 1, True).start()
    for ch in (0, 1):
        row = pl.multiple_of((chip * 2 + core) * n_loc, n_loc)
        full[pl.ds(ch * hb, hb), pl.ds(row, n_loc), :] = own(ch)[...]

    def arrive(way, k, ch):
        ring_copy(way, k, ch, False).wait_recv()
        if carries(way, k + 1, ch):
            ring_copy(way, k + 1, ch, True).start()
        sib_copy(slot_of(way, k), ch, True).start()

    def group(g):
        k = g // 2 + 1
        if g % 2 == 0:
            arrive(UP, k, 0)
            arrive(DOWN, k, 1)
        else:
            arrive(UP, k, 1)
            arrive(DOWN, k, 0)

    def save_copy(stream, slot, zz):
        rows = pl.ds(pl.multiple_of(zz * 2 * n_loc, 2 * n_loc), 2 * n_loc)
        return pltpu.make_async_copy(
            full.at[pl.ds(saves[stream] * batch, batch), rows, :], saved[stream].at[:, rows, :], save_sem.at[stream, slot])

    def step(slot, carry):
        for s in range(ring):
            @pl.when(slot == s)
            def _():
                if s < ring - 2:
                    group(s)
                elif s == ring - 1:
                    group(ring - 2)
                sib_copy(s, 0, False).wait_recv()
                sib_copy(s, 1, False).wait_recv()
        k = (slot + 1) // 2
        sign = 1 - 2 * lax.rem(slot, 2)
        zz = wrap(chip + sign * k)
        rows = pl.ds(pl.multiple_of(zz * 2 * n_loc, 2 * n_loc), 2 * n_loc)
        for stream in range(n_save):
            save_copy(stream, slot, zz).start()
        compute(rows, lambda i: full[pl.ds(i * batch, batch), rows, :].reshape(batch * 2 * n_loc, full.shape[2]), ins, outs)
        return carry

    lax.fori_loop(0, ring, step, None)

    for way in (UP, DOWN):
        for k in range(1, half + 1):
            for ch in (0, 1):
                if carries(way, k, ch):
                    ring_copy(way, k, ch, True).wait_send()
    for slot in range(ring):
        for ch in (0, 1):
            sib_copy(slot, ch, True).wait_send()
        for stream in range(n_save):
            save_copy(stream, slot, chip_at(slot)).wait()


def gather_call(tp_size, cid, name, blocks, ins, saves, outs, accs, compute):
    batch, n_loc, width = blocks[0].shape
    n_tok = n_loc * tp_size
    ring, half = tp_size // 2, tp_size // 4
    vmem = pl.BlockSpec(memory_space=pltpu.VMEM)
    return pl.pallas_call(
        functools.partial(gather_body, tp_size, len(blocks), len(ins), saves, len(accs), compute),
        out_shape=[jax.ShapeDtypeStruct((batch, n_tok, width), BF16)] * len(saves)
        + [jax.ShapeDtypeStruct(s, BF16) for s in outs] + [jax.ShapeDtypeStruct(s, F32) for s in accs],
        in_specs=[vmem] * (len(blocks) + len(ins)),
        out_specs=[pl.BlockSpec(memory_space=pl.ANY)] * len(saves) + [vmem] * (len(outs) + len(accs)),
        scratch_shapes=[
            pltpu.VMEM((batch * len(blocks), n_tok, width), BF16),
            pltpu.SemaphoreType.DMA((2, half, 2)),
            pltpu.SemaphoreType.DMA((2, half, 2)),
            pltpu.SemaphoreType.DMA((ring, 2)),
            pltpu.SemaphoreType.DMA((ring, 2)),
            pltpu.SemaphoreType.DMA((max(1, len(saves)), ring)),
        ],
        compiler_params=pltpu.CompilerParams(collective_id=cid, has_side_effects=True, vmem_limit_bytes=VMEM_LIMIT),
        name=name,
    )(*blocks, *ins)


def scatter_body(tp_size, n_out, n_in, n_load, n_acc, compute, *refs):
    ring, chip, core = place(tp_size)
    half = ring // 2
    ins, refs = refs[:n_in], refs[n_in:]
    loads, refs = refs[:n_load], refs[n_load:]
    result, refs = refs[0], refs[1:]
    accs, refs = refs[:n_acc], refs[n_acc:]
    held, refs = refs[:n_load], refs[n_load:]
    pbuf, sibr, snd, rcv, rsend, rrecv, ssend, srecv, load_sem = refs
    nb, n_loc = result.shape[0], result.shape[1]
    batch, hb = nb // n_out, nb // 2

    def wrap(zz):
        return lax.rem(zz + ring, ring)

    def load_copy(i):
        return pltpu.make_async_copy(loads[i], held[i], load_sem.at[i])

    for i in range(n_load):
        load_copy(i).start()
    for acc in accs:
        acc[...] = jnp.zeros_like(acc)

    def ring_copy(way, s, ch):
        sign = 1 if way == UP else -1
        part = pl.ds(ch * hb, hb)
        return pltpu.make_async_remote_copy(
            src_ref=snd.at[way, s, part], dst_ref=rcv.at[way, s, part],
            send_sem=rsend.at[way, s, ch], recv_sem=rrecv.at[way, s, ch],
            device_id={'tp': wrap(chip + sign) * 2 + core}, device_id_type=MESH)

    def sib_copy(slot):
        rows = pl.ds(pl.multiple_of((1 - core) * n_loc, n_loc), n_loc)
        return pltpu.make_async_remote_copy(
            src_ref=pbuf.at[slot, :, rows, :], dst_ref=sibr.at[slot],
            send_sem=ssend.at[slot], recv_sem=srecv.at[slot],
            device_id={'tp': chip * 2 + 1 - core}, device_id_type=MESH)

    def own_sum(slot, part):
        rows = pl.ds(pl.multiple_of(core * n_loc, n_loc), n_loc)
        return pbuf[slot, part, rows, :].astype(F32) + sibr[slot, part].astype(F32)

    def starts_at(way, ch):
        return 0 if ch == way else 1

    def pass_on(way, s, slot, ch):
        part = pl.ds(ch * hb, hb)
        total = own_sum(slot, part)
        if s > starts_at(way, ch):
            ring_copy(way, s - 1, ch).wait_recv()
            total = total + rcv[way, s - 1, part].astype(F32)
        snd[way, s, part] = total.astype(BF16)
        ring_copy(way, s, ch).start()

    def ring_step(s):
        if s == 0:
            sib_copy(0).wait_recv()
            pass_on(UP, 0, 0, 0)
            pass_on(DOWN, 0, 0, 1)
            return
        sib_copy(2 * s - 1).wait_recv()
        pass_on(UP, s, 2 * s - 1, 1)
        sib_copy(2 * s).wait_recv()
        pass_on(DOWN, s, 2 * s, 0)
        pass_on(UP, s, 2 * s - 1, 0)
        pass_on(DOWN, s, 2 * s, 1)

    greet(ring, chip, core)
    for i in range(n_load):
        load_copy(i).wait()

    def step(slot, carry):
        away = half - (slot + 1) // 2
        sign = 2 * lax.rem(slot, 2) - 1
        zz = wrap(chip + sign * away)
        rows = pl.ds(pl.multiple_of(zz * 2 * n_loc, 2 * n_loc), 2 * n_loc)

        def put(i, value):
            pbuf[slot, pl.ds(i * batch, batch)] = value.astype(BF16).reshape(batch, 2 * n_loc, value.shape[-1])

        compute(rows, put, ins, held, accs)
        sib_copy(slot).start()
        for s in range(half):
            @pl.when(slot == 2 * s + 1)
            def _():
                ring_step(s)
        return carry

    lax.fori_loop(0, ring, step, None)

    sib_copy(ring - 1).wait_recv()
    for ch, order in ((1, (UP, DOWN)), (0, (DOWN, UP))):
        part = pl.ds(ch * hb, hb)
        total = own_sum(ring - 1, part)
        for way in order:
            ring_copy(way, half - 1, ch).wait_recv()
            total = total + rcv[way, half - 1, part].astype(F32)
        result[part] = total
    for way in (UP, DOWN):
        for s in range(half):
            for ch in (0, 1):
                if s >= starts_at(way, ch):
                    ring_copy(way, s, ch).wait_send()
    for slot in range(ring):
        sib_copy(slot).wait_send()


def scatter_call(tp_size, cid, name, n_loc, width, n_out, ins, loads, accs, compute):
    batch = ins[0].shape[0]
    nb = batch * n_out
    ring, half = tp_size // 2, tp_size // 4
    vmem = pl.BlockSpec(memory_space=pltpu.VMEM)
    return pl.pallas_call(
        functools.partial(scatter_body, tp_size, n_out, len(ins), len(loads), len(accs), compute),
        out_shape=[jax.ShapeDtypeStruct((nb, n_loc, width), F32)] + [jax.ShapeDtypeStruct(s, F32) for s in accs],
        in_specs=[vmem] * len(ins) + [pl.BlockSpec(memory_space=pl.ANY)] * len(loads),
        out_specs=[vmem] * (1 + len(accs)),
        scratch_shapes=[pltpu.VMEM(a.shape, a.dtype) for a in loads] + [
            pltpu.VMEM((ring, nb, 2 * n_loc, width), BF16),
            pltpu.VMEM((ring, nb, n_loc, width), BF16),
            pltpu.VMEM((2, half, nb, n_loc, width), BF16),
            pltpu.VMEM((2, half, nb, n_loc, width), BF16),
            pltpu.SemaphoreType.DMA((2, half, 2)),
            pltpu.SemaphoreType.DMA((2, half, 2)),
            pltpu.SemaphoreType.DMA((ring,)),
            pltpu.SemaphoreType.DMA((ring,)),
            pltpu.SemaphoreType.DMA((max(1, len(loads)),)),
        ],
        compiler_params=pltpu.CompilerParams(collective_id=cid, has_side_effects=True, vmem_limit_bytes=VMEM_LIMIT),
        name=name,
    )(*ins, *loads)


def total_body(tp_size, src, out, got, mine, send1, recv1, send2, recv2):
    me = lax.axis_index('tp')
    barrier = pltpu.get_barrier_semaphore()
    for d in range(1, tp_size):
        pl.semaphore_signal(barrier, inc=1, device_id={'tp': lax.rem(me + d, tp_size)}, device_id_type=MESH)
    pl.semaphore_wait(barrier, tp_size - 1)

    def first(d):
        peer = lax.rem(me + d, tp_size)
        return pltpu.make_async_remote_copy(
            src_ref=src.at[peer], dst_ref=got.at[d - 1], send_sem=send1.at[d - 1], recv_sem=recv1.at[d - 1],
            device_id={'tp': peer}, device_id_type=MESH)

    def second(d, sending):
        peer = lax.rem(me + d, tp_size)
        slab = me if sending else lax.rem(me + tp_size - d, tp_size)
        return pltpu.make_async_remote_copy(
            src_ref=mine, dst_ref=out.at[slab], send_sem=send2.at[d - 1], recv_sem=recv2.at[d - 1],
            device_id={'tp': peer}, device_id_type=MESH)

    for d in range(1, tp_size):
        first(d).start()
    total = src[me]
    for d in range(1, tp_size):
        first(d).wait_recv()
        total = total + got[d - 1]
    mine[...] = total
    for d in range(1, tp_size):
        second(d, True).start()
    out[me] = total
    for d in range(1, tp_size):
        second(d, False).wait_recv()
    for d in range(1, tp_size):
        first(d).wait_send()
        second(d, True).wait_send()


def total_call(tp_size, cid, rows):
    width = rows[0].shape[0]
    flat = jnp.concatenate(rows)
    per = -(-flat.shape[0] // (tp_size * 8 * LANES)) * 8
    padded = jnp.pad(flat, (0, tp_size * per * LANES - flat.shape[0])).reshape(tp_size, per, LANES)
    vmem = pl.BlockSpec(memory_space=pltpu.VMEM)
    out = pl.pallas_call(
        functools.partial(total_body, tp_size),
        out_shape=jax.ShapeDtypeStruct(padded.shape, F32),
        in_specs=[vmem],
        out_specs=vmem,
        scratch_shapes=[
            pltpu.VMEM((tp_size - 1, per, LANES), F32),
            pltpu.VMEM((per, LANES), F32),
        ] + [pltpu.SemaphoreType.DMA((tp_size - 1,))] * 4,
        compiler_params=pltpu.CompilerParams(collective_id=cid, has_side_effects=True),
        name='small_total',
    )(padded)
    flat = out.reshape(-1)
    return [flat[i * width:(i + 1) * width] for i in range(len(rows))]


def layer_norm(tensor):
    tensor = tensor.astype(F32)
    centered = tensor - jnp.mean(tensor, axis=-1, keepdims=True)
    inv_std = lax.rsqrt(jnp.mean(centered * centered, axis=-1, keepdims=True) + LN_EPS)
    return centered * inv_std, inv_std


def layer_norm_back(normed, inv_std, g_normed):
    mean_g = jnp.mean(g_normed, axis=-1, keepdims=True)
    mean_gn = jnp.mean(g_normed * normed, axis=-1, keepdims=True)
    return inv_std * (g_normed - mean_g - normed * mean_gn)


def product(form, lhs, rhs):
    return jnp.einsum(form, lhs, rhs, preferred_element_type=F32)


def attend(q_all, k_all, v_all, key_ok, scale):
    scores = product('bqe,bke->bqk', q_all, k_all) * scale
    if key_ok is not None:
        scores = jnp.where(key_ok[:, None, :], scores, MASK_FILL)
    prob_bf = jax.nn.softmax(scores, axis=-1).astype(BF16)
    return product('bqk,bke->bqe', prob_bf, v_all).astype(BF16), prob_bf


def attend_back(q_all, k_all, v_all, prob_bf, g_val, scale):
    g_v = product('bqk,bqe->bke', prob_bf, g_val)
    g_prob = product('bqe,bke->bqk', g_val, v_all)
    row_dot = jnp.sum(g_prob * prob_bf, axis=-1, keepdims=True)
    g_scores = (prob_bf * (g_prob - row_dot) * scale).astype(BF16)
    g_q = product('bqk,bke->bqe', g_scores, k_all)
    g_k = product('bqk,bqe->bke', g_scores, q_all)
    return g_q.astype(BF16), g_k.astype(BF16), g_v.astype(BF16)


def pad_heads(weight, n_part, head_dim, head_pad):
    lead = weight.shape[:-1]
    weight = weight.reshape(*lead, n_part, head_dim)
    weight = jnp.pad(weight, [(0, 0)] * (len(lead) + 1) + [(0, head_pad - head_dim)])
    return weight.reshape(*lead, n_part * head_pad)


def drop_pad(grad, n_part, head_dim, head_pad):
    tail = grad.shape[1:]
    return grad.reshape(n_part, head_pad, *tail)[:, :head_dim].reshape(n_part * head_dim, *tail)


def rows_of(ref, rows):
    block = ref[:, rows, :]
    return block.reshape(block.shape[0] * block.shape[1], block.shape[2])


def put_rows(ref, rows, value):
    ref[:, rows, :] = value.astype(ref.dtype).reshape(ref.shape[0], rows.size, ref.shape[2])


def row_sum(value):
    return jnp.sum(value, axis=0, keepdims=True)


def gelu_pair(hidden):
    c0, c1 = 0.7978845608028654, 0.044715
    square = hidden * hidden
    tanh = jnp.tanh(c0 * hidden * (1.0 + c1 * square))
    half_up = 0.5 * (1.0 + tanh)
    slope = half_up + 0.5 * hidden * (1.0 - tanh * tanh) * (c0 * (1.0 + 3.0 * c1 * square))
    return hidden * half_up, slope


def token_sum(tensor):
    return jnp.sum(tensor.astype(F32), axis=(0, 1))


def device_block(tp_size, x_loc, y_loc, t_loc, len_loc, mod_table, w_qkv, b_qkv, w_o, b_o, w_q, b_q, w_kv, b_kv, w_co, b_co, w_1, b_1, w_2, b_2, g_loc):
    batch, n_loc, width = x_loc.shape
    n_tok = n_loc * tp_size
    head_dim, ffn = w_q.shape[2], w_1.shape[1]
    head_pad = -(-head_dim // LANES) * LANES
    scale = head_dim ** -0.5
    mod_rows = mod_table.astype(F32)[None] + t_loc.astype(F32).reshape(batch, 6, width)
    shift1, scale1, gate1, shift2, scale2, gate2 = [mod_rows[:, i, None, :] for i in range(6)]

    wqkv = pad_heads(w_qkv[:, 0], 3, head_dim, head_pad)
    wkv = pad_heads(w_kv[:, 0], 2, head_dim, head_pad)
    wq = pad_heads(w_q[:, 0], 1, head_dim, head_pad)
    bqkv = pad_heads(b_qkv.astype(F32), 3, head_dim, head_pad)
    bkv = pad_heads(b_kv.astype(F32), 2, head_dim, head_pad)
    bq = pad_heads(b_q.astype(F32), 1, head_dim, head_pad)
    wo = jnp.pad(w_o[0], ((0, head_pad - head_dim), (0, 0)))
    wco = jnp.pad(w_co[0], ((0, head_pad - head_dim), (0, 0)))
    b1 = b_1.astype(F32)[None]

    normed1, inv_std1 = layer_norm(x_loc)
    h1_loc = (normed1 * (1.0 + scale1) + shift1).astype(BF16)

    def project_both(rows, get, ins, outs):
        put_rows(outs[0], rows, dot(get(0), ins[0][...]) + ins[1][...])
        put_rows(outs[1], rows, dot(get(1), ins[2][...]) + ins[3][...])

    h1_all, y_all, qkv, kv = gather_call(
        tp_size, 0, 'gather_h1_y', [h1_loc, y_loc], [wqkv, bqkv, wkv, bkv], (0, 1),
        [(batch, n_tok, 3 * head_pad), (batch, n_tok, 2 * head_pad)], [], project_both)
    q_self, k_self, v_self = [qkv[..., i * head_pad:(i + 1) * head_pad] for i in range(3)]
    k_cross, v_cross = [kv[..., i * head_pad:(i + 1) * head_pad] for i in range(2)]
    attn_val, attn_prob = attend(q_self, k_self, v_self, None, scale)

    def project_out(rows, put, ins, held, accs):
        put(0, dot(rows_of(ins[0], rows), ins[1][...]))

    attn_total, = scatter_call(tp_size, 1, 'scatter_o', n_loc, width, 1, [attn_val, wo], [], [], project_out)
    attn_total = attn_total + b_o
    x1_loc = (x_loc + gate1 * attn_total).astype(BF16)

    def project_q(rows, get, ins, outs):
        put_rows(outs[0], rows, dot(get(0), ins[0][...]) + ins[1][...])

    x1_all, q_cross = gather_call(tp_size, 2, 'gather_x1', [x1_loc], [wq, bq], (0,), [(batch, n_tok, head_pad)], [], project_q)
    slot_ok = lax.broadcasted_iota(jnp.int32, (batch, n_tok), 1) < len_loc[:, None]
    cross_val, cross_prob = attend(q_cross, k_cross, v_cross, slot_ok, scale)
    cross_total, = scatter_call(tp_size, 3, 'scatter_co', n_loc, width, 1, [cross_val, wco], [], [], project_out)
    cross_total = cross_total + b_co
    x2_loc = (x1_loc + cross_total).astype(BF16)

    normed2, inv_std2 = layer_norm(x2_loc)
    h2_loc = (normed2 * (1.0 + scale2) + shift2).astype(BF16)
    g_x2 = g_loc.astype(F32)
    g_mlp_loc = (g_x2 * gate2).astype(BF16)

    def mlp(rows, get, ins, outs):
        w1, bias1, w2 = ins
        gelu_out, g_hid, acc_w1, acc_w2, acc_b1 = outs
        h2_blk, g_blk = get(0), get(1)
        hidden = dot(h2_blk, w1[...]) + bias1[...]
        act, slope = gelu_pair(hidden)
        act = act.astype(BF16)
        put_rows(gelu_out, rows, act)
        g_hidden = dot(g_blk, w2[...], NT) * slope
        acc_b1[...] += row_sum(g_hidden)
        g_hidden = g_hidden.astype(BF16)
        put_rows(g_hid, rows, g_hidden)
        acc_w1[...] += dot(g_hidden, h2_blk, TN)
        acc_w2[...] += dot(act, g_blk, TN)

    gelu_out, g_hid, g_w_1, g_w_2, g_b_1 = gather_call(
        tp_size, 4, 'gather_h2_g', [h2_loc, g_mlp_loc], [w_1, b1, w_2], (),
        [(batch, n_tok, ffn), (batch, n_tok, ffn)], [(ffn, width), (ffn, width), (1, ffn)], mlp)

    def mlp_out(rows, put, ins, held, accs):
        g_hid, act, w1, w2 = ins
        put(0, dot(rows_of(g_hid, rows), w1[...], NT))
        put(1, dot(rows_of(act, rows), w2[...]))

    both, = scatter_call(tp_size, 5, 'scatter_h2_out', n_loc, width, 2, [g_hid, gelu_out, w_1, w_2], [], [], mlp_out)
    g_h2, mlp_total = both[:batch], both[batch:] + b_2
    x_out = (x2_loc + gate2 * mlp_total).astype(BF16)
    g_gate2 = jnp.sum(g_x2 * mlp_total, axis=(0, 1))
    g_b_2 = token_sum(g_mlp_loc)
    g_shift2 = token_sum(g_h2)
    g_scale2 = token_sum(g_h2 * normed2)
    g_x2 = g_x2 + layer_norm_back(normed2, inv_std2, g_h2 * (1.0 + scale2))

    def out_back(rows, get, ins, outs):
        val, weight = ins
        g_val, acc_w = outs
        g_blk = get(0)
        put_rows(g_val, rows, dot(g_blk, weight[...], NT))
        acc_w[...] += dot(rows_of(val, rows), g_blk, TN)

    g_cross_loc = g_x2.astype(BF16)
    g_b_co = token_sum(g_cross_loc)
    g_cross_val, g_w_co = gather_call(
        tp_size, 6, 'gather_g_cross', [g_cross_loc], [cross_val, wco], (), [(batch, n_tok, head_pad)], [(head_pad, width)], out_back)
    g_q_cross, g_k_cross, g_v_cross = attend_back(q_cross, k_cross, v_cross, cross_prob, g_cross_val, scale)
    g_kv = jnp.concatenate([g_k_cross, g_v_cross], axis=-1)

    def cross_in_back(rows, put, ins, held, accs):
        g_q, g_kv, wq, wkv = ins
        g_q_blk, g_kv_blk = rows_of(g_q, rows), rows_of(g_kv, rows)
        put(0, dot(g_q_blk, wq[...], NT))
        put(1, dot(g_kv_blk, wkv[...], NT))
        accs[0][...] += dot(g_q_blk, rows_of(held[0], rows), TN)
        accs[1][...] += dot(g_kv_blk, rows_of(held[1], rows), TN)
        accs[2][...] += row_sum(g_q_blk.astype(F32))
        accs[3][...] += row_sum(g_kv_blk.astype(F32))

    both, g_w_q, g_w_kv, g_b_q, g_b_kv = scatter_call(
        tp_size, 7, 'scatter_q_kv', n_loc, width, 2, [g_q_cross, g_kv, wq, wkv], [x1_all, y_all],
        [(head_pad, width), (2 * head_pad, width), (1, head_pad), (1, 2 * head_pad)], cross_in_back)
    g_x1 = g_x2 + both[:batch]
    g_y = both[batch:]

    g_gate1 = jnp.sum(g_x1 * attn_total, axis=(0, 1))
    g_attn_loc = (g_x1 * gate1).astype(BF16)
    g_b_o = token_sum(g_attn_loc)
    g_attn_val, g_w_o = gather_call(
        tp_size, 8, 'gather_g_attn', [g_attn_loc], [attn_val, wo], (), [(batch, n_tok, head_pad)], [(head_pad, width)], out_back)
    g_qkv = jnp.concatenate(attend_back(q_self, k_self, v_self, attn_prob, g_attn_val, scale), axis=-1)

    def self_in_back(rows, put, ins, held, accs):
        g_blk = rows_of(ins[0], rows)
        put(0, dot(g_blk, ins[1][...], NT))
        accs[0][...] += dot(g_blk, rows_of(held[0], rows), TN)
        accs[1][...] += row_sum(g_blk.astype(F32))

    g_h1, g_w_qkv, g_b_qkv = scatter_call(
        tp_size, 9, 'scatter_qkv', n_loc, width, 1, [g_qkv, wqkv], [h1_all],
        [(3 * head_pad, width), (1, 3 * head_pad)], self_in_back)
    g_x = g_x1 + layer_norm_back(normed1, inv_std1, g_h1 * (1.0 + scale1))
    sums = total_call(tp_size, 10, [token_sum(g_h1), token_sum(g_h1 * normed1), g_gate1, g_shift2, g_scale2, g_gate2, g_b_o, g_b_co, g_b_2])
    g_table = jnp.stack(sums[:6])
    g_b_o, g_b_co, g_b_2 = sums[6:]

    def head_weight(grad, n_part):
        return drop_pad(grad, n_part, head_dim, head_pad).T.astype(BF16)[:, None, :]

    def head_bias(grad, n_part):
        return drop_pad(grad[0], n_part, head_dim, head_pad)[None].astype(BF16)

    return (x_out, g_x.astype(BF16), g_y.astype(BF16), g_table,
            head_weight(g_w_qkv, 3), head_bias(g_b_qkv, 3), g_w_o[None, :head_dim].astype(BF16), g_b_o.astype(BF16),
            head_weight(g_w_q, 1), head_bias(g_b_q, 1), head_weight(g_w_kv, 2), head_bias(g_b_kv, 2),
            g_w_co[None, :head_dim].astype(BF16), g_b_co.astype(BF16),
            g_w_1.T.astype(BF16), g_b_1[0].astype(BF16), g_w_2.astype(BF16), g_b_2.astype(BF16))


def solution(mesh):
    token_spec = P('dp', 'tp', None)
    group_rows = ('dp', 'tp')
    in_specs = (token_spec, token_spec, P('dp', None), P('dp'), P(None, None), P(None, 'tp', None), P('tp', None), P('tp', None, None), P(None), P(None, 'tp', None), P('tp', None), P(None, 'tp', None), P('tp', None), P('tp', None, None), P(None), P(None, 'tp'), P('tp'), P('tp', None), P(None), token_spec)
    out_specs = (token_spec, token_spec, token_spec, P('dp', None), P('dp', 'tp', None), P(group_rows, None), P(group_rows, None, None), P('dp'), P('dp', 'tp', None), P(group_rows, None), P('dp', 'tp', None), P(group_rows, None), P(group_rows, None, None), P('dp'), P('dp', 'tp'), P(group_rows), P(group_rows, None), P('dp'))
    return jax.shard_map(functools.partial(device_block, mesh.shape['tp']), mesh=mesh, in_specs=in_specs, out_specs=out_specs, check_vma=False)
```

```python
import functools

import jax
import jax.numpy as jnp
from jax import lax
from jax.experimental import pallas as pl
from jax.experimental.pallas import tpu as pltpu
from jax.sharding import PartitionSpec as P

LN_EPS = 1e-6
MASK_FILL = -1e30
LANES = 128
MESH = pl.DeviceIdType.MESH
BF16 = jnp.bfloat16
F32 = jnp.float32
VMEM_LIMIT = 67 * 1000 * 1000
NN = (((1,), (0,)), ((), ()))
NT = (((1,), (1,)), ((), ()))
TN = (((0,), (0,)), ((), ()))
UP, DOWN = 0, 1


def dot(lhs, rhs, dims=NN):
    return lax.dot_general(lhs, rhs, dims, preferred_element_type=F32)


def place(tp_size):
    me = lax.axis_index('tp')
    return tp_size // 2, me // 2, lax.rem(me, 2)


def greet(ring, chip, core):
    barrier = pltpu.get_barrier_semaphore()
    for zz, cc in ((lax.rem(chip + 1, ring), core), (lax.rem(chip + ring - 1, ring), core), (chip, 1 - core)):
        pl.semaphore_signal(barrier, inc=1, device_id={'tp': zz * 2 + cc}, device_id_type=MESH)
    pl.semaphore_wait(barrier, 3)


def gather_body(tp_size, n_src, n_in, saves, n_acc, compute, *refs):
    ring, chip, core = place(tp_size)
    half = ring // 2
    srcs, refs = refs[:n_src], refs[n_src:]
    ins, refs = refs[:n_in], refs[n_in:]
    n_save = len(saves)
    full, rsend, rrecv, ssend, srecv, save_sem = refs[-6:]
    outs = refs[:-6]
    saved, outs = outs[:n_save], outs[n_save:]
    batch, n_loc = srcs[0].shape[0], srcs[0].shape[1]
    hb = batch * n_src // 2

    for acc in outs[len(outs) - n_acc:]:
        acc[...] = jnp.zeros_like(acc)

    def wrap(zz):
        return lax.rem(zz + ring, ring)

    def part(zz, cc, ch):
        row = pl.multiple_of((zz * 2 + cc) * n_loc, n_loc)
        return full.at[pl.ds(ch * hb, hb), pl.ds(row, n_loc), :]

    def own(ch):
        return srcs[ch] if n_src == 2 else srcs[0].at[pl.ds(ch * hb, hb)]

    def ring_copy(way, k, ch, sending):
        sign = -1 if way == UP else 1
        zb = wrap(chip + sign * (k - 1 if sending else k))
        src = own(ch) if (sending and k == 1) else part(zb, core, ch)
        return pltpu.make_async_remote_copy(
            src_ref=src, dst_ref=part(zb, core, ch),
            send_sem=rsend.at[way, k - 1, ch], recv_sem=rrecv.at[way, k - 1, ch],
            device_id={'tp': wrap(chip - sign) * 2 + core}, device_id_type=MESH)

    def chip_at(slot):
        k = (slot + 1) // 2
        return wrap(chip - k) if slot % 2 else wrap(chip + k)

    def sib_copy(slot, ch, sending):
        zb = chip_at(slot)
        cc = core if sending else 1 - core
        src = own(ch) if (sending and slot == 0) else part(zb, cc, ch)
        return pltpu.make_async_remote_copy(
            src_ref=src, dst_ref=part(zb, cc, ch),
            send_sem=ssend.at[slot, ch], recv_sem=srecv.at[slot, ch],
            device_id={'tp': chip * 2 + 1 - core}, device_id_type=MESH)

    def carries(way, k, ch):
        return k < half or (k == half and ch == way)

    def slot_of(way, k):
        return 2 * half - 1 if k == half else (2 * k - 1 if way == UP else 2 * k)

    greet(ring, chip, core)
    ring_copy(UP, 1, 0, True).start()
    ring_copy(DOWN, 1, 1, True).start()
    ring_copy(UP, 1, 1, True).start()
    ring_copy(DOWN, 1, 0, True).start()
    sib_copy(0, 0, True).start()
    sib_copy(0, 1, True).start()
    for ch in (0, 1):
        row = pl.multiple_of((chip * 2 + core) * n_loc, n_loc)
        full[pl.ds(ch * hb, hb), pl.ds(row, n_loc), :] = own(ch)[...]

    def arrive(way, k, ch):
        ring_copy(way, k, ch, False).wait_recv()
        if carries(way, k + 1, ch):
            ring_copy(way, k + 1, ch, True).start()
        sib_copy(slot_of(way, k), ch, True).start()

    def group(g):
        k = g // 2 + 1
        if g % 2 == 0:
            arrive(UP, k, 0)
            arrive(DOWN, k, 1)
        else:
            arrive(UP, k, 1)
            arrive(DOWN, k, 0)

    def save_copy(stream, slot, zz):
        rows = pl.ds(pl.multiple_of(zz * 2 * n_loc, 2 * n_loc), 2 * n_loc)
        return pltpu.make_async_copy(
            full.at[pl.ds(saves[stream] * batch, batch), rows, :], saved[stream].at[:, rows, :], save_sem.at[stream, slot])

    def step(slot, carry):
        for s in range(ring):
            @pl.when(slot == s)
            def _():
                if s < ring - 2:
                    group(s)
                elif s == ring - 1:
                    group(ring - 2)
                sib_copy(s, 0, False).wait_recv()
                sib_copy(s, 1, False).wait_recv()
        k = (slot + 1) // 2
        sign = 1 - 2 * lax.rem(slot, 2)
        zz = wrap(chip + sign * k)
        rows = pl.ds(pl.multiple_of(zz * 2 * n_loc, 2 * n_loc), 2 * n_loc)
        for stream in range(n_save):
            save_copy(stream, slot, zz).start()
        compute(rows, lambda i: full[pl.ds(i * batch, batch), rows, :].reshape(batch * 2 * n_loc, full.shape[2]), ins, outs)
        return carry

    lax.fori_loop(0, ring, step, None)

    for way in (UP, DOWN):
        for k in range(1, half + 1):
            for ch in (0, 1):
                if carries(way, k, ch):
                    ring_copy(way, k, ch, True).wait_send()
    for slot in range(ring):
        for ch in (0, 1):
            sib_copy(slot, ch, True).wait_send()
        for stream in range(n_save):
            save_copy(stream, slot, chip_at(slot)).wait()


def gather_call(tp_size, cid, name, blocks, ins, saves, outs, accs, compute):
    batch, n_loc, width = blocks[0].shape
    n_tok = n_loc * tp_size
    ring, half = tp_size // 2, tp_size // 4
    vmem = pl.BlockSpec(memory_space=pltpu.VMEM)
    return pl.pallas_call(
        functools.partial(gather_body, tp_size, len(blocks), len(ins), saves, len(accs), compute),
        out_shape=[jax.ShapeDtypeStruct((batch, n_tok, width), BF16)] * len(saves)
        + [jax.ShapeDtypeStruct(s, BF16) for s in outs] + [jax.ShapeDtypeStruct(s, F32) for s in accs],
        in_specs=[vmem] * (len(blocks) + len(ins)),
        out_specs=[pl.BlockSpec(memory_space=pl.ANY)] * len(saves) + [vmem] * (len(outs) + len(accs)),
        scratch_shapes=[
            pltpu.VMEM((batch * len(blocks), n_tok, width), BF16),
            pltpu.SemaphoreType.DMA((2, half, 2)),
            pltpu.SemaphoreType.DMA((2, half, 2)),
            pltpu.SemaphoreType.DMA((ring, 2)),
            pltpu.SemaphoreType.DMA((ring, 2)),
            pltpu.SemaphoreType.DMA((max(1, len(saves)), ring)),
        ],
        compiler_params=pltpu.CompilerParams(collective_id=cid, has_side_effects=True, vmem_limit_bytes=VMEM_LIMIT),
        name=name,
    )(*blocks, *ins)


def scatter_body(tp_size, n_out, n_in, n_load, n_acc, compute, *refs):
    ring, chip, core = place(tp_size)
    half = ring // 2
    ins, refs = refs[:n_in], refs[n_in:]
    loads, refs = refs[:n_load], refs[n_load:]
    result, refs = refs[0], refs[1:]
    accs, refs = refs[:n_acc], refs[n_acc:]
    held, refs = refs[:n_load], refs[n_load:]
    pbuf, sibr, snd, rcv, rsend, rrecv, ssend, srecv, load_sem = refs
    nb, n_loc = result.shape[0], result.shape[1]
    batch, hb = nb // n_out, nb // 2

    def wrap(zz):
        return lax.rem(zz + ring, ring)

    def load_copy(i):
        return pltpu.make_async_copy(loads[i], held[i], load_sem.at[i])

    for i in range(n_load):
        load_copy(i).start()
    for acc in accs:
        acc[...] = jnp.zeros_like(acc)

    def ring_copy(way, s, ch):
        sign = 1 if way == UP else -1
        part = pl.ds(ch * hb, hb)
        return pltpu.make_async_remote_copy(
            src_ref=snd.at[way, s, part], dst_ref=rcv.at[way, s, part],
            send_sem=rsend.at[way, s, ch], recv_sem=rrecv.at[way, s, ch],
            device_id={'tp': wrap(chip + sign) * 2 + core}, device_id_type=MESH)

    def sib_copy(slot):
        rows = pl.ds(pl.multiple_of((1 - core) * n_loc, n_loc), n_loc)
        return pltpu.make_async_remote_copy(
            src_ref=pbuf.at[slot, :, rows, :], dst_ref=sibr.at[slot],
            send_sem=ssend.at[slot], recv_sem=srecv.at[slot],
            device_id={'tp': chip * 2 + 1 - core}, device_id_type=MESH)

    def own_sum(slot, part):
        rows = pl.ds(pl.multiple_of(core * n_loc, n_loc), n_loc)
        return pbuf[slot, part, rows, :].astype(F32) + sibr[slot, part].astype(F32)

    def starts_at(way, ch):
        return 0 if ch == way else 1

    def pass_on(way, s, slot, ch):
        part = pl.ds(ch * hb, hb)
        total = own_sum(slot, part)
        if s > starts_at(way, ch):
            ring_copy(way, s - 1, ch).wait_recv()
            total = total + rcv[way, s - 1, part].astype(F32)
        snd[way, s, part] = total.astype(BF16)
        ring_copy(way, s, ch).start()

    def ring_step(s):
        if s == 0:
            sib_copy(0).wait_recv()
            pass_on(UP, 0, 0, 0)
            pass_on(DOWN, 0, 0, 1)
            return
        sib_copy(2 * s - 1).wait_recv()
        pass_on(UP, s, 2 * s - 1, 1)
        sib_copy(2 * s).wait_recv()
        pass_on(DOWN, s, 2 * s, 0)
        pass_on(UP, s, 2 * s - 1, 0)
        pass_on(DOWN, s, 2 * s, 1)

    greet(ring, chip, core)
    for i in range(n_load):
        load_copy(i).wait()

    def step(slot, carry):
        away = half - (slot + 1) // 2
        sign = 2 * lax.rem(slot, 2) - 1
        zz = wrap(chip + sign * away)
        rows = pl.ds(pl.multiple_of(zz * 2 * n_loc, 2 * n_loc), 2 * n_loc)

        def put(i, value):
            pbuf[slot, pl.ds(i * batch, batch)] = value.astype(BF16).reshape(batch, 2 * n_loc, value.shape[-1])

        compute(rows, put, ins, held, accs)
        sib_copy(slot).start()
        for s in range(half):
            @pl.when(slot == 2 * s + 1)
            def _():
                ring_step(s)
        return carry

    lax.fori_loop(0, ring, step, None)

    sib_copy(ring - 1).wait_recv()
    for ch, order in ((1, (UP, DOWN)), (0, (DOWN, UP))):
        part = pl.ds(ch * hb, hb)
        total = own_sum(ring - 1, part)
        for way in order:
            ring_copy(way, half - 1, ch).wait_recv()
            total = total + rcv[way, half - 1, part].astype(F32)
        result[part] = total
    for way in (UP, DOWN):
        for s in range(half):
            for ch in (0, 1):
                if s >= starts_at(way, ch):
                    ring_copy(way, s, ch).wait_send()
    for slot in range(ring):
        sib_copy(slot).wait_send()


def scatter_call(tp_size, cid, name, n_loc, width, n_out, ins, loads, accs, compute):
    batch = ins[0].shape[0]
    nb = batch * n_out
    ring, half = tp_size // 2, tp_size // 4
    vmem = pl.BlockSpec(memory_space=pltpu.VMEM)
    return pl.pallas_call(
        functools.partial(scatter_body, tp_size, n_out, len(ins), len(loads), len(accs), compute),
        out_shape=[jax.ShapeDtypeStruct((nb, n_loc, width), F32)] + [jax.ShapeDtypeStruct(s, F32) for s in accs],
        in_specs=[vmem] * len(ins) + [pl.BlockSpec(memory_space=pl.ANY)] * len(loads),
        out_specs=[vmem] * (1 + len(accs)),
        scratch_shapes=[pltpu.VMEM(a.shape, a.dtype) for a in loads] + [
            pltpu.VMEM((ring, nb, 2 * n_loc, width), BF16),
            pltpu.VMEM((ring, nb, n_loc, width), BF16),
            pltpu.VMEM((2, half, nb, n_loc, width), BF16),
            pltpu.VMEM((2, half, nb, n_loc, width), BF16),
            pltpu.SemaphoreType.DMA((2, half, 2)),
            pltpu.SemaphoreType.DMA((2, half, 2)),
            pltpu.SemaphoreType.DMA((ring,)),
            pltpu.SemaphoreType.DMA((ring,)),
            pltpu.SemaphoreType.DMA((max(1, len(loads)),)),
        ],
        compiler_params=pltpu.CompilerParams(collective_id=cid, has_side_effects=True, vmem_limit_bytes=VMEM_LIMIT),
        name=name,
    )(*ins, *loads)


class Place:
    def __init__(self, tp_size):
        self.tp_size = tp_size
        self.me = lax.axis_index('tp')
        self.ring, self.chip, self.core = tp_size // 2, self.me // 2, lax.rem(self.me, 2)
        self.half = self.ring // 2

    def wrap(self, zz):
        return lax.rem(zz + self.ring, self.ring)

    def sibling(self):
        return {'tp': self.chip * 2 + 1 - self.core}

    def ahead(self, sign):
        return {'tp': self.wrap(self.chip + sign) * 2 + self.core}

    def greet_all(self):
        barrier = pltpu.get_barrier_semaphore()
        for d in range(1, self.tp_size):
            pl.semaphore_signal(barrier, inc=1, device_id={'tp': lax.rem(self.me + d, self.tp_size)}, device_id_type=MESH)
        pl.semaphore_wait(barrier, self.tp_size - 1)

    def greet(self):
        greet(self.ring, self.chip, self.core)


class Gather:
    def __init__(self, at, own, full, sems):
        self.at, self.own_ref, self.full = at, own, full
        self.rsend, self.rrecv, self.ssend, self.srecv = sems
        self.batch, self.n_loc = own.shape[0], own.shape[1]
        self.hb = self.batch // 2

    def part(self, zz, cc, ch):
        row = pl.multiple_of((zz * 2 + cc) * self.n_loc, self.n_loc)
        return self.full.at[pl.ds(ch * self.hb, self.hb), pl.ds(row, self.n_loc), :]

    def own(self, ch):
        return self.own_ref.at[pl.ds(ch * self.hb, self.hb)]

    def ring_copy(self, way, k, ch, sending):
        at = self.at
        sign = -1 if way == UP else 1
        zb = at.wrap(at.chip + sign * (k - 1 if sending else k))
        src = self.own(ch) if (sending and k == 1) else self.part(zb, at.core, ch)
        return pltpu.make_async_remote_copy(
            src_ref=src, dst_ref=self.part(zb, at.core, ch),
            send_sem=self.rsend.at[way, k - 1, ch], recv_sem=self.rrecv.at[way, k - 1, ch],
            device_id=at.ahead(-sign), device_id_type=MESH)

    def chip_at(self, slot):
        k = (slot + 1) // 2
        return self.at.wrap(self.at.chip - k) if slot % 2 else self.at.wrap(self.at.chip + k)

    def sib_copy(self, slot, ch, sending):
        at = self.at
        cc = at.core if sending else 1 - at.core
        zb = self.chip_at(slot)
        src = self.own(ch) if (sending and slot == 0) else self.part(zb, cc, ch)
        return pltpu.make_async_remote_copy(
            src_ref=src, dst_ref=self.part(zb, cc, ch),
            send_sem=self.ssend.at[slot, ch], recv_sem=self.srecv.at[slot, ch],
            device_id=at.sibling(), device_id_type=MESH)

    def carries(self, way, k, ch):
        return k < self.at.half or (k == self.at.half and ch == way)

    def slot_of(self, way, k):
        half = self.at.half
        return 2 * half - 1 if k == half else (2 * k - 1 if way == UP else 2 * k)

    def start(self):
        for way, ch in ((UP, 0), (DOWN, 1), (UP, 1), (DOWN, 0)):
            self.ring_copy(way, 1, ch, True).start()
        for ch in (0, 1):
            self.sib_copy(0, ch, True).start()
        row = pl.multiple_of(self.at.me * self.n_loc, self.n_loc)
        self.full[:, pl.ds(row, self.n_loc), :] = self.own_ref[...]

    def arrive(self, way, k, ch):
        self.ring_copy(way, k, ch, False).wait_recv()
        if self.carries(way, k + 1, ch):
            self.ring_copy(way, k + 1, ch, True).start()
        self.sib_copy(self.slot_of(way, k), ch, True).start()

    def group(self, g):
        k = g // 2 + 1
        first, second = ((UP, 0), (DOWN, 1)) if g % 2 == 0 else ((UP, 1), (DOWN, 0))
        self.arrive(first[0], k, first[1])
        self.arrive(second[0], k, second[1])

    def groups_before(self, slot):
        last = self.at.ring - 1
        return () if slot == last - 1 else ((last - 1,) if slot == last else (slot,))

    def ready(self, slot):
        for ch in (0, 1):
            self.sib_copy(slot, ch, False).wait_recv()

    def rows(self, slot):
        k = (slot + 1) // 2
        zz = self.at.wrap(self.at.chip + (1 - 2 * lax.rem(slot, 2)) * k)
        return pl.ds(pl.multiple_of(zz * 2 * self.n_loc, 2 * self.n_loc), 2 * self.n_loc)

    def save_copy(self, dest, sem, slot):
        rows = self.rows(slot)
        return pltpu.make_async_copy(self.full.at[:, rows, :], dest.at[:, rows, :], sem.at[slot])

    def finish(self):
        for way in (UP, DOWN):
            for k in range(1, self.at.half + 1):
                for ch in (0, 1):
                    if self.carries(way, k, ch):
                        self.ring_copy(way, k, ch, True).wait_send()
        for slot in range(self.at.ring):
            for ch in (0, 1):
                self.sib_copy(slot, ch, True).wait_send()


class Scatter:
    def __init__(self, at, pbuf, sibr, rcv, sems):
        self.at, self.pbuf, self.sibr, self.rcv = at, pbuf, sibr, rcv
        self.rsend, self.rrecv, self.ssend, self.srecv = sems
        self.batch, self.n_loc = sibr.shape[1], sibr.shape[2]
        self.hb = self.batch // 2

    def slot_of(self, way, s):
        return 0 if s == 0 else (2 * s - 1 if way == UP else 2 * s)

    def rows(self, slot):
        at = self.at
        away = at.half - (slot + 1) // 2
        zz = at.wrap(at.chip + (2 * lax.rem(slot, 2) - 1) * away)
        return pl.ds(pl.multiple_of(zz * 2 * self.n_loc, 2 * self.n_loc), 2 * self.n_loc)

    def put(self, slot, value):
        self.pbuf[slot] = value.astype(BF16).reshape(self.batch, 2 * self.n_loc, value.shape[-1])
        self.sib_copy(slot).start()

    def ring_copy(self, way, s, ch):
        part = pl.ds(ch * self.hb, self.hb)
        return pltpu.make_async_remote_copy(
            src_ref=self.sibr.at[self.slot_of(way, s), part], dst_ref=self.rcv.at[way, s, part],
            send_sem=self.rsend.at[way, s, ch], recv_sem=self.rrecv.at[way, s, ch],
            device_id=self.at.ahead(1 if way == UP else -1), device_id_type=MESH)

    def sib_copy(self, slot):
        rows = pl.ds(pl.multiple_of((1 - self.at.core) * self.n_loc, self.n_loc), self.n_loc)
        return pltpu.make_async_remote_copy(
            src_ref=self.pbuf.at[slot, :, rows, :], dst_ref=self.sibr.at[slot],
            send_sem=self.ssend.at[slot], recv_sem=self.srecv.at[slot],
            device_id=self.at.sibling(), device_id_type=MESH)

    def own_sum(self, slot, part):
        rows = pl.ds(pl.multiple_of(self.at.core * self.n_loc, self.n_loc), self.n_loc)
        return self.pbuf[slot, part, rows, :].astype(F32) + self.sibr[slot, part].astype(F32)

    def starts_at(self, way, ch):
        return 0 if ch == way else 1

    def pass_on(self, way, s, ch):
        slot, part = self.slot_of(way, s), pl.ds(ch * self.hb, self.hb)
        total = self.own_sum(slot, part)
        if s > self.starts_at(way, ch):
            self.ring_copy(way, s - 1, ch).wait_recv()
            total = total + self.rcv[way, s - 1, part].astype(F32)
        self.sibr[slot, part] = total.astype(BF16)
        self.ring_copy(way, s, ch).start()

    def step(self, s):
        if s == 0:
            self.sib_copy(0).wait_recv()
            self.pass_on(UP, 0, 0)
            self.pass_on(DOWN, 0, 1)
            return
        self.sib_copy(2 * s - 1).wait_recv()
        self.pass_on(UP, s, 1)
        self.sib_copy(2 * s).wait_recv()
        self.pass_on(DOWN, s, 0)
        self.pass_on(UP, s, 0)
        self.pass_on(DOWN, s, 1)

    def final(self, use):
        last = self.at.ring - 1
        self.sib_copy(last).wait_recv()
        for ch, order in ((1, (UP, DOWN)), (0, (DOWN, UP))):
            part = pl.ds(ch * self.hb, self.hb)
            total = self.own_sum(last, part)
            for way in order:
                self.ring_copy(way, self.at.half - 1, ch).wait_recv()
                total = total + self.rcv[way, self.at.half - 1, part].astype(F32)
            use(part, total)

    def finish(self):
        for way in (UP, DOWN):
            for s in range(self.at.half):
                for ch in (0, 1):
                    if s >= self.starts_at(way, ch):
                        self.ring_copy(way, s, ch).wait_send()
        for slot in range(self.at.ring):
            self.sib_copy(slot).wait_send()


def loop_slots(n, hooks, body):
    def step(slot, carry):
        for s in range(n):
            @pl.when(slot == s)
            def _():
                hooks(s)
        body(slot)
        return carry
    lax.fori_loop(0, n, step, None)


def gather_sems(tp_size):
    ring, half = tp_size // 2, tp_size // 4
    return [pltpu.SemaphoreType.DMA(s) for s in ((2, half, 2), (2, half, 2), (ring, 2), (ring, 2))]


def scatter_sems(tp_size):
    ring, half = tp_size // 2, tp_size // 4
    return [pltpu.SemaphoreType.DMA(s) for s in ((2, half, 2), (2, half, 2), (ring,), (ring,))]


def pad_rows(dest, source, head_dim):
    parts = source.shape[0] // head_dim
    head_pad = dest.shape[0] // parts
    width = dest.shape[1]
    for i in range(parts):
        dest[i * head_pad:i * head_pad + head_dim, :] = source[i * head_dim:(i + 1) * head_dim, :]
        dest[i * head_pad + head_dim:(i + 1) * head_pad, :] = jnp.zeros((head_pad - head_dim, width), dest.dtype)


def mod_row(t_ref, table_ref, i):
    width = table_ref.shape[1]
    return table_ref[i:i + 1, :].astype(F32) + t_ref[:, i * width:(i + 1) * width].astype(F32)


def softmax_of(scores):
    top = jnp.max(scores, axis=-1, keepdims=True)
    powers = jnp.exp(scores - top)
    return powers * (1.0 / jnp.sum(powers, axis=-1, keepdims=True))


def forward_body(tp_size, head_dim, *refs):
    at = Place(tp_size)
    ins, refs = refs[:15], refs[15:]
    x, y, t_emb, table, lens, wqkv_in, bqkv, wkv_in, bkv, wq_in, bq, wo_in, bo, wco_in, bco = ins
    outs, refs = refs[:12], refs[12:]
    h1_out, y_out, x1_out = outs[:3]
    scratch, refs = refs[:9], refs[9:]
    qkv, kv, q_c, val, cval, prob, cprob, atot, x2 = scratch
    h1, x1, mod, fh, fy, fx, pbuf, sibr1, rcv1, sibr2, rcv2, wqkv, wkv, wq, wo, wco = refs[:16]
    sems = refs[16:]
    gather_h = Gather(at, h1, fh, sems[0:4])
    gather_y = Gather(at, y, fy, sems[4:8])
    gather_x = Gather(at, x1, fx, sems[8:12])
    scat_o = Scatter(at, pbuf, sibr1, rcv1, sems[12:16])
    scat_c = Scatter(at, pbuf, sibr2, rcv2, sems[16:20])
    save_sem, out_sem = sems[20], sems[21]
    batch = x.shape[0]
    head_pad = wq.shape[0]
    scale = head_dim ** -0.5

    def out_copy(i):
        return pltpu.make_async_copy(scratch[i], outs[3 + i], out_sem.at[i])

    for i in range(3):
        mod[i] = mod_row(t_emb, table, i)

    def norm_one(b, carry):
        rows = x[b].astype(F32)
        centered = rows - jnp.mean(rows, axis=-1, keepdims=True)
        normed = centered * lax.rsqrt(jnp.mean(centered * centered, axis=-1, keepdims=True) + LN_EPS)
        h1[b] = (normed * (1.0 + mod[1, pl.ds(b, 1), :]) + mod[0, pl.ds(b, 1), :]).astype(BF16)
        return carry

    lax.fori_loop(0, batch, norm_one, None)
    at.greet()
    gather_h.start()
    for dest, source in ((wqkv, wqkv_in), (wkv, wkv_in), (wq, wq_in), (wo, wo_in), (wco, wco_in)):
        pad_rows(dest, source, head_dim)

    def hooks(s):
        for g in gather_h.groups_before(s):
            gather_h.group(g)
        gather_h.ready(s)
        if s == at.ring - 4:
            gather_y.start()

    def project(slot):
        rows = gather_h.rows(slot)
        gather_h.save_copy(h1_out, save_sem.at[0], slot).start()
        put_rows(qkv, rows, dot(rows_of(fh, rows), wqkv[...], NT) + bqkv[...])

    loop_slots(at.ring, hooks, project)

    def hooks(b):
        if b == batch // 2:
            gather_y.group(0)
        if b == batch - 1:
            gather_y.group(1)

    def attend_self(b):
        q_b, k_b, v_b = [qkv[b, :, i * head_pad:(i + 1) * head_pad] for i in range(3)]
        p_b = softmax_of(dot(q_b, k_b, NT) * scale).astype(BF16)
        prob[b] = p_b
        val[b] = dot(p_b, v_b).astype(BF16)

    loop_slots(batch, hooks, attend_self)
    for i in (0, 3, 5):
        out_copy(i).start()

    ynext = {2: 2, 3: 3, 5: 4, 6: 5, 7: 6}

    def hooks(s):
        if s >= 2 and s % 2 == 0:
            scat_o.step(s // 2 - 1)
        if s in ynext:
            gather_y.group(ynext[s])

    def project_o(slot):
        scat_o.put(slot, dot(rows_of(val, scat_o.rows(slot)), wo[...]))

    loop_slots(at.ring, hooks, project_o)
    scat_o.step(at.half - 1)

    def take_o(part, total):
        atot[part] = total + bo[...].astype(F32)

    scat_o.final(take_o)
    out_copy(7).start()

    def x1_one(b, carry):
        x1[b] = (x[b].astype(F32) + mod[2, pl.ds(b, 1), :] * atot[b]).astype(BF16)
        return carry

    lax.fori_loop(0, batch, x1_one, None)

    gather_x.start()

    def hooks(s):
        for g in gather_x.groups_before(s):
            gather_x.group(g)
        gather_y.ready(s)
        gather_x.ready(s)

    def project(slot):
        rows = gather_x.rows(slot)
        gather_y.save_copy(y_out, save_sem.at[1], slot).start()
        gather_x.save_copy(x1_out, save_sem.at[2], slot).start()
        put_rows(kv, rows, dot(rows_of(fy, rows), wkv[...], NT) + bkv[...])
        put_rows(q_c, rows, dot(rows_of(fx, rows), wq[...], NT) + bq[...])

    loop_slots(at.ring, hooks, project)
    scat_o.finish()

    def attend_cross(b, carry):
        k_b, v_b = [kv[b, :, i * head_pad:(i + 1) * head_pad] for i in range(2)]
        scores = dot(q_c[b], k_b, NT) * scale
        slots = lax.broadcasted_iota(jnp.int32, scores.shape, 1)
        p_b = softmax_of(jnp.where(slots < lens[b], scores, MASK_FILL)).astype(BF16)
        cprob[b] = p_b
        cval[b] = dot(p_b, v_b).astype(BF16)
        return carry

    lax.fori_loop(0, batch, attend_cross, None)
    for i in (1, 2, 4, 6):
        out_copy(i).start()

    def hooks(s):
        if s >= 2 and s % 2 == 0:
            scat_c.step(s // 2 - 1)

    def project_c(slot):
        scat_c.put(slot, dot(rows_of(cval, scat_c.rows(slot)), wco[...]))

    loop_slots(at.ring, hooks, project_c)
    scat_c.step(at.half - 1)

    def take_c(part, total):
        x2[part] = (x1[part].astype(F32) + total + bco[...].astype(F32)).astype(BF16)

    scat_c.final(take_c)
    out_copy(8).start()
    for stream in (gather_h, gather_y, gather_x, scat_c):
        stream.finish()
    for slot in range(at.ring):
        gather_h.save_copy(h1_out, save_sem.at[0], slot).wait()
        gather_y.save_copy(y_out, save_sem.at[1], slot).wait()
        gather_x.save_copy(x1_out, save_sem.at[2], slot).wait()
    for i in range(9):
        out_copy(i).wait()


def forward_call(tp_size, cid, head_dim, head_pad, *ins):
    batch, n_loc, width = ins[0].shape
    n_tok = n_loc * tp_size
    ring, half = tp_size // 2, tp_size // 4
    tokens = lambda last: (batch, n_tok, last)
    local = (batch, n_loc, width)
    kept = [(tokens(3 * head_pad), BF16), (tokens(2 * head_pad), BF16), (tokens(head_pad), BF16), (tokens(head_pad), BF16),
            (tokens(head_pad), BF16), (tokens(n_tok), BF16), (tokens(n_tok), BF16), (local, F32), (local, BF16)]
    vmem = pl.BlockSpec(memory_space=pltpu.VMEM)
    sib, rcv = (ring, *local), (2, half, *local)
    return pl.pallas_call(
        functools.partial(forward_body, tp_size, head_dim),
        out_shape=[jax.ShapeDtypeStruct(tokens(width), BF16)] * 3 + [jax.ShapeDtypeStruct(*k) for k in kept],
        in_specs=[vmem] * len(ins),
        out_specs=[pl.BlockSpec(memory_space=pl.ANY)] * (3 + len(kept)),
        scratch_shapes=[pltpu.VMEM(*k) for k in kept] + [
            pltpu.VMEM(local, BF16), pltpu.VMEM(local, BF16), pltpu.VMEM((3, batch, width), F32),
            pltpu.VMEM(tokens(width), BF16), pltpu.VMEM(tokens(width), BF16), pltpu.VMEM(tokens(width), BF16),
            pltpu.VMEM((ring, batch, 2 * n_loc, width), BF16),
            pltpu.VMEM(sib, BF16), pltpu.VMEM(rcv, BF16), pltpu.VMEM(sib, BF16), pltpu.VMEM(rcv, BF16)]
        + [pltpu.VMEM((n * head_pad, width), BF16) for n in (3, 2, 1, 1, 1)]
        + gather_sems(tp_size) * 3 + scatter_sems(tp_size) * 2
        + [pltpu.SemaphoreType.DMA((3, ring)), pltpu.SemaphoreType.DMA((len(kept),))],
        compiler_params=pltpu.CompilerParams(collective_id=cid, has_side_effects=True, vmem_limit_bytes=VMEM_LIMIT),
        name='attention_forward',
    )(*ins)


class RowFeed:
    def __init__(self, source, buf, sem, rows):
        self.source, self.buf, self.sem, self.rows = source, buf, sem, rows

    def copy(self, slot):
        side = lax.rem(slot, 2)
        return pltpu.make_async_copy(self.source.at[:, self.rows(slot), :], self.buf.at[side], self.sem.at[side])

    def take(self, slot, n):
        @pl.when(slot + 1 < n)
        def _():
            self.copy(slot + 1).start()
        self.copy(slot).wait()
        block = self.buf[lax.rem(slot, 2)]
        return block.reshape(block.shape[0] * block.shape[1], block.shape[2])


def small_total(at, src, got, mine, out, sems):
    send1, recv1, send2, recv2 = sems
    tiles = src.shape[1] // LANES

    def lanes(i):
        return pl.ds(i * LANES, LANES)

    def first(tile, peer_slot):
        return pltpu.make_async_remote_copy(
            src_ref=src.at[:, lanes(tile)], dst_ref=got.at[peer_slot], send_sem=send1.at[tile], recv_sem=recv1.at[peer_slot],
            device_id={'tp': tile}, device_id_type=MESH)

    def second(tile, d):
        return pltpu.make_async_remote_copy(
            src_ref=mine, dst_ref=out.at[:, lanes(tile)], send_sem=send2.at[d - 1], recv_sem=recv2.at[tile],
            device_id={'tp': lax.rem(at.me + d, at.tp_size)}, device_id_type=MESH)

    for tile in range(tiles):
        @pl.when(at.me != tile)
        def _():
            first(tile, lax.rem(at.me - tile + at.tp_size, at.tp_size) - 1).start()
    for tile in range(tiles):
        @pl.when(at.me == tile)
        def _():
            total = src[:, tile * LANES:(tile + 1) * LANES]
            for d in range(1, at.tp_size):
                first(tile, d - 1).wait_recv()
                total = total + got[d - 1]
            mine[...] = total
            for d in range(1, at.tp_size):
                second(tile, d).start()
            out[:, tile * LANES:(tile + 1) * LANES] = total
            for d in range(1, at.tp_size):
                second(tile, d).wait_send()
    for tile in range(tiles):
        @pl.when(at.me != tile)
        def _():
            second(tile, 1).wait_recv()
            first(tile, 0).wait_send()


def backward_body(tp_size, head_dim, *refs):
    at = Place(tp_size)
    ins, refs = refs[:12], refs[12:]
    g_cross, g_x2, x, atot, t_emb, table, wqkv_in, wkv_in, wq_in, wo_in, wco_in, sums_in = ins
    loads, refs = refs[:7], refs[7:]
    feeds, refs = refs[:3], refs[3:]
    outs, refs = refs[:11], refs[11:]
    g_x, g_y, sums_out, gw_qkv, gw_kv, gw_q, gw_o, gw_co, gb_qkv, gb_kv, gb_q = outs
    held, refs = refs[:7], refs[7:]
    qkv, kv, q_c, val, cval, prob, cprob = held
    full, pbuf, sibr1, rcv1, pbufy, sibr2, rcv2, wqkv, wkv, wq, wo, wco = refs[:12]
    g_val, g_qkv, g_kv, g_q, g_x1, g_h1, g_attn, mod, sums, got, mine, feed_a, feed_y = refs[12:25]
    sems = refs[25:]
    gather_c = Gather(at, g_cross, full, sems[0:4])
    gather_a = Gather(at, g_attn, full, sems[4:8])
    scat_q = Scatter(at, pbuf, sibr1, rcv1, sems[8:12])
    scat_y = Scatter(at, pbufy, sibr2, rcv2, sems[12:16])
    scat_h = Scatter(at, pbuf, sibr1, rcv1, sems[16:20])
    load_sem, feed_sem = sems[20], sems[21]
    feed_h = RowFeed(feeds[0], feed_a, feed_sem.at[0], scat_h.rows)
    feed_x = RowFeed(feeds[1], feed_a, feed_sem.at[1], scat_q.rows)
    feed_yy = RowFeed(feeds[2], feed_y, feed_sem.at[2], scat_y.rows)
    batch, n_loc, width = x.shape
    ring, half = at.ring, at.half
    head_pad = wq.shape[0]
    scale = head_dim ** -0.5

    def load_copy(i):
        return pltpu.make_async_copy(loads[i], held[i], load_sem.at[i])

    for i in range(7):
        load_copy(i).start()
    at.greet_all()
    gather_c.start()
    feed_x.copy(0).start()
    feed_yy.copy(0).start()
    for i in range(3):
        mod[i] = mod_row(t_emb, table, i)
    for dest, source in ((wqkv, wqkv_in), (wkv, wkv_in), (wq, wq_in), (wo, wo_in), (wco, wco_in)):
        pad_rows(dest, source, head_dim)
    sums[...] = sums_in[...]
    for acc in outs[3:]:
        acc[...] = jnp.zeros_like(acc)
    for i in range(7):
        load_copy(i).wait()

    def out_back(gather, value, weight, acc):
        def body(slot):
            rows = gather.rows(slot)
            block = rows_of(full, rows)
            put_rows(g_val, rows, dot(block, weight[...], NT))
            acc[...] += dot(rows_of(value, rows), block, TN)
        return body

    def hooks(s):
        for g in gather_c.groups_before(s):
            gather_c.group(g)
        gather_c.ready(s)

    loop_slots(ring, hooks, out_back(gather_c, cval, wco, gw_co))
    gather_c.finish()

    def back_one(q_b, k_b, v_b, p_b, g_b):
        g_p = dot(g_b, v_b, NT)
        p_f = p_b.astype(F32)
        row_dot = jnp.sum(g_p * p_f, axis=-1, keepdims=True)
        g_s = (p_f * (g_p - row_dot) * scale).astype(BF16)
        return dot(g_s, k_b).astype(BF16), dot(g_s, q_b, TN).astype(BF16), dot(p_b, g_b, TN).astype(BF16)

    def cross_back(b, carry):
        parts = back_one(q_c[b], kv[b, :, :head_pad], kv[b, :, head_pad:], cprob[b], g_val[b])
        g_q[b] = parts[0]
        g_kv[b, :, :head_pad] = parts[1]
        g_kv[b, :, head_pad:] = parts[2]
        return carry

    lax.fori_loop(0, batch, cross_back, None)

    def hooks(s):
        if s >= 2 and s % 2 == 0:
            scat_q.step(s // 2 - 1)

    def put_q(slot):
        block = rows_of(g_q, scat_q.rows(slot))
        scat_q.put(slot, dot(block, wq[...]))
        gw_q[...] += dot(block, feed_x.take(slot, ring), TN)
        gb_q[...] += row_sum(block.astype(F32))

    def put_y(first, last):
        def body(slot, carry):
            block = rows_of(g_kv, scat_y.rows(slot))
            scat_y.put(slot, dot(block, wkv[...]))
            gw_kv[...] += dot(block, feed_yy.take(slot, ring), TN)
            gb_kv[...] += row_sum(block.astype(F32))
            return carry
        lax.fori_loop(first, last, body, None)

    loop_slots(ring, hooks, put_q)
    scat_q.step(half - 1)
    put_y(0, 3)
    scat_y.step(0)

    def take_q(part, total):
        g_x1[part] = g_x2[part] + total

    scat_q.final(take_q)
    feed_h.copy(0).start()

    def x1_back(b, carry):
        gate_sum, bias_sum = carry
        rows = g_x1[b]
        block = (rows * mod[2, pl.ds(b, 1), :]).astype(BF16)
        g_attn[b] = block
        return gate_sum + row_sum(rows * atot[b]), bias_sum + row_sum(block.astype(F32))

    zero = jnp.zeros((1, width), F32)
    gate_sum, bias_sum = lax.fori_loop(0, batch, x1_back, (zero, zero))
    sums[2:3, :] = gate_sum
    sums[6:7, :] = bias_sum

    scat_q.finish()
    gather_a.start()

    def hooks(s):
        for g in gather_a.groups_before(s):
            gather_a.group(g)
        if s == 1:
            put_y(3, 5)
            scat_y.step(1)
        if s == 5:
            put_y(5, ring)
            scat_y.step(2)
        gather_a.ready(s)

    loop_slots(ring, hooks, out_back(gather_a, val, wo, gw_o))

    def hooks(b):
        if b == batch // 4:
            scat_y.step(half - 1)

    def self_back(b):
        parts = back_one(*[qkv[b, :, i * head_pad:(i + 1) * head_pad] for i in range(3)], prob[b], g_val[b])
        for i in range(3):
            g_qkv[b, :, i * head_pad:(i + 1) * head_pad] = parts[i]

    loop_slots(batch, hooks, self_back)

    def take_y(part, total):
        g_y[part] = total.astype(BF16)

    def hooks(s):
        if s >= 2 and s % 2 == 0:
            scat_h.step(s // 2 - 1)
        if s == 5:
            scat_y.final(take_y)

    def put_h(slot):
        block = rows_of(g_qkv, scat_h.rows(slot))
        scat_h.put(slot, dot(block, wqkv[...]))
        gw_qkv[...] += dot(block, feed_h.take(slot, ring), TN)
        gb_qkv[...] += row_sum(block.astype(F32))

    loop_slots(ring, hooks, put_h)
    scat_h.step(half - 1)
    def take_h(part, total):
        g_h1[part] = total

    scat_h.final(take_h)

    def x_back(b, carry):
        shift_sum, scale_sum = carry
        rows = x[b].astype(F32)
        centered = rows - jnp.mean(rows, axis=-1, keepdims=True)
        inv_std = lax.rsqrt(jnp.mean(centered * centered, axis=-1, keepdims=True) + LN_EPS)
        normed = centered * inv_std
        grad = g_h1[b]
        g_normed = grad * (1.0 + mod[1, pl.ds(b, 1), :])
        mean_g = jnp.mean(g_normed, axis=-1, keepdims=True)
        mean_gn = jnp.mean(g_normed * normed, axis=-1, keepdims=True)
        g_x[b] = (g_x1[b] + inv_std * (g_normed - mean_g - normed * mean_gn)).astype(BF16)
        return shift_sum + row_sum(grad), scale_sum + row_sum(grad * normed)

    shift_sum, scale_sum = lax.fori_loop(0, batch, x_back, (zero, zero))
    sums[0:1, :] = shift_sum
    sums[1:2, :] = scale_sum
    small_total(at, sums, got, mine, sums_out, sems[22:26])
    for stream in (gather_a, scat_y, scat_h):
        stream.finish()


def backward_call(tp_size, cid, head_dim, head_pad, ins, loads, feeds):
    batch, n_loc, width = ins[0].shape
    n_tok = n_loc * tp_size
    ring, half = tp_size // 2, tp_size // 4
    n_sum = ins[-1].shape[0]
    tokens = lambda last: (batch, n_tok, last)
    local = (batch, n_loc, width)
    vmem, anywhere = pl.BlockSpec(memory_space=pltpu.VMEM), pl.BlockSpec(memory_space=pl.ANY)
    sib, rcv, pbuf = (ring, *local), (2, half, *local), (ring, batch, 2 * n_loc, width)
    outs = [(local, BF16), (local, BF16), ((n_sum, width), F32)]
    outs += [((n * head_pad, width), F32) for n in (3, 2, 1, 1, 1)] + [((1, n * head_pad), F32) for n in (3, 2, 1)]
    return pl.pallas_call(
        functools.partial(backward_body, tp_size, head_dim),
        out_shape=[jax.ShapeDtypeStruct(*o) for o in outs],
        in_specs=[vmem] * len(ins) + [anywhere] * (len(loads) + len(feeds)),
        out_specs=[vmem] * len(outs),
        scratch_shapes=[pltpu.VMEM(a.shape, a.dtype) for a in loads]
        + [pltpu.VMEM(s, BF16) for s in (tokens(width), pbuf, sib, rcv, pbuf, sib, rcv)]
        + [pltpu.VMEM((n * head_pad, width), BF16) for n in (3, 2, 1, 1, 1)]
        + [pltpu.VMEM(tokens(n * head_pad), BF16) for n in (1, 3, 2, 1)]
        + [pltpu.VMEM(local, F32), pltpu.VMEM(local, F32), pltpu.VMEM(local, BF16), pltpu.VMEM((3, batch, width), F32), pltpu.VMEM((n_sum, width), F32),
           pltpu.VMEM((tp_size - 1, n_sum, LANES), F32), pltpu.VMEM((n_sum, LANES), F32)]
        + [pltpu.VMEM((2, batch, 2 * n_loc, width), BF16)] * 2
        + gather_sems(tp_size) * 2 + scatter_sems(tp_size) * 3
        + [pltpu.SemaphoreType.DMA((len(loads),)), pltpu.SemaphoreType.DMA((3, 2))]
        + [pltpu.SemaphoreType.DMA((n,)) for n in (width // LANES, tp_size - 1, tp_size - 1, width // LANES)],
        compiler_params=pltpu.CompilerParams(collective_id=cid, has_side_effects=True, vmem_limit_bytes=VMEM_LIMIT),
        name='attention_backward',
    )(*ins, *loads, *feeds)


def layer_norm(tensor):
    tensor = tensor.astype(F32)
    centered = tensor - jnp.mean(tensor, axis=-1, keepdims=True)
    inv_std = lax.rsqrt(jnp.mean(centered * centered, axis=-1, keepdims=True) + LN_EPS)
    return centered * inv_std, inv_std


def layer_norm_back(normed, inv_std, g_normed):
    mean_g = jnp.mean(g_normed, axis=-1, keepdims=True)
    mean_gn = jnp.mean(g_normed * normed, axis=-1, keepdims=True)
    return inv_std * (g_normed - mean_g - normed * mean_gn)


def drop_pad(grad, n_part, head_dim, head_pad):
    tail = grad.shape[1:]
    return grad.reshape(n_part, head_pad, *tail)[:, :head_dim].reshape(n_part * head_dim, *tail)


def rows_of(ref, rows):
    block = ref[:, rows, :]
    return block.reshape(block.shape[0] * block.shape[1], block.shape[2])


def put_rows(ref, rows, value):
    ref[:, rows, :] = value.astype(ref.dtype).reshape(ref.shape[0], rows.size, ref.shape[2])


def row_sum(value):
    return jnp.sum(value, axis=0, keepdims=True)


def gelu_pair(hidden):
    c0, c1 = 0.7978845608028654, 0.044715
    square = hidden * hidden
    tanh = jnp.tanh(c0 * hidden * (1.0 + c1 * square))
    half_up = 0.5 * (1.0 + tanh)
    slope = half_up + 0.5 * hidden * (1.0 - tanh * tanh) * (c0 * (1.0 + 3.0 * c1 * square))
    return hidden * half_up, slope


def token_sum(tensor):
    return jnp.sum(tensor.astype(F32), axis=(0, 1))


def device_block(tp_size, x_loc, y_loc, t_loc, len_loc, mod_table, w_qkv, b_qkv, w_o, b_o, w_q, b_q, w_kv, b_kv, w_co, b_co, w_1, b_1, w_2, b_2, g_loc):
    batch, n_loc, width = x_loc.shape
    n_tok = n_loc * tp_size
    head_dim, ffn = w_q.shape[2], w_1.shape[1]
    head_pad = -(-head_dim // LANES) * LANES
    mod_rows = mod_table[3:].astype(F32)[None] + t_loc[:, 3 * width:].astype(F32).reshape(batch, 3, width)
    shift2, scale2, gate2 = [mod_rows[:, i, None, :] for i in range(3)]

    wqkv, wq, wkv = [w.transpose(1, 2, 0)[0] for w in (w_qkv, w_q, w_kv)]
    wo, wco = w_o[0], w_co[0]

    def pad_bias(bias):
        bias = bias.astype(F32).reshape(-1, head_dim)
        return jnp.pad(bias, ((0, 0), (0, head_pad - head_dim))).reshape(1, -1)

    b1 = b_1.astype(F32)[None]
    lens = jnp.broadcast_to(len_loc[:, None, None], (batch, 1, n_tok))
    h1_all, y_all, x1_all, qkv, kv, q_cross, attn_val, cross_val, attn_prob, cross_prob, attn_total, x2_loc = forward_call(
        tp_size, 0, head_dim, head_pad, x_loc, y_loc, t_loc, mod_table, lens, wqkv, pad_bias(b_qkv), wkv, pad_bias(b_kv),
        wq, pad_bias(b_q), wo, b_o[None], wco, b_co[None])

    normed2, inv_std2 = layer_norm(x2_loc)
    h2_loc = (normed2 * (1.0 + scale2) + shift2).astype(BF16)
    g_x2 = g_loc.astype(F32)
    g_mlp_loc = (g_x2 * gate2).astype(BF16)

    def mlp(rows, get, ins, outs):
        w1, bias1, w2 = ins
        gelu_out, g_hid, acc_w1, acc_w2, acc_b1 = outs
        h2_blk, g_blk = get(0), get(1)
        hidden = dot(h2_blk, w1[...]) + bias1[...]
        act, slope = gelu_pair(hidden)
        act = act.astype(BF16)
        put_rows(gelu_out, rows, act)
        g_hidden = dot(g_blk, w2[...], NT) * slope
        acc_b1[...] += row_sum(g_hidden)
        g_hidden = g_hidden.astype(BF16)
        put_rows(g_hid, rows, g_hidden)
        acc_w1[...] += dot(g_hidden, h2_blk, TN)
        acc_w2[...] += dot(act, g_blk, TN)

    gelu_out, g_hid, g_w_1, g_w_2, g_b_1 = gather_call(
        tp_size, 1, 'gather_h2_g', [h2_loc, g_mlp_loc], [w_1, b1, w_2], (),
        [(batch, n_tok, ffn), (batch, n_tok, ffn)], [(ffn, width), (ffn, width), (1, ffn)], mlp)

    def mlp_out(rows, put, ins, held, accs):
        g_hid, act, w1, w2 = ins
        put(0, dot(rows_of(g_hid, rows), w1[...], NT))
        put(1, dot(rows_of(act, rows), w2[...]))

    both, = scatter_call(tp_size, 2, 'scatter_h2_out', n_loc, width, 2, [g_hid, gelu_out, w_1, w_2], [], [], mlp_out)
    g_h2, mlp_total = both[:batch], both[batch:] + b_2
    x_out = (x2_loc + gate2 * mlp_total).astype(BF16)
    g_gate2 = jnp.sum(g_x2 * mlp_total, axis=(0, 1))
    g_b_2 = token_sum(g_mlp_loc)
    g_shift2 = token_sum(g_h2)
    g_scale2 = token_sum(g_h2 * normed2)
    g_x2 = g_x2 + layer_norm_back(normed2, inv_std2, g_h2 * (1.0 + scale2))
    g_cross_loc = g_x2.astype(BF16)
    g_b_co = token_sum(g_cross_loc)

    zero = jnp.zeros_like(g_b_2)
    sums_in = jnp.stack([zero, zero, zero, g_shift2, g_scale2, g_gate2, zero, g_b_co, g_b_2] + [zero] * 7)
    g_x, g_y, sums, g_w_qkv, g_w_kv, g_w_q, g_w_o, g_w_co, g_b_qkv, g_b_kv, g_b_q = backward_call(
        tp_size, 3, head_dim, head_pad,
        [g_cross_loc, g_x2, x_loc, attn_total, t_loc, mod_table, wqkv, wkv, wq, wo, wco, sums_in],
        [qkv, kv, q_cross, attn_val, cross_val, attn_prob, cross_prob], [h1_all, x1_all, y_all])

    def head_weight(grad, n_part):
        return drop_pad(grad, n_part, head_dim, head_pad).astype(BF16)[None].transpose(2, 0, 1)

    def head_bias(grad, n_part):
        return drop_pad(grad[0], n_part, head_dim, head_pad)[None].astype(BF16)

    return (x_out, g_x, g_y, sums[:6],
            head_weight(g_w_qkv, 3), head_bias(g_b_qkv, 3), g_w_o[None, :head_dim].astype(BF16), sums[6].astype(BF16),
            head_weight(g_w_q, 1), head_bias(g_b_q, 1), head_weight(g_w_kv, 2), head_bias(g_b_kv, 2),
            g_w_co[None, :head_dim].astype(BF16), sums[7].astype(BF16),
            g_w_1.T.astype(BF16), g_b_1[0].astype(BF16), g_w_2.astype(BF16), sums[8].astype(BF16))


def solution(mesh):
    token_spec = P('dp', 'tp', None)
    group_rows = ('dp', 'tp')
    in_specs = (token_spec, token_spec, P('dp', None), P('dp'), P(None, None), P(None, 'tp', None), P('tp', None), P('tp', None, None), P(None), P(None, 'tp', None), P('tp', None), P(None, 'tp', None), P('tp', None), P('tp', None, None), P(None), P(None, 'tp'), P('tp'), P('tp', None), P(None), token_spec)
    out_specs = (token_spec, token_spec, token_spec, P('dp', None), P('dp', 'tp', None), P(group_rows, None), P(group_rows, None, None), P('dp'), P('dp', 'tp', None), P(group_rows, None), P('dp', 'tp', None), P(group_rows, None), P(group_rows, None, None), P('dp'), P('dp', 'tp'), P(group_rows), P(group_rows, None), P('dp'))
    return jax.shard_map(functools.partial(device_block, mesh.shape['tp']), mesh=mesh, in_specs=in_specs, out_specs=out_specs, check_vma=False)
```

```python
import functools
import itertools

import jax
import jax.numpy as jnp
from jax import lax
from jax.experimental import pallas as pl
from jax.experimental.pallas import tpu as pltpu
from jax.sharding import PartitionSpec as P

LN_EPS = 1e-6
MASK_FILL = -1e30
LANES = 128
MESH = pl.DeviceIdType.MESH
BF16 = jnp.bfloat16
F32 = jnp.float32
NN = (((1,), (0,)), ((), ()))
NT = (((1,), (1,)), ((), ()))
TN = (((0,), (0,)), ((), ()))
SHIFT1, SCALE1, GATE1, SHIFT2, SCALE2, GATE2, B_O, B_CO, B_2 = range(9)
SUM_ROWS = 16
FORWARD_BIASES = 'qkv', 'kv', 'q', 'o', 'co'
UP, DOWN = HALVES = WAYS = 0, 1
SEND, TAKE = True, False
KERNEL = functools.partial(pltpu.CompilerParams, has_side_effects=True, vmem_limit_bytes=67 * 1000 * 1000)
VMEM, ANY = pl.BlockSpec(memory_space=pltpu.VMEM), pl.BlockSpec(memory_space=pl.ANY)


def dot(lhs, rhs, dims=NN):
    return lax.dot_general(lhs, rhs, dims, preferred_element_type=F32)


def cutter(refs):
    left = iter(refs)
    return lambda n: list(itertools.islice(left, n))


def biases_of(packed, names, width, head_dim):
    return [packed[:, at:at + size] for at, size in (bias_place(name, width, head_dim, packed.shape[1]) for name in names)]


def bias_place(name, width, head_dim, total):
    head_pad = -(-head_dim // LANES) * LANES
    sizes = {'qkv': 3 * head_pad, 'kv': 2 * head_pad, 'q': head_pad, 'o': width, 'co': width, '2': width}
    sizes['1'] = total - sum(sizes.values())
    names = list(sizes)
    return sum(sizes[n] for n in names[:names.index(name)]), sizes[name]


class Place:
    def __init__(self, tp_size):
        self.tp_size = tp_size
        self.me = lax.axis_index('tp')
        self.ring, self.chip, self.core = tp_size // 2, self.me // 2, lax.rem(self.me, 2)
        self.half = self.ring // 2

    def wrap(self, zz):
        return lax.rem(zz + self.ring, self.ring)

    def sibling(self):
        return {'tp': self.chip * 2 + 1 - self.core}

    def ahead(self, sign):
        return {'tp': self.wrap(self.chip + sign) * 2 + self.core}

    def other(self, d):
        return {'tp': lax.rem(self.me + d, self.tp_size)}

    def greet(self, peers):
        barrier = pltpu.get_barrier_semaphore()
        for peer in peers:
            pl.semaphore_signal(barrier, device_id=peer, device_id_type=MESH)
        pl.semaphore_wait(barrier, len(peers))

    def greet_all(self):
        self.greet([self.other(d) for d in range(1, self.tp_size)])

    def greet_near(self):
        self.greet([self.ahead(1), self.ahead(-1), self.sibling()])


class Gather:
    def __init__(self, at, own, full, sems):
        self.at, self.own_ref, self.full = at, own, full
        self.rsend, self.rrecv, self.ssend, self.srecv = sems
        self.batch, self.n_loc = own.shape[0], own.shape[1]
        self.hb = self.batch // 2

    def part(self, zz, cc, ch):
        row = pl.multiple_of((zz * 2 + cc) * self.n_loc, self.n_loc)
        return self.full.at[pl.ds(ch * self.hb, self.hb), pl.ds(row, self.n_loc), :]

    def own(self, ch):
        return self.own_ref.at[pl.ds(ch * self.hb, self.hb)]

    def ring_copy(self, way, k, ch, sending):
        at = self.at
        sign = -1 if way == UP else 1
        zb = at.wrap(at.chip + sign * (k - 1 if sending else k))
        src = self.own(ch) if (sending and k == 1) else self.part(zb, at.core, ch)
        return pltpu.make_async_remote_copy(
            src_ref=src, dst_ref=self.part(zb, at.core, ch),
            send_sem=self.rsend.at[way, k - 1, ch], recv_sem=self.rrecv.at[way, k - 1, ch],
            device_id=at.ahead(-sign), device_id_type=MESH)

    def chip_at(self, slot):
        k = (slot + 1) // 2
        return self.at.wrap(self.at.chip - k) if slot % 2 else self.at.wrap(self.at.chip + k)

    def sib_copy(self, slot, ch, sending):
        at = self.at
        cc = at.core if sending else 1 - at.core
        zb = self.chip_at(slot)
        src = self.own(ch) if (sending and slot == 0) else self.part(zb, cc, ch)
        return pltpu.make_async_remote_copy(
            src_ref=src, dst_ref=self.part(zb, cc, ch),
            send_sem=self.ssend.at[slot, ch], recv_sem=self.srecv.at[slot, ch],
            device_id=at.sibling(), device_id_type=MESH)

    def carries(self, way, k, ch):
        return k < self.at.half or (k == self.at.half and ch == way)

    def slot_of(self, way, k):
        half = self.at.half
        return 2 * half - 1 if k == half else (2 * k - 1 if way == UP else 2 * k)

    def start(self):
        for way, ch in ((UP, 0), (DOWN, 1), (UP, 1), (DOWN, 0)):
            self.ring_copy(way, 1, ch, SEND).start()
        for ch in HALVES:
            self.sib_copy(0, ch, SEND).start()
        row = pl.multiple_of(self.at.me * self.n_loc, self.n_loc)
        self.full[:, pl.ds(row, self.n_loc), :] = self.own_ref[...]

    def arrive(self, way, k, ch):
        self.ring_copy(way, k, ch, TAKE).wait_recv()
        if self.carries(way, k + 1, ch):
            self.ring_copy(way, k + 1, ch, SEND).start()
        self.sib_copy(self.slot_of(way, k), ch, SEND).start()

    def group(self, g):
        k = g // 2 + 1
        first, second = ((UP, 0), (DOWN, 1)) if g % 2 == 0 else ((UP, 1), (DOWN, 0))
        self.arrive(first[0], k, first[1])
        self.arrive(second[0], k, second[1])

    def groups_before(self, slot):
        last = self.at.ring - 1
        return () if slot == last - 1 else ((last - 1,) if slot == last else (slot,))

    def ready(self, slot):
        for ch in HALVES:
            self.sib_copy(slot, ch, TAKE).wait_recv()

    def rows(self, slot):
        k = (slot + 1) // 2
        zz = self.at.wrap(self.at.chip + (1 - 2 * lax.rem(slot, 2)) * k)
        return pl.ds(pl.multiple_of(zz * 2 * self.n_loc, 2 * self.n_loc), 2 * self.n_loc)

    def save_copy(self, dest, sem, slot):
        rows = self.rows(slot)
        return pltpu.make_async_copy(self.full.at[:, rows, :], dest.at[:, rows, :], sem.at[slot])

    def finish(self):
        for way in WAYS:
            for k in range(1, self.at.half + 1):
                for ch in HALVES:
                    if self.carries(way, k, ch):
                        self.ring_copy(way, k, ch, SEND).wait_send()
        for slot in range(self.at.ring):
            for ch in HALVES:
                self.sib_copy(slot, ch, SEND).wait_send()


class Scatter:
    def __init__(self, at, pbuf, sibr, rcv, sems):
        self.at, self.pbuf, self.sibr, self.rcv = at, pbuf, sibr, rcv
        self.rsend, self.rrecv, self.ssend, self.srecv = sems
        self.batch, self.n_loc = sibr.shape[1], sibr.shape[2]
        self.hb = self.batch // 2

    def slot_of(self, way, s):
        return 0 if s == 0 else (2 * s - 1 if way == UP else 2 * s)

    def rows(self, slot):
        at = self.at
        away = at.half - (slot + 1) // 2
        zz = at.wrap(at.chip + (2 * lax.rem(slot, 2) - 1) * away)
        return pl.ds(pl.multiple_of(zz * 2 * self.n_loc, 2 * self.n_loc), 2 * self.n_loc)

    def put(self, slot, value):
        self.pbuf[slot] = value.astype(BF16).reshape(self.batch, 2 * self.n_loc, value.shape[-1])
        self.sib_copy(slot).start()

    def ring_copy(self, way, s, ch):
        part = pl.ds(ch * self.hb, self.hb)
        return pltpu.make_async_remote_copy(
            src_ref=self.sibr.at[self.slot_of(way, s), part], dst_ref=self.rcv.at[way, s, part],
            send_sem=self.rsend.at[way, s, ch], recv_sem=self.rrecv.at[way, s, ch],
            device_id=self.at.ahead(1 if way == UP else -1), device_id_type=MESH)

    def sib_copy(self, slot):
        rows = pl.ds(pl.multiple_of((1 - self.at.core) * self.n_loc, self.n_loc), self.n_loc)
        return pltpu.make_async_remote_copy(
            src_ref=self.pbuf.at[slot, :, rows, :], dst_ref=self.sibr.at[slot],
            send_sem=self.ssend.at[slot], recv_sem=self.srecv.at[slot],
            device_id=self.at.sibling(), device_id_type=MESH)

    def own_sum(self, slot, part):
        rows = pl.ds(pl.multiple_of(self.at.core * self.n_loc, self.n_loc), self.n_loc)
        return self.pbuf[slot, part, rows, :].astype(F32) + self.sibr[slot, part].astype(F32)

    def starts_at(self, way, ch):
        return 0 if ch == way else 1

    def pass_on(self, way, s, ch):
        slot, part = self.slot_of(way, s), pl.ds(ch * self.hb, self.hb)
        total = self.own_sum(slot, part)
        if s > self.starts_at(way, ch):
            self.ring_copy(way, s - 1, ch).wait_recv()
            total = total + self.rcv[way, s - 1, part].astype(F32)
        self.sibr[slot, part] = total.astype(BF16)
        self.ring_copy(way, s, ch).start()

    def step(self, s):
        if s == 0:
            self.sib_copy(0).wait_recv()
            self.pass_on(UP, 0, 0)
            self.pass_on(DOWN, 0, 1)
            return
        self.sib_copy(2 * s - 1).wait_recv()
        self.pass_on(UP, s, 1)
        self.sib_copy(2 * s).wait_recv()
        self.pass_on(DOWN, s, 0)
        self.pass_on(UP, s, 0)
        self.pass_on(DOWN, s, 1)

    def final(self, use):
        last = self.at.ring - 1
        self.sib_copy(last).wait_recv()
        for ch, order in ((1, (UP, DOWN)), (0, (DOWN, UP))):
            part = pl.ds(ch * self.hb, self.hb)
            total = self.own_sum(last, part)
            for way in order:
                self.ring_copy(way, self.at.half - 1, ch).wait_recv()
                total = total + self.rcv[way, self.at.half - 1, part].astype(F32)
            use(part, total)

    def finish(self):
        for way in WAYS:
            for s in range(self.at.half):
                for ch in HALVES:
                    if s >= self.starts_at(way, ch):
                        self.ring_copy(way, s, ch).wait_send()
        for slot in range(self.at.ring):
            self.sib_copy(slot).wait_send()


def loop_slots(n, hooks, body):
    def step(slot, carry):
        for s in range(n):
            @pl.when(slot == s)
            def _():
                hooks(s)
        body(slot)
        return carry
    lax.fori_loop(0, n, step, None)


def gather_sems(tp_size):
    ring, half = tp_size // 2, tp_size // 4
    return [pltpu.SemaphoreType.DMA(s) for s in ((2, half, 2), (2, half, 2), (ring, 2), (ring, 2))]


def scatter_sems(tp_size):
    ring, half = tp_size // 2, tp_size // 4
    return [pltpu.SemaphoreType.DMA(s) for s in ((2, half, 2), (2, half, 2), (ring,), (ring,))]


def pad_rows(dest, source, head_dim):
    parts = source.shape[0] // head_dim
    head_pad = dest.shape[0] // parts
    width = dest.shape[1]
    for i in range(parts):
        dest[i * head_pad:i * head_pad + head_dim, :] = source[i * head_dim:(i + 1) * head_dim, :]
        dest[i * head_pad + head_dim:(i + 1) * head_pad, :] = jnp.zeros((head_pad - head_dim, width), dest.dtype)


def mod_row(t_ref, table_ref, i):
    width = table_ref.shape[1]
    return table_ref[i:i + 1, :].astype(F32) + t_ref[:, i * width:(i + 1) * width].astype(F32)


def rows_of(ref, rows):
    block = ref[:, rows, :]
    return block.reshape(block.shape[0] * block.shape[1], block.shape[2])


def put_rows(ref, rows, value):
    ref[:, rows, :] = value.astype(ref.dtype).reshape(ref.shape[0], rows.size, ref.shape[2])


def row_sum(value):
    return jnp.sum(value, axis=0, keepdims=True)


def gelu_pair(hidden):
    c0, c1 = 0.7978845608028654, 0.044715
    square = hidden * hidden
    tanh = jnp.tanh(c0 * hidden * (1.0 + c1 * square))
    half_up = 0.5 * (1.0 + tanh)
    slope = half_up + 0.5 * hidden * (1.0 - tanh * tanh) * (c0 * (1.0 + 3.0 * c1 * square))
    return hidden * half_up, slope


def normalize(rows):
    rows = rows.astype(F32)
    centered = rows - jnp.mean(rows, axis=-1, keepdims=True)
    inv_std = lax.rsqrt(jnp.mean(centered * centered, axis=-1, keepdims=True) + LN_EPS)
    return centered * inv_std, inv_std


def normalize_back(normed, inv_std, g_normed):
    mean_g = jnp.mean(g_normed, axis=-1, keepdims=True)
    mean_gn = jnp.mean(g_normed * normed, axis=-1, keepdims=True)
    return inv_std * (g_normed - mean_g - normed * mean_gn)


def softmax_of(scores):
    top = jnp.max(scores, axis=-1, keepdims=True)
    powers = jnp.exp(scores - top)
    return powers * (1.0 / jnp.sum(powers, axis=-1, keepdims=True))


def forward_body(tp_size, head_dim, *refs):
    at = Place(tp_size)
    take = cutter(refs)
    x, y, t_emb, table, lens, biases, wqkv_in, wkv_in, wq_in, wo_in, wco_in = take(11)
    bqkv, bkv, bq, bo, bco = biases_of(biases, FORWARD_BIASES, wqkv_in.shape[1], head_dim)
    h1_out, y_out, x1_out = take(3)
    outs, scratch = take(9), take(9)
    qkv, kv, q_c, val, cval, prob, cprob, atot, x2 = scratch
    h1, x1, mod, fh, fy, fx, pbuf, sibr1, rcv1, sibr2, rcv2, wqkv, wkv, wq, wo, wco = take(16)
    gather_h, gather_y, gather_x = [Gather(at, own, full, take(4)) for own, full in ((h1, fh), (y, fy), (x1, fx))]
    scat_o, scat_c = [Scatter(at, pbuf, sibr, rcv, take(4)) for sibr, rcv in ((sibr1, rcv1), (sibr2, rcv2))]
    saves, out_sem = take(3), refs[-1]
    batch = x.shape[0]
    head_pad = wq.shape[0]
    scale = head_dim ** -0.5

    def out_copy(i):
        return pltpu.make_async_copy(scratch[i], outs[i], out_sem.at[i])

    for i in range(3):
        mod[i] = mod_row(t_emb, table, i)

    def norm_one(b, carry):
        normed, _ = normalize(x[b])
        h1[b] = (normed * (1.0 + mod[1, pl.ds(b, 1), :]) + mod[0, pl.ds(b, 1), :]).astype(BF16)
        return carry

    lax.fori_loop(0, batch, norm_one, None)
    at.greet_near()
    gather_h.start()
    for dest, source in ((wqkv, wqkv_in), (wkv, wkv_in), (wq, wq_in), (wo, wo_in), (wco, wco_in)):
        pad_rows(dest, source, head_dim)

    def hooks(s):
        for g in gather_h.groups_before(s):
            gather_h.group(g)
        gather_h.ready(s)
        if s == at.ring - 4:
            gather_y.start()

    def project(slot):
        rows = gather_h.rows(slot)
        gather_h.save_copy(h1_out, saves[0], slot).start()
        put_rows(qkv, rows, dot(rows_of(fh, rows), wqkv[...], NT) + bqkv)

    loop_slots(at.ring, hooks, project)

    def hooks(b):
        if b == batch // 2:
            gather_y.group(0)
        if b == batch - 1:
            gather_y.group(1)

    def attend_self(b):
        q_b, k_b, v_b = [qkv[b, :, i * head_pad:(i + 1) * head_pad] for i in range(3)]
        p_b = softmax_of(dot(q_b, k_b, NT) * scale).astype(BF16)
        prob[b] = p_b
        val[b] = dot(p_b, v_b).astype(BF16)

    loop_slots(batch, hooks, attend_self)
    for i in (0, 3, 5):
        out_copy(i).start()

    ynext = {2: 2, 3: 3, 5: 4, 6: 5, 7: 6}

    def hooks(s):
        if s >= 2 and s % 2 == 0:
            scat_o.step(s // 2 - 1)
        if s in ynext:
            gather_y.group(ynext[s])

    def project_o(slot):
        scat_o.put(slot, dot(rows_of(val, scat_o.rows(slot)), wo[...]))

    loop_slots(at.ring, hooks, project_o)
    scat_o.step(at.half - 1)

    def take_o(part, total):
        atot[part] = total + bo

    scat_o.final(take_o)
    out_copy(7).start()

    def x1_one(b, carry):
        x1[b] = (x[b].astype(F32) + mod[2, pl.ds(b, 1), :] * atot[b]).astype(BF16)
        return carry

    lax.fori_loop(0, batch, x1_one, None)

    gather_x.start()

    def hooks(s):
        for g in gather_x.groups_before(s):
            gather_x.group(g)
        gather_y.ready(s)
        gather_x.ready(s)

    def project(slot):
        rows = gather_x.rows(slot)
        gather_y.save_copy(y_out, saves[1], slot).start()
        gather_x.save_copy(x1_out, saves[2], slot).start()
        put_rows(kv, rows, dot(rows_of(fy, rows), wkv[...], NT) + bkv)
        put_rows(q_c, rows, dot(rows_of(fx, rows), wq[...], NT) + bq)

    loop_slots(at.ring, hooks, project)
    scat_o.finish()

    def attend_cross(b, carry):
        k_b, v_b = [kv[b, :, i * head_pad:(i + 1) * head_pad] for i in range(2)]
        scores = dot(q_c[b], k_b, NT) * scale
        slots = lax.broadcasted_iota(jnp.int32, scores.shape, 1)
        p_b = softmax_of(jnp.where(slots < lens[b], scores, MASK_FILL)).astype(BF16)
        cprob[b] = p_b
        cval[b] = dot(p_b, v_b).astype(BF16)
        return carry

    lax.fori_loop(0, batch, attend_cross, None)
    for i in (1, 2, 4, 6):
        out_copy(i).start()

    def hooks(s):
        if s >= 2 and s % 2 == 0:
            scat_c.step(s // 2 - 1)

    def project_c(slot):
        scat_c.put(slot, dot(rows_of(cval, scat_c.rows(slot)), wco[...]))

    loop_slots(at.ring, hooks, project_c)
    scat_c.step(at.half - 1)

    def take_c(part, total):
        x2[part] = (x1[part].astype(F32) + total + bco).astype(BF16)

    scat_c.final(take_c)
    out_copy(8).start()
    for stream in (gather_h, gather_y, gather_x, scat_c):
        stream.finish()
    for slot in range(at.ring):
        gather_h.save_copy(h1_out, saves[0], slot).wait()
        gather_y.save_copy(y_out, saves[1], slot).wait()
        gather_x.save_copy(x1_out, saves[2], slot).wait()
    for i in range(9):
        out_copy(i).wait()


def forward_call(tp_size, cid, head_dim, head_pad, *ins):
    batch, n_loc, width = ins[0].shape
    n_tok = n_loc * tp_size
    ring, half = tp_size // 2, tp_size // 4
    tokens = lambda last: (batch, n_tok, last)
    local = (batch, n_loc, width)
    kept = [(tokens(3 * head_pad), BF16), (tokens(2 * head_pad), BF16), (tokens(head_pad), BF16), (tokens(head_pad), BF16),
            (tokens(head_pad), BF16), (tokens(n_tok), BF16), (tokens(n_tok), BF16), (local, F32), (local, BF16)]
    sib, rcv = (ring, *local), (2, half, *local)
    return pl.pallas_call(
        functools.partial(forward_body, tp_size, head_dim),
        out_shape=[jax.ShapeDtypeStruct(tokens(width), BF16)] * 3 + [jax.ShapeDtypeStruct(*k) for k in kept],
        in_specs=[VMEM] * 4 + [pl.BlockSpec(memory_space=pltpu.SMEM)] + [VMEM] * (len(ins) - 5),
        out_specs=[ANY] * (3 + len(kept)),
        scratch_shapes=[pltpu.VMEM(*k) for k in kept] + [
            pltpu.VMEM(local, BF16), pltpu.VMEM(local, BF16), pltpu.VMEM((3, batch, width), F32),
            pltpu.VMEM(tokens(width), BF16), pltpu.VMEM(tokens(width), BF16), pltpu.VMEM(tokens(width), BF16),
            pltpu.VMEM((ring, batch, 2 * n_loc, width), BF16),
            pltpu.VMEM(sib, BF16), pltpu.VMEM(rcv, BF16), pltpu.VMEM(sib, BF16), pltpu.VMEM(rcv, BF16)]
        + [pltpu.VMEM((n * head_pad, width), BF16) for n in (3, 2, 1, 1, 1)]
        + gather_sems(tp_size) * 3 + scatter_sems(tp_size) * 2
        + [pltpu.SemaphoreType.DMA((ring,))] * 3 + [pltpu.SemaphoreType.DMA((len(kept),))],
        compiler_params=KERNEL(collective_id=cid),
        name='attention_forward',
    )(*ins)


class RowFeed:
    def __init__(self, source, buf, sem, rows):
        self.source, self.buf, self.sem, self.rows = source, buf, sem, rows

    def copy(self, slot):
        side = lax.rem(slot, 2)
        return pltpu.make_async_copy(self.source.at[:, self.rows(slot), :], self.buf.at[side], self.sem.at[side])

    def take(self, slot, n):
        @pl.when(slot + 1 < n)
        def _():
            self.copy(slot + 1).start()
        self.copy(slot).wait()
        block = self.buf[lax.rem(slot, 2)]
        return block.reshape(block.shape[0] * block.shape[1], block.shape[2])


def small_total(at, src, got, mine, out, sems):
    send1, recv1, send2, recv2 = sems
    tiles = src.shape[1] // LANES

    def lanes(i):
        return pl.ds(i * LANES, LANES)

    def first(tile, peer_slot):
        return pltpu.make_async_remote_copy(
            src_ref=src.at[:, lanes(tile)], dst_ref=got.at[peer_slot], send_sem=send1.at[tile], recv_sem=recv1.at[peer_slot],
            device_id={'tp': tile}, device_id_type=MESH)

    def second(tile, d):
        return pltpu.make_async_remote_copy(
            src_ref=mine, dst_ref=out.at[:, lanes(tile)], send_sem=send2.at[d - 1], recv_sem=recv2.at[tile],
            device_id=at.other(d), device_id_type=MESH)

    for tile in range(tiles):
        @pl.when(at.me != tile)
        def _():
            first(tile, lax.rem(at.me - tile + at.tp_size, at.tp_size) - 1).start()
    for tile in range(tiles):
        @pl.when(at.me == tile)
        def _():
            total = src[:, tile * LANES:(tile + 1) * LANES]
            for d in range(1, at.tp_size):
                first(tile, d - 1).wait_recv()
                total = total + got[d - 1]
            mine[...] = total
            for d in range(1, at.tp_size):
                second(tile, d).start()
            out[:, tile * LANES:(tile + 1) * LANES] = total
            for d in range(1, at.tp_size):
                second(tile, d).wait_send()
    for tile in range(tiles):
        @pl.when(at.me != tile)
        def _():
            second(tile, 1).wait_recv()
            first(tile, 0).wait_send()


def backward_body(tp_size, head_dim, *refs):
    at = Place(tp_size)
    take = cutter(refs)
    g_cross, g_x2, x, atot, t_emb, table, wqkv_in, wkv_in, wq_in, wo_in, wco_in, sums_in = take(12)
    loads, feeds = take(7), take(3)
    g_x, g_y, sums_out = take(3)
    accs = take(8)
    gw_qkv, gw_kv, gw_q, gw_o, gw_co, gb_qkv, gb_kv, gb_q = accs
    held = take(7)
    qkv, kv, q_c, val, cval, prob, cprob = held
    full, pbuf, sibr1, rcv1, pbufy, sibr2, rcv2, wqkv, wkv, wq, wo, wco = take(12)
    g_val, g_qkv, g_kv, g_q, g_x1, g_h1, g_attn, mod, sums, got, mine, feed_a, feed_y = take(13)
    gather_c, gather_a = [Gather(at, own, full, take(4)) for own in (g_cross, g_attn)]
    near, far = (pbuf, sibr1, rcv1), (pbufy, sibr2, rcv2)
    scat_q, scat_y, scat_h = [Scatter(at, *bufs, take(4)) for bufs in (near, far, near)]
    load_sem, *feed_sems = take(4)
    feed_h, feed_x, feed_yy = [
        RowFeed(source, buf, sem, scat.rows)
        for source, buf, sem, scat in zip(feeds, (feed_a, feed_a, feed_y), feed_sems, (scat_h, scat_q, scat_y))]
    batch, n_loc, width = x.shape
    ring, half = at.ring, at.half
    head_pad = wq.shape[0]
    scale = head_dim ** -0.5

    def load_copy(i):
        return pltpu.make_async_copy(loads[i], held[i], load_sem.at[i])

    for i in range(len(held)):
        load_copy(i).start()
    at.greet_all()
    gather_c.start()
    feed_x.copy(0).start()
    feed_yy.copy(0).start()
    for i in range(3):
        mod[i] = mod_row(t_emb, table, i)
    for dest, source in ((wqkv, wqkv_in), (wkv, wkv_in), (wq, wq_in), (wo, wo_in), (wco, wco_in)):
        pad_rows(dest, source, head_dim)
    sums[...] = sums_in[...]
    for acc in accs:
        acc[...] = jnp.zeros_like(acc)
    for i in range(len(held)):
        load_copy(i).wait()

    def out_back(gather, value, weight, acc):
        def body(slot):
            rows = gather.rows(slot)
            block = rows_of(full, rows)
            put_rows(g_val, rows, dot(block, weight[...], NT))
            acc[...] += dot(rows_of(value, rows), block, TN)
        return body

    def hooks(s):
        for g in gather_c.groups_before(s):
            gather_c.group(g)
        gather_c.ready(s)

    loop_slots(ring, hooks, out_back(gather_c, cval, wco, gw_co))
    gather_c.finish()

    def back_one(q_b, k_b, v_b, p_b, g_b):
        g_p = dot(g_b, v_b, NT)
        p_f = p_b.astype(F32)
        row_dot = jnp.sum(g_p * p_f, axis=-1, keepdims=True)
        g_s = (p_f * (g_p - row_dot) * scale).astype(BF16)
        return dot(g_s, k_b).astype(BF16), dot(g_s, q_b, TN).astype(BF16), dot(p_b, g_b, TN).astype(BF16)

    def cross_back(b, carry):
        parts = back_one(q_c[b], kv[b, :, :head_pad], kv[b, :, head_pad:], cprob[b], g_val[b])
        g_q[b] = parts[0]
        g_kv[b, :, :head_pad] = parts[1]
        g_kv[b, :, head_pad:] = parts[2]
        return carry

    lax.fori_loop(0, batch, cross_back, None)

    def hooks(s):
        if s >= 2 and s % 2 == 0:
            scat_q.step(s // 2 - 1)

    def put_q(slot):
        block = rows_of(g_q, scat_q.rows(slot))
        scat_q.put(slot, dot(block, wq[...]))
        gw_q[...] += dot(block, feed_x.take(slot, ring), TN)
        gb_q[...] += row_sum(block.astype(F32))

    def put_y(first, last):
        def body(slot, carry):
            block = rows_of(g_kv, scat_y.rows(slot))
            scat_y.put(slot, dot(block, wkv[...]))
            gw_kv[...] += dot(block, feed_yy.take(slot, ring), TN)
            gb_kv[...] += row_sum(block.astype(F32))
            return carry
        lax.fori_loop(first, last, body, None)

    loop_slots(ring, hooks, put_q)
    scat_q.step(half - 1)
    put_y(0, 3)
    scat_y.step(0)

    def take_q(part, total):
        g_x1[part] = g_x2[part] + total

    scat_q.final(take_q)
    feed_h.copy(0).start()

    def x1_back(b, carry):
        gate_sum, bias_sum = carry
        rows = g_x1[b]
        block = (rows * mod[2, pl.ds(b, 1), :]).astype(BF16)
        g_attn[b] = block
        return gate_sum + row_sum(rows * atot[b]), bias_sum + row_sum(block.astype(F32))

    zero = jnp.zeros((1, width), F32)
    gate_sum, bias_sum = lax.fori_loop(0, batch, x1_back, (zero, zero))
    for row, value in ((GATE1, gate_sum), (B_O, bias_sum)):
        sums[row:row + 1, :] = value

    scat_q.finish()
    gather_a.start()

    def hooks(s):
        for g in gather_a.groups_before(s):
            gather_a.group(g)
        if s == 1:
            put_y(3, 5)
            scat_y.step(1)
        if s == 5:
            put_y(5, ring)
            scat_y.step(2)
        gather_a.ready(s)

    loop_slots(ring, hooks, out_back(gather_a, val, wo, gw_o))

    def hooks(b):
        if b == batch // 4:
            scat_y.step(half - 1)

    def self_back(b):
        parts = back_one(*[qkv[b, :, i * head_pad:(i + 1) * head_pad] for i in range(3)], prob[b], g_val[b])
        for i in range(3):
            g_qkv[b, :, i * head_pad:(i + 1) * head_pad] = parts[i]

    loop_slots(batch, hooks, self_back)

    def take_y(part, total):
        g_y[part] = total.astype(BF16)

    def hooks(s):
        if s >= 2 and s % 2 == 0:
            scat_h.step(s // 2 - 1)
        if s == 5:
            scat_y.final(take_y)

    def put_h(slot):
        block = rows_of(g_qkv, scat_h.rows(slot))
        scat_h.put(slot, dot(block, wqkv[...]))
        gw_qkv[...] += dot(block, feed_h.take(slot, ring), TN)
        gb_qkv[...] += row_sum(block.astype(F32))

    loop_slots(ring, hooks, put_h)
    scat_h.step(half - 1)
    def take_h(part, total):
        g_h1[part] = total

    scat_h.final(take_h)

    def x_back(b, carry):
        shift_sum, scale_sum = carry
        normed, inv_std = normalize(x[b])
        grad = g_h1[b]
        back = normalize_back(normed, inv_std, grad * (1.0 + mod[1, pl.ds(b, 1), :]))
        g_x[b] = (g_x1[b] + back).astype(BF16)
        return shift_sum + row_sum(grad), scale_sum + row_sum(grad * normed)

    shift_sum, scale_sum = lax.fori_loop(0, batch, x_back, (zero, zero))
    for row, value in ((SHIFT1, shift_sum), (SCALE1, scale_sum)):
        sums[row:row + 1, :] = value
    small_total(at, sums, got, mine, sums_out, take(4))
    for stream in (gather_a, scat_y, scat_h):
        stream.finish()


def backward_call(tp_size, cid, head_dim, head_pad, ins, loads, feeds):
    batch, n_loc, width = ins[0].shape
    n_tok = n_loc * tp_size
    ring, half = tp_size // 2, tp_size // 4
    n_sum = ins[-1].shape[0]
    tokens = lambda last: (batch, n_tok, last)
    local = (batch, n_loc, width)
    sib, rcv, pbuf = (ring, *local), (2, half, *local), (ring, batch, 2 * n_loc, width)
    outs = [(local, BF16), (local, BF16), ((n_sum, width), F32)]
    outs += [((n * head_pad, width), F32) for n in (3, 2, 1, 1, 1)] + [((1, n * head_pad), F32) for n in (3, 2, 1)]
    return pl.pallas_call(
        functools.partial(backward_body, tp_size, head_dim),
        out_shape=[jax.ShapeDtypeStruct(*o) for o in outs],
        in_specs=[VMEM] * len(ins) + [ANY] * (len(loads) + len(feeds)),
        out_specs=[VMEM] * len(outs),
        scratch_shapes=[pltpu.VMEM(a.shape, a.dtype) for a in loads]
        + [pltpu.VMEM(s, BF16) for s in (tokens(width), pbuf, sib, rcv, pbuf, sib, rcv)]
        + [pltpu.VMEM((n * head_pad, width), BF16) for n in (3, 2, 1, 1, 1)]
        + [pltpu.VMEM(tokens(n * head_pad), BF16) for n in (1, 3, 2, 1)]
        + [pltpu.VMEM(local, F32), pltpu.VMEM(local, F32), pltpu.VMEM(local, BF16), pltpu.VMEM((3, batch, width), F32), pltpu.VMEM((n_sum, width), F32),
           pltpu.VMEM((tp_size - 1, n_sum, LANES), F32), pltpu.VMEM((n_sum, LANES), F32)]
        + [pltpu.VMEM((2, batch, 2 * n_loc, width), BF16)] * 2
        + gather_sems(tp_size) * 2 + scatter_sems(tp_size) * 3
        + [pltpu.SemaphoreType.DMA((len(loads),))] + [pltpu.SemaphoreType.DMA((2,))] * 3
        + [pltpu.SemaphoreType.DMA((n,)) for n in (width // LANES, tp_size - 1, tp_size - 1, width // LANES)],
        compiler_params=KERNEL(collective_id=cid),
        name='attention_backward',
    )(*ins, *loads, *feeds)


def mlp_body(tp_size, head_dim, *refs):
    at = Place(tp_size)
    take = cutter(refs)
    x2, g, t_emb, table, biases, w1, w2 = take(7)
    b1, b2 = biases_of(biases, ('1', '2'), x2.shape[-1], head_dim)
    x_out, g_x2, g_cross, sums, gw_1, gw_2, gb_1 = take(7)
    h2, gm, mod, fh, fg, act_all, hid_all, g_h2, total = take(9)
    ring_bufs = take(3), take(3)
    gather_h, gather_g = [Gather(at, own, full, take(4)) for own, full in ((h2, fh), (gm, fg))]
    scat_h, scat_m = [Scatter(at, *bufs, take(4)) for bufs in ring_bufs]
    batch = x2.shape[0]

    for i in range(3):
        mod[i] = mod_row(t_emb, table, 3 + i)

    def shift_scale_gate(b):
        return [mod[i, pl.ds(b, 1), :] for i in range(3)]

    def norm_one(b, carry):
        shift, scale, gate = shift_scale_gate(b)
        normed, _ = normalize(x2[b])
        h2[b] = (normed * (1.0 + scale) + shift).astype(BF16)
        gm[b] = (g[b].astype(F32) * gate).astype(BF16)
        return carry

    lax.fori_loop(0, batch, norm_one, None)
    at.greet_near()
    gather_h.start()
    gather_g.start()
    for acc in (gw_1, gw_2, gb_1):
        acc[...] = jnp.zeros_like(acc)

    def hooks(s):
        for stream in (gather_h, gather_g):
            for group in stream.groups_before(s):
                stream.group(group)
        gather_h.ready(s)
        gather_g.ready(s)

    def mlp(slot):
        rows = gather_h.rows(slot)
        h2_blk, g_blk = rows_of(fh, rows), rows_of(fg, rows)
        act, slope = gelu_pair(dot(h2_blk, w1[...]) + b1)
        act = act.astype(BF16)
        put_rows(act_all, rows, act)
        g_hidden = dot(g_blk, w2[...], NT) * slope
        gb_1[...] += row_sum(g_hidden)
        g_hidden = g_hidden.astype(BF16)
        put_rows(hid_all, rows, g_hidden)
        gw_1[...] += dot(g_hidden, h2_blk, TN)
        gw_2[...] += dot(act, g_blk, TN)

    loop_slots(at.ring, hooks, mlp)

    def hooks(s):
        if s >= 2 and s % 2 == 0:
            scat_h.step(s // 2 - 1)
            scat_m.step(s // 2 - 1)

    def put_both(slot):
        rows = scat_h.rows(slot)
        scat_h.put(slot, dot(rows_of(hid_all, rows), w1[...], NT))
        scat_m.put(slot, dot(rows_of(act_all, rows), w2[...]))

    loop_slots(at.ring, hooks, put_both)
    scat_h.step(at.half - 1)
    scat_m.step(at.half - 1)

    def take_h(part, value):
        g_h2[part] = value

    def take_m(part, value):
        total[part] = value + b2

    scat_h.final(take_h)
    scat_m.final(take_m)

    def back_one(b, carry):
        _, scale, gate = shift_scale_gate(b)
        g_out, mlp_total, grad = g[b].astype(F32), total[b], g_h2[b]
        x_out[b] = (x2[b].astype(F32) + gate * mlp_total).astype(BF16)
        normed, inv_std = normalize(x2[b])
        back = g_out + normalize_back(normed, inv_std, grad * (1.0 + scale))
        g_x2[b] = back
        g_cross[b] = back.astype(BF16)
        terms = grad, grad * normed, g_out * mlp_total, back.astype(BF16).astype(F32), gm[b].astype(F32)
        return tuple(c + row_sum(t) for c, t in zip(carry, terms))

    zero = jnp.zeros((1, x2.shape[-1]), F32)
    sums[...] = jnp.zeros_like(sums)
    found = lax.fori_loop(0, batch, back_one, (zero,) * 5)
    for row, value in zip((SHIFT2, SCALE2, GATE2, B_CO, B_2), found):
        sums[row:row + 1, :] = value
    for stream in (gather_h, gather_g, scat_h, scat_m):
        stream.finish()


def mlp_call(tp_size, cid, head_dim, *ins):
    batch, n_loc, width = ins[0].shape
    ffn = ins[-1].shape[0]
    n_tok = n_loc * tp_size
    ring, half = tp_size // 2, tp_size // 4
    local, tokens, hidden = (batch, n_loc, width), (batch, n_tok, width), (batch, n_tok, ffn)
    bufs = (ring, batch, 2 * n_loc, width), (ring, *local), (2, half, *local)
    outs = [(local, BF16), (local, F32), (local, BF16), ((SUM_ROWS, width), F32), ((ffn, width), F32), ((ffn, width), F32), ((1, ffn), F32)]
    scratch = [(local, BF16), (local, BF16), ((3, batch, width), F32), (tokens, BF16), (tokens, BF16), (hidden, BF16), (hidden, BF16),
               (local, F32), (local, F32)]
    return pl.pallas_call(
        functools.partial(mlp_body, tp_size, head_dim),
        out_shape=[jax.ShapeDtypeStruct(*o) for o in outs],
        in_specs=[VMEM] * len(ins),
        out_specs=[VMEM] * len(outs),
        scratch_shapes=[pltpu.VMEM(*k) for k in scratch] + [pltpu.VMEM(k, BF16) for k in bufs * 2]
        + gather_sems(tp_size) * 2 + scatter_sems(tp_size) * 2,
        compiler_params=KERNEL(collective_id=cid),
        name='mlp_both_ways',
    )(*ins)


def finish_body(head_dim, n_head, *refs):
    sources, results = refs[:len(refs) // 2], refs[len(refs) // 2:]
    for i, (source, result) in enumerate(zip(sources, results)):
        if i >= n_head:
            result[...] = source[...].astype(result.dtype)
            continue
        parts = result.shape[0] // head_dim
        head_pad = source.shape[0] // parts
        for p in range(parts):
            result[p * head_dim:(p + 1) * head_dim, :] = source[p * head_pad:p * head_pad + head_dim, :].astype(result.dtype)


def finish_call(head_dim, head_pad, padded, plain):
    shapes = [(a.shape[0] // head_pad * head_dim, a.shape[1]) for a in padded] + [a.shape for a in plain]
    return pl.pallas_call(
        functools.partial(finish_body, head_dim, len(padded)),
        out_shape=[jax.ShapeDtypeStruct(shape, BF16) for shape in shapes],
        in_specs=[VMEM] * len(shapes),
        out_specs=[VMEM] * len(shapes),
        compiler_params=pltpu.CompilerParams(vmem_limit_bytes=67 * 1000 * 1000),
        name='results',
    )(*padded, *plain)


def device_block(tp_size, x_loc, y_loc, t_loc, len_loc, mod_table, w_qkv, b_qkv, w_o, b_o, w_q, b_q, w_kv, b_kv, w_co, b_co, w_1, b_1, w_2, b_2, g_loc):
    head_dim = w_q.shape[2]
    head_pad = -(-head_dim // LANES) * LANES
    wqkv, wq, wkv = [w.transpose(1, 2, 0)[0] for w in (w_qkv, w_q, w_kv)]
    wo, wco = w_o[0], w_co[0]

    gap = jnp.zeros((1, head_pad - head_dim), BF16)
    pieces = []
    for bias in (b_qkv, b_kv, b_q):
        for at in range(0, bias.shape[1], head_dim):
            pieces += [bias[:, at:at + head_dim], gap]
    biases = jnp.concatenate(pieces + [b[None] for b in (b_o, b_co, b_2, b_1)], axis=1).astype(F32)

    h1_all, y_all, x1_all, qkv, kv, q_cross, attn_val, cross_val, attn_prob, cross_prob, attn_total, x2_loc = forward_call(
        tp_size, 0, head_dim, head_pad, x_loc, y_loc, t_loc, mod_table, len_loc, biases, wqkv, wkv, wq, wo, wco)
    x_out, g_x2, g_cross, sums, g_w_1, g_w_2, g_b_1 = mlp_call(tp_size, 1, head_dim, x2_loc, g_loc, t_loc, mod_table, biases, w_1, w_2)
    g_x, g_y, sums, g_w_qkv, g_w_kv, g_w_q, g_w_o, g_w_co, g_b_qkv, g_b_kv, g_b_q = backward_call(
        tp_size, 2, head_dim, head_pad,
        [g_cross, g_x2, x_loc, attn_total, t_loc, mod_table, wqkv, wkv, wq, wo, wco, sums],
        [qkv, kv, q_cross, attn_val, cross_val, attn_prob, cross_prob], [h1_all, x1_all, y_all])

    g_w_qkv, g_w_kv, g_w_q, g_w_o, g_w_co, g_w_2, x_out, g_x, g_y = finish_call(
        head_dim, head_pad, [g_w_qkv, g_w_kv, g_w_q, g_w_o, g_w_co], [g_w_2, x_out, g_x, g_y])

    def head_weight(grad):
        return grad[None].transpose(2, 0, 1)

    def head_bias(grad):
        return grad.reshape(-1, head_pad)[:, :head_dim].reshape(1, -1).astype(BF16)

    vectors = sums.astype(BF16)
    return (x_out, g_x, g_y, sums[:6],
            head_weight(g_w_qkv), head_bias(g_b_qkv), g_w_o[None], vectors[B_O],
            head_weight(g_w_q), head_bias(g_b_q), head_weight(g_w_kv), head_bias(g_b_kv),
            g_w_co[None], vectors[B_CO],
            g_w_1.T.astype(BF16), g_b_1[0].astype(BF16), g_w_2, vectors[B_2])


def solution(mesh):
    token, heads, rows, whole = P('dp', 'tp'), P(None, 'tp'), P('tp'), P()
    group, group_rows, group_heads = P('dp'), P(('dp', 'tp')), P('dp', 'tp')
    in_specs = (token, token, group, group, whole, heads, rows, rows, whole, heads, rows, heads, rows, rows, whole, heads, rows, rows, whole, token)
    out_specs = (token, token, token, group, group_heads, group_rows, group_rows, group, group_heads, group_rows, group_heads, group_rows,
                 group_rows, group, group_heads, group_rows, group_rows, group)
    return jax.shard_map(functools.partial(device_block, mesh.shape['tp']), mesh=mesh, in_specs=in_specs, out_specs=out_specs, check_vma=False)
```

```python
import functools
import itertools

import jax
import jax.numpy as jnp
from jax import lax
from jax.experimental import pallas as pl
from jax.experimental.pallas import tpu as pltpu
from jax.sharding import PartitionSpec as P

LN_EPS = 1e-6
MASK_FILL = -1e30
LANES = 128
MESH = pl.DeviceIdType.MESH
BF16 = jnp.bfloat16
F32 = jnp.float32
NN = (((1,), (0,)), ((), ()))
NT = (((1,), (1,)), ((), ()))
TN = (((0,), (0,)), ((), ()))
SHIFT1, SCALE1, GATE1, SHIFT2, SCALE2, GATE2, B_O, B_CO, B_2 = range(9)
SUM_ROWS = 16
FORWARD_BIASES = 'qkv', 'kv', 'q', 'o', 'co'
UP, DOWN = HALVES = WAYS = 0, 1
SEND, TAKE = True, False
KERNEL = functools.partial(pltpu.CompilerParams, has_side_effects=True, vmem_limit_bytes=67 * 1000 * 1000)
VMEM, ANY = pl.BlockSpec(memory_space=pltpu.VMEM), pl.BlockSpec(memory_space=pl.ANY)


def dot(lhs, rhs, dims=NN):
    return lax.dot_general(lhs, rhs[...], dims, preferred_element_type=F32)


def add_to(acc, value):
    acc[...] += value


def clear(refs):
    for ref in refs:
        ref[...] = jnp.zeros_like(ref)


def each(n, body):
    def step(i, carry):
        body(i)
        return carry
    lax.fori_loop(0, n, step, None)


def cutter(refs):
    left = iter(refs)
    return lambda n: list(itertools.islice(left, n))


def biases_of(packed, names, width, head_dim):
    return [packed[:, at:at + size] for at, size in (bias_place(name, width, head_dim, packed.shape[1]) for name in names)]


def bias_place(name, width, head_dim, total):
    head_pad = -(-head_dim // LANES) * LANES
    sizes = {'qkv': 3 * head_pad, 'kv': 2 * head_pad, 'q': head_pad, 'o': width, 'co': width, '2': width}
    sizes['1'] = total - sum(sizes.values())
    names = list(sizes)
    return sum(sizes[n] for n in names[:names.index(name)]), sizes[name]


class Place:
    def __init__(self, tp_size):
        self.tp_size = tp_size
        self.me = lax.axis_index('tp')
        self.ring, self.chip, self.core = tp_size // 2, self.me // 2, lax.rem(self.me, 2)
        self.half = self.ring // 2

    def wrap(self, zz):
        return lax.rem(zz + self.ring, self.ring)

    def sibling(self):
        return {'tp': self.chip * 2 + 1 - self.core}

    def ahead(self, sign):
        return {'tp': self.wrap(self.chip + sign) * 2 + self.core}

    def other(self, d):
        return {'tp': lax.rem(self.me + d, self.tp_size)}

    def greet(self, peers):
        barrier = pltpu.get_barrier_semaphore()
        for peer in peers:
            pl.semaphore_signal(barrier, device_id=peer, device_id_type=MESH)
        pl.semaphore_wait(barrier, len(peers))

    def greet_all(self):
        self.greet([self.other(d) for d in range(1, self.tp_size)])

    def greet_near(self):
        self.greet([self.ahead(1), self.ahead(-1), self.sibling()])


class Gather:
    def __init__(self, at, own, full, sems):
        self.at, self.own_ref, self.full = at, own, full
        self.rsend, self.rrecv, self.ssend, self.srecv = sems
        self.batch, self.n_loc = own.shape[0], own.shape[1]
        self.hb = self.batch // 2

    def part(self, zz, cc, ch):
        row = pl.multiple_of((zz * 2 + cc) * self.n_loc, self.n_loc)
        return self.full.at[pl.ds(ch * self.hb, self.hb), pl.ds(row, self.n_loc), :]

    def own(self, ch):
        return self.own_ref.at[pl.ds(ch * self.hb, self.hb)]

    def ring_copy(self, way, k, ch, sending):
        at = self.at
        sign = -1 if way == UP else 1
        zb = at.wrap(at.chip + sign * (k - 1 if sending else k))
        src = self.own(ch) if (sending and k == 1) else self.part(zb, at.core, ch)
        return pltpu.make_async_remote_copy(
            src_ref=src, dst_ref=self.part(zb, at.core, ch),
            send_sem=self.rsend.at[way, k - 1, ch], recv_sem=self.rrecv.at[way, k - 1, ch],
            device_id=at.ahead(-sign), device_id_type=MESH)

    def chip_at(self, slot):
        k = (slot + 1) // 2
        return self.at.wrap(self.at.chip - k) if slot % 2 else self.at.wrap(self.at.chip + k)

    def sib_copy(self, slot, ch, sending):
        at = self.at
        cc = at.core if sending else 1 - at.core
        zb = self.chip_at(slot)
        src = self.own(ch) if (sending and slot == 0) else self.part(zb, cc, ch)
        return pltpu.make_async_remote_copy(
            src_ref=src, dst_ref=self.part(zb, cc, ch),
            send_sem=self.ssend.at[slot, ch], recv_sem=self.srecv.at[slot, ch],
            device_id=at.sibling(), device_id_type=MESH)

    def carries(self, way, k, ch):
        return k < self.at.half or (k == self.at.half and ch == way)

    def slot_of(self, way, k):
        half = self.at.half
        return 2 * half - 1 if k == half else (2 * k - 1 if way == UP else 2 * k)

    def start(self):
        for way, ch in ((UP, 0), (DOWN, 1), (UP, 1), (DOWN, 0)):
            self.ring_copy(way, 1, ch, SEND).start()
        for ch in HALVES:
            self.sib_copy(0, ch, SEND).start()
        row = pl.multiple_of(self.at.me * self.n_loc, self.n_loc)
        self.full[:, pl.ds(row, self.n_loc), :] = self.own_ref[...]

    def arrive(self, way, k, ch):
        self.ring_copy(way, k, ch, TAKE).wait_recv()
        if self.carries(way, k + 1, ch):
            self.ring_copy(way, k + 1, ch, SEND).start()
        self.sib_copy(self.slot_of(way, k), ch, SEND).start()

    def group(self, g):
        k = g // 2 + 1
        first, second = ((UP, 0), (DOWN, 1)) if g % 2 == 0 else ((UP, 1), (DOWN, 0))
        self.arrive(first[0], k, first[1])
        self.arrive(second[0], k, second[1])

    def groups_before(self, slot):
        last = self.at.ring - 1
        return () if slot == last - 1 else ((last - 1,) if slot == last else (slot,))

    def ready(self, slot):
        for ch in HALVES:
            self.sib_copy(slot, ch, TAKE).wait_recv()

    def rows(self, slot):
        k = (slot + 1) // 2
        zz = self.at.wrap(self.at.chip + (1 - 2 * lax.rem(slot, 2)) * k)
        return pl.ds(pl.multiple_of(zz * 2 * self.n_loc, 2 * self.n_loc), 2 * self.n_loc)

    def save_copy(self, dest, sem, slot):
        rows = self.rows(slot)
        return pltpu.make_async_copy(self.full.at[:, rows, :], dest.at[:, rows, :], sem.at[slot])

    def finish(self):
        for way in WAYS:
            for k in range(1, self.at.half + 1):
                for ch in HALVES:
                    if self.carries(way, k, ch):
                        self.ring_copy(way, k, ch, SEND).wait_send()
        for slot in range(self.at.ring):
            for ch in HALVES:
                self.sib_copy(slot, ch, SEND).wait_send()


class Scatter:
    def __init__(self, at, pbuf, sibr, rcv, sems):
        self.at, self.pbuf, self.sibr, self.rcv = at, pbuf, sibr, rcv
        self.rsend, self.rrecv, self.ssend, self.srecv = sems
        self.batch, self.n_loc = sibr.shape[1], sibr.shape[2]
        self.hb = self.batch // 2

    def slot_of(self, way, s):
        return 0 if s == 0 else (2 * s - 1 if way == UP else 2 * s)

    def rows(self, slot):
        at = self.at
        away = at.half - (slot + 1) // 2
        zz = at.wrap(at.chip + (2 * lax.rem(slot, 2) - 1) * away)
        return pl.ds(pl.multiple_of(zz * 2 * self.n_loc, 2 * self.n_loc), 2 * self.n_loc)

    def put(self, slot, value):
        self.pbuf[slot] = value.astype(BF16).reshape(self.batch, 2 * self.n_loc, value.shape[-1])
        self.sib_copy(slot).start()

    def ring_copy(self, way, s, ch):
        part = pl.ds(ch * self.hb, self.hb)
        return pltpu.make_async_remote_copy(
            src_ref=self.sibr.at[self.slot_of(way, s), part], dst_ref=self.rcv.at[way, s, part],
            send_sem=self.rsend.at[way, s, ch], recv_sem=self.rrecv.at[way, s, ch],
            device_id=self.at.ahead(1 if way == UP else -1), device_id_type=MESH)

    def sib_copy(self, slot):
        rows = pl.ds(pl.multiple_of((1 - self.at.core) * self.n_loc, self.n_loc), self.n_loc)
        return pltpu.make_async_remote_copy(
            src_ref=self.pbuf.at[slot, :, rows, :], dst_ref=self.sibr.at[slot],
            send_sem=self.ssend.at[slot], recv_sem=self.srecv.at[slot],
            device_id=self.at.sibling(), device_id_type=MESH)

    def own_sum(self, slot, part):
        rows = pl.ds(pl.multiple_of(self.at.core * self.n_loc, self.n_loc), self.n_loc)
        return self.pbuf[slot, part, rows, :].astype(F32) + self.sibr[slot, part].astype(F32)

    def starts_at(self, way, ch):
        return 0 if ch == way else 1

    def pass_on(self, way, s, ch):
        slot, part = self.slot_of(way, s), pl.ds(ch * self.hb, self.hb)
        total = self.own_sum(slot, part)
        if s > self.starts_at(way, ch):
            self.ring_copy(way, s - 1, ch).wait_recv()
            total = total + self.rcv[way, s - 1, part].astype(F32)
        self.sibr[slot, part] = total.astype(BF16)
        self.ring_copy(way, s, ch).start()

    def step(self, s):
        if s == 0:
            self.sib_copy(0).wait_recv()
            self.pass_on(UP, 0, 0)
            self.pass_on(DOWN, 0, 1)
            return
        self.sib_copy(2 * s - 1).wait_recv()
        self.pass_on(UP, s, 1)
        self.sib_copy(2 * s).wait_recv()
        self.pass_on(DOWN, s, 0)
        self.pass_on(UP, s, 0)
        self.pass_on(DOWN, s, 1)

    def final(self, use):
        last = self.at.ring - 1
        self.sib_copy(last).wait_recv()
        for ch, order in ((1, (UP, DOWN)), (0, (DOWN, UP))):
            part = pl.ds(ch * self.hb, self.hb)
            total = self.own_sum(last, part)
            for way in order:
                self.ring_copy(way, self.at.half - 1, ch).wait_recv()
                total = total + self.rcv[way, self.at.half - 1, part].astype(F32)
            use(part, total)

    def finish(self):
        for way in WAYS:
            for s in range(self.at.half):
                for ch in HALVES:
                    if s >= self.starts_at(way, ch):
                        self.ring_copy(way, s, ch).wait_send()
        for slot in range(self.at.ring):
            self.sib_copy(slot).wait_send()


def loop_slots(n, hooks, body):
    def step(slot):
        for s in range(n):
            @pl.when(slot == s)
            def _():
                hooks(s)
        body(slot)
    each(n, step)


def gather_sems(tp_size):
    ring, half = tp_size // 2, tp_size // 4
    return [pltpu.SemaphoreType.DMA(s) for s in ((2, half, 2), (2, half, 2), (ring, 2), (ring, 2))]


def scatter_sems(tp_size):
    ring, half = tp_size // 2, tp_size // 4
    return [pltpu.SemaphoreType.DMA(s) for s in ((2, half, 2), (2, half, 2), (ring,), (ring,))]


def pad_rows(dest, source, head_dim):
    parts = source.shape[0] // head_dim
    head_pad = dest.shape[0] // parts
    width = dest.shape[1]
    for i in range(parts):
        dest[i * head_pad:i * head_pad + head_dim, :] = source[i * head_dim:(i + 1) * head_dim, :]
        dest[i * head_pad + head_dim:(i + 1) * head_pad, :] = jnp.zeros((head_pad - head_dim, width), dest.dtype)


def at_sample(mod, b):
    return [mod[i, pl.ds(b, 1), :] for i in range(mod.shape[0])]


def fill_mod(mod, t_ref, table_ref, rows):
    for i, row in enumerate(rows):
        mod[i] = mod_row(t_ref, table_ref, row)


def mod_row(t_ref, table_ref, i):
    width = table_ref.shape[1]
    return table_ref[i:i + 1, :].astype(F32) + t_ref[:, i * width:(i + 1) * width].astype(F32)


def rows_of(ref, rows):
    block = ref[:, rows, :]
    return block.reshape(block.shape[0] * block.shape[1], block.shape[2])


def put_rows(ref, rows, value):
    ref[:, rows, :] = value.astype(ref.dtype).reshape(ref.shape[0], rows.size, ref.shape[2])


def row_sum(value):
    return jnp.sum(value, axis=0, keepdims=True)


def gelu_pair(hidden):
    c0, c1 = 0.7978845608028654, 0.044715
    square = hidden * hidden
    tanh = jnp.tanh(c0 * hidden * (1.0 + c1 * square))
    half_up = 0.5 * (1.0 + tanh)
    slope = half_up + 0.5 * hidden * (1.0 - tanh * tanh) * (c0 * (1.0 + 3.0 * c1 * square))
    return hidden * half_up, slope


def normalize(rows):
    rows = rows.astype(F32)
    centered = rows - jnp.mean(rows, axis=-1, keepdims=True)
    inv_std = lax.rsqrt(jnp.mean(centered * centered, axis=-1, keepdims=True) + LN_EPS)
    return centered * inv_std, inv_std


def normalize_back(normed, inv_std, g_normed):
    mean_g = jnp.mean(g_normed, axis=-1, keepdims=True)
    mean_gn = jnp.mean(g_normed * normed, axis=-1, keepdims=True)
    return inv_std * (g_normed - mean_g - normed * mean_gn)


def softmax_of(scores):
    top = jnp.max(scores, axis=-1, keepdims=True)
    powers = jnp.exp(scores - top)
    return powers * (1.0 / jnp.sum(powers, axis=-1, keepdims=True))


def forward_body(tp_size, head_dim, *refs):
    at = Place(tp_size)
    take = cutter(refs)
    x, y, g, t_emb, table, lens, biases, wqkv_in, wkv_in, wq_in, wo_in, wco_in = take(12)
    bqkv, bkv, bq, bo, bco = biases_of(biases, FORWARD_BIASES, wqkv_in.shape[1], head_dim)
    h1_out, y_out, x1_out, g_out = take(4)
    outs, scratch = take(9), take(9)
    qkv, kv, q_c, val, cval, prob, cprob, atot, x2 = scratch
    h1, x1, gm, mod, fh, fy, fx, fg, pbuf, sibr1, rcv1, sibr2, rcv2, wqkv, wkv, wq, wo, wco = take(18)
    gather_h, gather_y, gather_x, gather_g = [Gather(at, own, full, take(4)) for own, full in ((h1, fh), (y, fy), (x1, fx), (gm, fg))]
    scat_o, scat_c = [Scatter(at, pbuf, sibr, rcv, take(4)) for sibr, rcv in ((sibr1, rcv1), (sibr2, rcv2))]
    saves, out_sem = take(4), refs[-1]
    batch = x.shape[0]
    head_pad = wq.shape[0]
    scale = head_dim ** -0.5

    def out_copy(i):
        return pltpu.make_async_copy(scratch[i], outs[i], out_sem.at[i])

    at.greet_near()
    gather_y.start()
    fill_mod(mod, t_emb, table, (SHIFT1, SCALE1, GATE1, GATE2))

    def norm_one(b):
        shift, scale, _, gate = at_sample(mod, b)
        normed, _ = normalize(x[b])
        h1[b] = (normed * (1.0 + scale) + shift).astype(BF16)
        gm[b] = (g[b].astype(F32) * gate).astype(BF16)

    each(batch, norm_one)
    gather_h.start()
    for dest, source in ((wqkv, wqkv_in), (wkv, wkv_in), (wq, wq_in), (wo, wo_in), (wco, wco_in)):
        pad_rows(dest, source, head_dim)

    def hooks(s):
        for g in gather_h.groups_before(s):
            gather_h.group(g)
        gather_h.ready(s)
        if s in (3, 5):
            gather_y.group(s // 2 - 1)

    def project(slot):
        rows = gather_h.rows(slot)
        gather_h.save_copy(h1_out, saves[0], slot).start()
        put_rows(qkv, rows, dot(rows_of(fh, rows), wqkv, NT) + bqkv)

    loop_slots(at.ring, hooks, project)

    def hooks(b):
        if b == batch // 2:
            gather_y.group(2)
        if b == batch - 1:
            gather_y.group(3)

    def attend_self(b):
        q_b, k_b, v_b = [qkv[b, :, i * head_pad:(i + 1) * head_pad] for i in range(3)]
        p_b = softmax_of(dot(q_b, k_b, NT) * scale).astype(BF16)
        prob[b] = p_b
        val[b] = dot(p_b, v_b).astype(BF16)

    loop_slots(batch, hooks, attend_self)
    for i in (0, 3, 5):
        out_copy(i).start()

    def hooks(s):
        if s >= 2 and s % 2 == 0:
            scat_o.step(s // 2 - 1)
            gather_y.group(s // 2 + 3)
        if s == at.ring - 1:
            gather_g.start()

    def project_o(slot):
        scat_o.put(slot, dot(rows_of(val, scat_o.rows(slot)), wo))

    loop_slots(at.ring, hooks, project_o)
    scat_o.step(at.half - 1)

    def take_o(part, total):
        atot[part] = total + bo

    scat_o.final(take_o)
    out_copy(7).start()

    def x1_one(b):
        _, _, gate, _ = at_sample(mod, b)
        x1[b] = (x[b].astype(F32) + gate * atot[b]).astype(BF16)

    each(batch, x1_one)

    gather_x.start()

    def hooks(s):
        for g in gather_x.groups_before(s):
            gather_x.group(g)
        gather_y.ready(s)
        gather_x.ready(s)
        if s >= 2 and s % 2 == 0:
            gather_g.group(s // 2 - 1)

    def project(slot):
        rows = gather_x.rows(slot)
        gather_y.save_copy(y_out, saves[1], slot).start()
        gather_x.save_copy(x1_out, saves[2], slot).start()
        put_rows(kv, rows, dot(rows_of(fy, rows), wkv, NT) + bkv)
        put_rows(q_c, rows, dot(rows_of(fx, rows), wq, NT) + bq)

    loop_slots(at.ring, hooks, project)
    scat_o.finish()

    def hooks(b):
        if b == batch // 2:
            gather_g.group(3)
        if b == batch - 1:
            gather_g.group(4)

    def attend_cross(b):
        k_b, v_b = [kv[b, :, i * head_pad:(i + 1) * head_pad] for i in range(2)]
        scores = dot(q_c[b], k_b, NT) * scale
        slots = lax.broadcasted_iota(jnp.int32, scores.shape, 1)
        p_b = softmax_of(jnp.where(slots < lens[b], scores, MASK_FILL)).astype(BF16)
        cprob[b] = p_b
        cval[b] = dot(p_b, v_b).astype(BF16)

    loop_slots(batch, hooks, attend_cross)
    for i in (1, 2, 4, 6):
        out_copy(i).start()

    def save_g(slots):
        for slot in slots:
            gather_g.ready(slot)
            gather_g.save_copy(g_out, saves[3], slot).start()

    def hooks(s):
        if s >= 2 and s % 2 == 0:
            scat_c.step(s // 2 - 1)
        if s == 3:
            gather_g.group(5)
            save_g(range(3))
        if s == 5:
            gather_g.group(6)
            save_g((3, 4))

    def project_c(slot):
        scat_c.put(slot, dot(rows_of(cval, scat_c.rows(slot)), wco))

    loop_slots(at.ring, hooks, project_c)
    scat_c.step(at.half - 1)
    save_g(range(5, at.ring))

    def take_c(part, total):
        x2[part] = (x1[part].astype(F32) + total + bco).astype(BF16)

    scat_c.final(take_c)
    out_copy(8).start()
    for stream in (gather_h, gather_y, gather_x, gather_g, scat_c):
        stream.finish()
    for slot in range(at.ring):
        gather_h.save_copy(h1_out, saves[0], slot).wait()
        gather_y.save_copy(y_out, saves[1], slot).wait()
        gather_x.save_copy(x1_out, saves[2], slot).wait()
        gather_g.save_copy(g_out, saves[3], slot).wait()
    for i in range(9):
        out_copy(i).wait()


def forward_call(tp_size, cid, head_dim, head_pad, *ins):
    batch, n_loc, width = ins[0].shape
    n_tok = n_loc * tp_size
    ring, half = tp_size // 2, tp_size // 4
    tokens = lambda last: (batch, n_tok, last)
    local = (batch, n_loc, width)
    kept = [(tokens(3 * head_pad), BF16), (tokens(2 * head_pad), BF16), (tokens(head_pad), BF16), (tokens(head_pad), BF16),
            (tokens(head_pad), BF16), (tokens(n_tok), BF16), (tokens(n_tok), BF16), (local, F32), (local, BF16)]
    sib, rcv = (ring, *local), (2, half, *local)
    return pl.pallas_call(
        functools.partial(forward_body, tp_size, head_dim),
        out_shape=[jax.ShapeDtypeStruct(tokens(width), BF16)] * 4 + [jax.ShapeDtypeStruct(*k) for k in kept],
        in_specs=[VMEM] * 5 + [pl.BlockSpec(memory_space=pltpu.SMEM)] + [VMEM] * (len(ins) - 6),
        out_specs=[ANY] * (4 + len(kept)),
        scratch_shapes=[pltpu.VMEM(*k) for k in kept] + [
            *[pltpu.VMEM(local, BF16)] * 3, pltpu.VMEM((4, batch, width), F32), *[pltpu.VMEM(tokens(width), BF16)] * 4,
            pltpu.VMEM((ring, batch, 2 * n_loc, width), BF16),
            pltpu.VMEM(sib, BF16), pltpu.VMEM(rcv, BF16), pltpu.VMEM(sib, BF16), pltpu.VMEM(rcv, BF16)]
        + [pltpu.VMEM((n * head_pad, width), BF16) for n in (3, 2, 1, 1, 1)]
        + gather_sems(tp_size) * 4 + scatter_sems(tp_size) * 2
        + [pltpu.SemaphoreType.DMA((ring,))] * 4 + [pltpu.SemaphoreType.DMA((len(kept),))],
        compiler_params=KERNEL(collective_id=cid),
        name='attention_forward',
    )(*ins)


class RowFeed:
    def __init__(self, source, buf, sem, rows):
        self.source, self.buf, self.sem, self.rows = source, buf, sem, rows

    def copy(self, slot):
        side = lax.rem(slot, 2)
        return pltpu.make_async_copy(self.source.at[:, self.rows(slot), :], self.buf.at[side], self.sem.at[side])

    def take(self, slot, n):
        @pl.when(slot + 1 < n)
        def _():
            self.copy(slot + 1).start()
        self.copy(slot).wait()
        block = self.buf[lax.rem(slot, 2)]
        return block.reshape(block.shape[0] * block.shape[1], block.shape[2])


def small_total(at, src, got, mine, out, sems):
    send1, recv1, send2, recv2 = sems
    tiles = src.shape[1] // LANES

    def lanes(i):
        return pl.ds(i * LANES, LANES)

    def first(tile, peer_slot):
        return pltpu.make_async_remote_copy(
            src_ref=src.at[:, lanes(tile)], dst_ref=got.at[peer_slot], send_sem=send1.at[tile], recv_sem=recv1.at[peer_slot],
            device_id={'tp': tile}, device_id_type=MESH)

    def second(tile, d):
        return pltpu.make_async_remote_copy(
            src_ref=mine, dst_ref=out.at[:, lanes(tile)], send_sem=send2.at[d - 1], recv_sem=recv2.at[tile],
            device_id=at.other(d), device_id_type=MESH)

    for tile in range(tiles):
        @pl.when(at.me != tile)
        def _():
            first(tile, lax.rem(at.me - tile + at.tp_size, at.tp_size) - 1).start()
    for tile in range(tiles):
        @pl.when(at.me == tile)
        def _():
            total = src[:, tile * LANES:(tile + 1) * LANES]
            for d in range(1, at.tp_size):
                first(tile, d - 1).wait_recv()
                total = total + got[d - 1]
            mine[...] = total
            for d in range(1, at.tp_size):
                second(tile, d).start()
            out[:, tile * LANES:(tile + 1) * LANES] = total
            for d in range(1, at.tp_size):
                second(tile, d).wait_send()
    for tile in range(tiles):
        @pl.when(at.me != tile)
        def _():
            second(tile, 1).wait_recv()
            first(tile, 0).wait_send()


def backward_body(tp_size, head_dim, *refs):
    at = Place(tp_size)
    take = cutter(refs)
    g_cross, g_x2, x, x2, g, atot, t_emb, table, biases, w2, wqkv_in, wkv_in, wq_in, wo_in, wco_in, sums_in = take(16)
    b2, = biases_of(biases, ('2',), x.shape[-1], head_dim)
    loads, feeds = take(8), take(3)
    x_out, g_x, g_y, sums_out = take(4)
    accs = take(8)
    gw_qkv, gw_kv, gw_q, gw_o, gw_co, gb_qkv, gb_kv, gb_q = accs
    held = take(8)
    qkv, kv, q_c, val, cval, prob, cprob, act_all = held
    full, pbuf, sibr1, rcv1, pbufy, sibr2, rcv2, wqkv, wkv, wq, wo, wco = take(12)
    g_val, g_qkv, g_kv, g_q, g_x1, g_h1, g_attn, mod, sums, got, mine, feed_a, feed_y = take(13)
    gather_c, gather_a = [Gather(at, own, full, take(4)) for own in (g_cross, g_attn)]
    near, far = (pbuf, sibr1, rcv1), (pbufy, sibr2, rcv2)
    scat_m, scat_q, scat_y, scat_h = [Scatter(at, *bufs, take(4)) for bufs in (far, near, far, near)]
    load_sem, *feed_sems = take(4)
    feed_h, feed_x, feed_yy = [
        RowFeed(source, buf, sem, scat.rows)
        for source, buf, sem, scat in zip(feeds, (feed_a, feed_a, feed_y), feed_sems, (scat_h, scat_q, scat_y))]
    batch, n_loc, width = x.shape
    ring, half = at.ring, at.half
    head_pad = wq.shape[0]
    scale = head_dim ** -0.5

    def load_copy(i):
        return pltpu.make_async_copy(loads[i], held[i], load_sem.at[i])

    for i in range(len(held)):
        load_copy(i).start()
    at.greet_all()
    gather_c.start()
    feed_x.copy(0).start()
    feed_yy.copy(0).start()
    fill_mod(mod, t_emb, table, (SHIFT1, SCALE1, GATE1, GATE2))
    for dest, source in ((wqkv, wqkv_in), (wkv, wkv_in), (wq, wq_in), (wo, wo_in), (wco, wco_in)):
        pad_rows(dest, source, head_dim)
    sums[...] = sums_in[...]
    clear(accs)
    for i in range(len(held)):
        load_copy(i).wait()

    def put_m(first, last):
        def body(slot, carry):
            scat_m.put(slot, dot(rows_of(act_all, scat_m.rows(slot)), w2))
            return carry
        lax.fori_loop(first, last, body, None)

    def out_back(gather, value, weight, acc):
        def body(slot):
            rows = gather.rows(slot)
            block = rows_of(full, rows)
            put_rows(g_val, rows, dot(block, weight, NT))
            add_to(acc, dot(rows_of(value, rows), block, TN))
        return body

    def hooks(s):
        for g in gather_c.groups_before(s):
            gather_c.group(g)
        if s == 1:
            put_m(0, 3)
            scat_m.step(0)
        if s == 3:
            put_m(3, 5)
            scat_m.step(1)
        if s == 5:
            put_m(5, ring)
            scat_m.step(2)
        gather_c.ready(s)

    loop_slots(ring, hooks, out_back(gather_c, cval, wco, gw_co))
    gather_c.finish()

    def back_one(q_b, k_b, v_b, p_b, g_b):
        g_p = dot(g_b, v_b, NT)
        p_f = p_b.astype(F32)
        row_dot = jnp.sum(g_p * p_f, axis=-1, keepdims=True)
        g_s = (p_f * (g_p - row_dot) * scale).astype(BF16)
        return dot(g_s, k_b).astype(BF16), dot(g_s, q_b, TN).astype(BF16), dot(p_b, g_b, TN).astype(BF16)

    def hooks(b):
        if b == batch // 2:
            scat_m.step(half - 1)

    def cross_back(b):
        parts = back_one(q_c[b], kv[b, :, :head_pad], kv[b, :, head_pad:], cprob[b], g_val[b])
        g_q[b] = parts[0]
        g_kv[b, :, :head_pad] = parts[1]
        g_kv[b, :, head_pad:] = parts[2]

    loop_slots(batch, hooks, cross_back)

    def hooks(s):
        if s >= 2 and s % 2 == 0:
            scat_q.step(s // 2 - 1)
        if s == 3:
            scat_m.final(take_m)
            scat_m.finish()

    def take_m(part, total):
        g_h1[part] = total + b2

    def put_q(slot):
        block = rows_of(g_q, scat_q.rows(slot))
        scat_q.put(slot, dot(block, wq))
        add_to(gw_q, dot(block, feed_x.take(slot, ring), TN))
        add_to(gb_q, row_sum(block.astype(F32)))

    def put_y(first, last):
        def body(slot, carry):
            block = rows_of(g_kv, scat_y.rows(slot))
            scat_y.put(slot, dot(block, wkv))
            add_to(gw_kv, dot(block, feed_yy.take(slot, ring), TN))
            add_to(gb_kv, row_sum(block.astype(F32)))
            return carry
        lax.fori_loop(first, last, body, None)

    loop_slots(ring, hooks, put_q)
    scat_q.step(half - 1)

    def out_one(b, gate_sum):
        gate, g_out, total = at_sample(mod, b)[-1], g[b].astype(F32), g_h1[b]
        x_out[b] = (x2[b].astype(F32) + gate * total).astype(BF16)
        return gate_sum + row_sum(g_out * total)

    zero = jnp.zeros((1, width), F32)
    sums[GATE2:GATE2 + 1, :] = lax.fori_loop(0, batch, out_one, zero)

    def take_q(part, total):
        g_x1[part] = g_x2[part] + total

    scat_q.final(take_q)
    feed_h.copy(0).start()

    def x1_back(b, carry):
        gate_sum, bias_sum = carry
        rows = g_x1[b]
        block = (rows * mod[2, pl.ds(b, 1), :]).astype(BF16)
        g_attn[b] = block
        return gate_sum + row_sum(rows * atot[b]), bias_sum + row_sum(block.astype(F32))

    gate_sum, bias_sum = lax.fori_loop(0, batch, x1_back, (zero, zero))
    for row, value in ((GATE1, gate_sum), (B_O, bias_sum)):
        sums[row:row + 1, :] = value

    scat_q.finish()
    gather_a.start()
    put_y(0, 3)
    scat_y.step(0)

    def hooks(s):
        for g in gather_a.groups_before(s):
            gather_a.group(g)
        if s == 1:
            put_y(3, 5)
            scat_y.step(1)
        if s == 5:
            put_y(5, ring)
            scat_y.step(2)
        gather_a.ready(s)

    loop_slots(ring, hooks, out_back(gather_a, val, wo, gw_o))

    def hooks(b):
        if b == batch // 4:
            scat_y.step(half - 1)

    def self_back(b):
        parts = back_one(*[qkv[b, :, i * head_pad:(i + 1) * head_pad] for i in range(3)], prob[b], g_val[b])
        for i in range(3):
            g_qkv[b, :, i * head_pad:(i + 1) * head_pad] = parts[i]

    loop_slots(batch, hooks, self_back)

    def take_y(part, total):
        g_y[part] = total.astype(BF16)

    def hooks(s):
        if s >= 2 and s % 2 == 0:
            scat_h.step(s // 2 - 1)
        if s == 5:
            scat_y.final(take_y)

    def put_h(slot):
        block = rows_of(g_qkv, scat_h.rows(slot))
        scat_h.put(slot, dot(block, wqkv))
        add_to(gw_qkv, dot(block, feed_h.take(slot, ring), TN))
        add_to(gb_qkv, row_sum(block.astype(F32)))

    loop_slots(ring, hooks, put_h)
    scat_h.step(half - 1)
    def take_h(part, total):
        g_h1[part] = total

    scat_h.final(take_h)

    def x_back(b, carry):
        shift_sum, scale_sum = carry
        normed, inv_std = normalize(x[b])
        grad = g_h1[b]
        back = normalize_back(normed, inv_std, grad * (1.0 + mod[1, pl.ds(b, 1), :]))
        g_x[b] = (g_x1[b] + back).astype(BF16)
        return shift_sum + row_sum(grad), scale_sum + row_sum(grad * normed)

    shift_sum, scale_sum = lax.fori_loop(0, batch, x_back, (zero, zero))
    for row, value in ((SHIFT1, shift_sum), (SCALE1, scale_sum)):
        sums[row:row + 1, :] = value
    small_total(at, sums, got, mine, sums_out, take(4))
    for stream in (gather_a, scat_y, scat_h):
        stream.finish()


def backward_call(tp_size, cid, head_dim, head_pad, ins, loads, feeds):
    batch, n_loc, width = ins[0].shape
    n_tok = n_loc * tp_size
    ring, half = tp_size // 2, tp_size // 4
    n_sum = ins[-1].shape[0]
    tokens = lambda last: (batch, n_tok, last)
    local = (batch, n_loc, width)
    sib, rcv, pbuf = (ring, *local), (2, half, *local), (ring, batch, 2 * n_loc, width)
    outs = [(local, BF16)] * 3 + [((n_sum, width), F32)]
    outs += [((n * head_pad, width), F32) for n in (3, 2, 1, 1, 1)] + [((1, n * head_pad), F32) for n in (3, 2, 1)]
    return pl.pallas_call(
        functools.partial(backward_body, tp_size, head_dim),
        out_shape=[jax.ShapeDtypeStruct(*o) for o in outs],
        in_specs=[VMEM] * len(ins) + [ANY] * (len(loads) + len(feeds)),
        out_specs=[VMEM] * len(outs),
        scratch_shapes=[pltpu.VMEM(a.shape, a.dtype) for a in loads]
        + [pltpu.VMEM(s, BF16) for s in (tokens(width), pbuf, sib, rcv, pbuf, sib, rcv)]
        + [pltpu.VMEM((n * head_pad, width), BF16) for n in (3, 2, 1, 1, 1)]
        + [pltpu.VMEM(tokens(n * head_pad), BF16) for n in (1, 3, 2, 1)]
        + [pltpu.VMEM(local, F32), pltpu.VMEM(local, F32), pltpu.VMEM(local, BF16), pltpu.VMEM((4, batch, width), F32), pltpu.VMEM((n_sum, width), F32),
           pltpu.VMEM((tp_size - 1, n_sum, LANES), F32), pltpu.VMEM((n_sum, LANES), F32)]
        + [pltpu.VMEM((2, batch, 2 * n_loc, width), BF16)] * 2
        + gather_sems(tp_size) * 2 + scatter_sems(tp_size) * 4
        + [pltpu.SemaphoreType.DMA((len(loads),))] + [pltpu.SemaphoreType.DMA((2,))] * 3
        + [pltpu.SemaphoreType.DMA((n,)) for n in (width // LANES, tp_size - 1, tp_size - 1, width // LANES)],
        compiler_params=KERNEL(collective_id=cid),
        name='attention_backward',
    )(*ins, *loads, *feeds)


def mlp_body(tp_size, head_dim, *refs):
    at = Place(tp_size)
    take = cutter(refs)
    x2, g, t_emb, table, biases, w1, w2, g_all = take(8)
    b1, = biases_of(biases, ('1',), x2.shape[-1], head_dim)
    act_all, g_x2, g_cross, sums, gw_1, gw_2, gb_1 = take(7)
    h2, mod, fh, hid_all, g_h2, feed, *bufs = take(9)
    gather_h, scat_h = Gather(at, h2, fh, take(4)), Scatter(at, *bufs, take(4))
    feed_g = RowFeed(g_all, feed, refs[-1], gather_h.rows)
    batch = x2.shape[0]

    feed_g.copy(0).start()
    at.greet_near()
    fill_mod(mod, t_emb, table, (SHIFT2, SCALE2, GATE2))

    def norm_one(b):
        shift, scale, _ = at_sample(mod, b)
        normed, _ = normalize(x2[b])
        h2[b] = (normed * (1.0 + scale) + shift).astype(BF16)

    each(batch, norm_one)
    gather_h.start()
    clear((gw_1, gw_2, gb_1, sums))

    def hooks(s):
        for group in gather_h.groups_before(s):
            gather_h.group(group)
        gather_h.ready(s)

    def mlp(slot):
        rows = gather_h.rows(slot)
        h2_blk, g_blk = rows_of(fh, rows), feed_g.take(slot, at.ring)
        act, slope = gelu_pair(dot(h2_blk, w1) + b1)
        act = act.astype(BF16)
        put_rows(act_all, rows, act)
        g_hidden = dot(g_blk, w2, NT) * slope
        add_to(gb_1, row_sum(g_hidden))
        g_hidden = g_hidden.astype(BF16)
        put_rows(hid_all, rows, g_hidden)
        add_to(gw_1, dot(g_hidden, h2_blk, TN))
        add_to(gw_2, dot(act, g_blk, TN))

    loop_slots(at.ring, hooks, mlp)

    def hooks(s):
        if s >= 2 and s % 2 == 0:
            scat_h.step(s // 2 - 1)

    def put_h(slot):
        scat_h.put(slot, dot(rows_of(hid_all, scat_h.rows(slot)), w1, NT))

    loop_slots(at.ring, hooks, put_h)
    scat_h.step(at.half - 1)

    def take_h(part, value):
        g_h2[part] = value

    scat_h.final(take_h)

    def back_one(b, carry):
        _, scale, gate = at_sample(mod, b)
        g_out, grad = g[b].astype(F32), g_h2[b]
        normed, inv_std = normalize(x2[b])
        back = g_out + normalize_back(normed, inv_std, grad * (1.0 + scale))
        g_x2[b] = back
        g_cross[b] = back.astype(BF16)
        terms = grad, grad * normed, back.astype(BF16).astype(F32), (g_out * gate).astype(BF16).astype(F32)
        return tuple(c + row_sum(t) for c, t in zip(carry, terms))

    zero = jnp.zeros((1, x2.shape[-1]), F32)
    found = lax.fori_loop(0, batch, back_one, (zero,) * 4)
    for row, value in zip((SHIFT2, SCALE2, B_CO, B_2), found):
        sums[row:row + 1, :] = value
    gather_h.finish()
    scat_h.finish()


def mlp_call(tp_size, cid, head_dim, *ins):
    batch, n_loc, width = ins[0].shape
    ffn = ins[-2].shape[0]
    n_tok = n_loc * tp_size
    ring, half = tp_size // 2, tp_size // 4
    local, tokens, hidden = (batch, n_loc, width), (batch, n_tok, width), (batch, n_tok, ffn)
    chip = batch, 2 * n_loc, width
    outs = [(hidden, BF16), (local, F32), (local, BF16), ((SUM_ROWS, width), F32), ((ffn, width), F32), ((ffn, width), F32), ((1, ffn), F32)]
    scratch = [(local, BF16), ((3, batch, width), F32), (tokens, BF16), (hidden, BF16), (local, F32), ((2, *chip), BF16),
               ((ring, *chip), BF16), ((ring, *local), BF16), ((2, half, *local), BF16)]
    return pl.pallas_call(
        functools.partial(mlp_body, tp_size, head_dim),
        out_shape=[jax.ShapeDtypeStruct(*o) for o in outs],
        in_specs=[VMEM] * (len(ins) - 1) + [ANY],
        out_specs=[VMEM] * len(outs),
        scratch_shapes=[pltpu.VMEM(*k) for k in scratch] + gather_sems(tp_size) + scatter_sems(tp_size) + [pltpu.SemaphoreType.DMA((2,))],
        compiler_params=KERNEL(collective_id=cid),
        name='mlp_both_ways',
    )(*ins)


def finish_body(head_dim, n_head, *refs):
    sources, results = refs[:len(refs) // 2], refs[len(refs) // 2:]
    for i, (source, result) in enumerate(zip(sources, results)):
        if i >= n_head:
            result[...] = source[...].astype(result.dtype)
            continue
        parts = result.shape[0] // head_dim
        head_pad = source.shape[0] // parts
        for p in range(parts):
            result[p * head_dim:(p + 1) * head_dim, :] = source[p * head_pad:p * head_pad + head_dim, :].astype(result.dtype)


def finish_call(head_dim, head_pad, padded, plain):
    shapes = [(a.shape[0] // head_pad * head_dim, a.shape[1]) for a in padded] + [a.shape for a in plain]
    return pl.pallas_call(
        functools.partial(finish_body, head_dim, len(padded)),
        out_shape=[jax.ShapeDtypeStruct(shape, BF16) for shape in shapes],
        in_specs=[VMEM] * len(shapes),
        out_specs=[VMEM] * len(shapes),
        compiler_params=pltpu.CompilerParams(vmem_limit_bytes=67 * 1000 * 1000),
        name='results',
    )(*padded, *plain)


def device_block(tp_size, x_loc, y_loc, t_loc, len_loc, mod_table, w_qkv, b_qkv, w_o, b_o, w_q, b_q, w_kv, b_kv, w_co, b_co, w_1, b_1, w_2, b_2, g_loc):
    head_dim = w_q.shape[2]
    head_pad = -(-head_dim // LANES) * LANES
    wqkv, wq, wkv = [w.transpose(1, 2, 0)[0] for w in (w_qkv, w_q, w_kv)]
    wo, wco = w_o[0], w_co[0]

    gap = jnp.zeros((1, head_pad - head_dim), BF16)
    pieces = []
    for bias in (b_qkv, b_kv, b_q):
        for at in range(0, bias.shape[1], head_dim):
            pieces += [bias[:, at:at + head_dim], gap]
    biases = jnp.concatenate(pieces + [b[None] for b in (b_o, b_co, b_2, b_1)], axis=1).astype(F32)

    h1_all, y_all, x1_all, g_all, qkv, kv, q_cross, attn_val, cross_val, attn_prob, cross_prob, attn_total, x2_loc = forward_call(
        tp_size, 0, head_dim, head_pad, x_loc, y_loc, g_loc, t_loc, mod_table, len_loc, biases, wqkv, wkv, wq, wo, wco)
    gelu_out, g_x2, g_cross, sums, g_w_1, g_w_2, g_b_1 = mlp_call(
        tp_size, 1, head_dim, x2_loc, g_loc, t_loc, mod_table, biases, w_1, w_2, g_all)
    x_out, g_x, g_y, sums, g_w_qkv, g_w_kv, g_w_q, g_w_o, g_w_co, g_b_qkv, g_b_kv, g_b_q = backward_call(
        tp_size, 2, head_dim, head_pad,
        [g_cross, g_x2, x_loc, x2_loc, g_loc, attn_total, t_loc, mod_table, biases, w_2, wqkv, wkv, wq, wo, wco, sums],
        [qkv, kv, q_cross, attn_val, cross_val, attn_prob, cross_prob, gelu_out], [h1_all, x1_all, y_all])

    g_w_qkv, g_w_kv, g_w_q, g_w_o, g_w_co, g_w_2, x_out, g_x, g_y = finish_call(
        head_dim, head_pad, [g_w_qkv, g_w_kv, g_w_q, g_w_o, g_w_co], [g_w_2, x_out, g_x, g_y])

    def head_weight(grad):
        return grad[None].transpose(2, 0, 1)

    def head_bias(grad):
        return grad.reshape(-1, head_pad)[:, :head_dim].reshape(1, -1).astype(BF16)

    vectors = sums.astype(BF16)
    return (x_out, g_x, g_y, sums[:6],
            head_weight(g_w_qkv), head_bias(g_b_qkv), g_w_o[None], vectors[B_O],
            head_weight(g_w_q), head_bias(g_b_q), head_weight(g_w_kv), head_bias(g_b_kv),
            g_w_co[None], vectors[B_CO],
            g_w_1.T.astype(BF16), g_b_1[0].astype(BF16), g_w_2, vectors[B_2])


def solution(mesh):
    token, heads, rows, whole = P('dp', 'tp'), P(None, 'tp'), P('tp'), P()
    group, group_rows, group_heads = P('dp'), P(('dp', 'tp')), P('dp', 'tp')
    in_specs = (token, token, group, group, whole, heads, rows, rows, whole, heads, rows, heads, rows, rows, whole, heads, rows, rows, whole, token)
    out_specs = (token, token, token, group, group_heads, group_rows, group_rows, group, group_heads, group_rows, group_heads, group_rows,
                 group_rows, group, group_heads, group_rows, group_rows, group)
    return jax.shard_map(functools.partial(device_block, mesh.shape['tp']), mesh=mesh, in_specs=in_specs, out_specs=out_specs, check_vma=False)
```

```python
import functools
import itertools

import jax
import jax.numpy as jnp
from jax import lax
from jax.experimental import pallas as pl
from jax.experimental.pallas import tpu as pltpu
from jax.sharding import PartitionSpec as P

LN_EPS = 1e-6
MASK_FILL = -1e30
LANES = 128
MESH = pl.DeviceIdType.MESH
BF16 = jnp.bfloat16
F32 = jnp.float32
NN = (((1,), (0,)), ((), ()))
NT = (((1,), (1,)), ((), ()))
TN = (((0,), (0,)), ((), ()))
SHIFT1, SCALE1, GATE1, SHIFT2, SCALE2, GATE2, B_O, B_CO, B_2 = range(9)
SUM_ROWS = 16
UP, DOWN = HALVES = WAYS = 0, 1
SEND, TAKE = True, False
KERNEL = functools.partial(pltpu.CompilerParams, has_side_effects=True, vmem_limit_bytes=67 * 1000 * 1000)
VMEM, ANY = pl.BlockSpec(memory_space=pltpu.VMEM), pl.BlockSpec(memory_space=pl.ANY)


def dot(lhs, rhs, dims=NN):
    return lax.dot_general(lhs, rhs[...], dims, preferred_element_type=F32)


def add_to(acc, value):
    acc[...] += value


def clear(refs):
    for ref in refs:
        ref[...] = jnp.zeros_like(ref)


def each(n, body):
    def step(i, carry):
        body(i)
        return carry
    lax.fori_loop(0, n, step, None)


def cutter(refs):
    left = iter(refs)
    return lambda n: list(itertools.islice(left, n))


def padded_bias(ref, head_dim, head_pad):
    gap = jnp.zeros((1, head_pad - head_dim), F32)
    parts = [ref[:, p:p + head_dim].astype(F32) for p in range(0, ref.shape[1], head_dim)]
    return jnp.concatenate([piece for part in parts for piece in (part, gap)], axis=1)


def row_of(ref):
    return ref[...].astype(F32).reshape(1, -1)


class Place:
    def __init__(self, tp_size):
        self.tp_size = tp_size
        self.me = lax.axis_index('tp')
        self.ring, self.chip, self.core = tp_size // 2, self.me // 2, lax.rem(self.me, 2)
        self.half = self.ring // 2

    def wrap(self, zz):
        return lax.rem(zz + self.ring, self.ring)

    def sibling(self):
        return {'tp': self.chip * 2 + 1 - self.core}

    def ahead(self, sign):
        return {'tp': self.wrap(self.chip + sign) * 2 + self.core}

    def other(self, d):
        return {'tp': lax.rem(self.me + d, self.tp_size)}

    def greet(self, peers):
        barrier = pltpu.get_barrier_semaphore()
        for peer in peers:
            pl.semaphore_signal(barrier, device_id=peer, device_id_type=MESH)
        pl.semaphore_wait(barrier, len(peers))

    def greet_all(self):
        self.greet([self.other(d) for d in range(1, self.tp_size)])

    def greet_near(self):
        self.greet([self.ahead(1), self.ahead(-1), self.sibling()])


class Gather:
    def __init__(self, at, own, full, sems):
        self.at, self.own_ref, self.full = at, own, full
        self.rsend, self.rrecv, self.ssend, self.srecv = sems
        self.batch, self.n_loc = own.shape[0], own.shape[1]
        self.hb = self.batch // 2

    def part(self, zz, cc, ch):
        row = pl.multiple_of((zz * 2 + cc) * self.n_loc, self.n_loc)
        return self.full.at[pl.ds(ch * self.hb, self.hb), pl.ds(row, self.n_loc), :]

    def own(self, ch):
        return self.own_ref.at[pl.ds(ch * self.hb, self.hb)]

    def ring_copy(self, way, k, ch, sending):
        at = self.at
        sign = -1 if way == UP else 1
        zb = at.wrap(at.chip + sign * (k - 1 if sending else k))
        src = self.own(ch) if (sending and k == 1) else self.part(zb, at.core, ch)
        return pltpu.make_async_remote_copy(
            src_ref=src, dst_ref=self.part(zb, at.core, ch),
            send_sem=self.rsend.at[way, k - 1, ch], recv_sem=self.rrecv.at[way, k - 1, ch],
            device_id=at.ahead(-sign), device_id_type=MESH)

    def chip_at(self, slot):
        k = (slot + 1) // 2
        return self.at.wrap(self.at.chip - k) if slot % 2 else self.at.wrap(self.at.chip + k)

    def sib_copy(self, slot, ch, sending):
        at = self.at
        cc = at.core if sending else 1 - at.core
        zb = self.chip_at(slot)
        src = self.own(ch) if (sending and slot == 0) else self.part(zb, cc, ch)
        return pltpu.make_async_remote_copy(
            src_ref=src, dst_ref=self.part(zb, cc, ch),
            send_sem=self.ssend.at[slot, ch], recv_sem=self.srecv.at[slot, ch],
            device_id=at.sibling(), device_id_type=MESH)

    def carries(self, way, k, ch):
        return k < self.at.half or (k == self.at.half and ch == way)

    def slot_of(self, way, k):
        half = self.at.half
        return 2 * half - 1 if k == half else (2 * k - 1 if way == UP else 2 * k)

    def start(self):
        for way, ch in ((UP, 0), (DOWN, 1), (UP, 1), (DOWN, 0)):
            self.ring_copy(way, 1, ch, SEND).start()
        for ch in HALVES:
            self.sib_copy(0, ch, SEND).start()
        row = pl.multiple_of(self.at.me * self.n_loc, self.n_loc)
        self.full[:, pl.ds(row, self.n_loc), :] = self.own_ref[...]

    def arrive(self, way, k, ch):
        self.ring_copy(way, k, ch, TAKE).wait_recv()
        if self.carries(way, k + 1, ch):
            self.ring_copy(way, k + 1, ch, SEND).start()
        self.sib_copy(self.slot_of(way, k), ch, SEND).start()

    def group(self, g):
        k = g // 2 + 1
        first, second = ((UP, 0), (DOWN, 1)) if g % 2 == 0 else ((UP, 1), (DOWN, 0))
        self.arrive(first[0], k, first[1])
        self.arrive(second[0], k, second[1])

    def groups_before(self, slot):
        last = self.at.ring - 1
        return () if slot == last - 1 else ((last - 1,) if slot == last else (slot,))

    def ready(self, slot):
        for ch in HALVES:
            self.sib_copy(slot, ch, TAKE).wait_recv()

    def rows(self, slot):
        k = (slot + 1) // 2
        zz = self.at.wrap(self.at.chip + (1 - 2 * lax.rem(slot, 2)) * k)
        return pl.ds(pl.multiple_of(zz * 2 * self.n_loc, 2 * self.n_loc), 2 * self.n_loc)

    def save_copy(self, dest, sem, slot):
        rows = self.rows(slot)
        return pltpu.make_async_copy(self.full.at[:, rows, :], dest.at[:, rows, :], sem.at[slot])

    def finish(self):
        for way in WAYS:
            for k in range(1, self.at.half + 1):
                for ch in HALVES:
                    if self.carries(way, k, ch):
                        self.ring_copy(way, k, ch, SEND).wait_send()
        for slot in range(self.at.ring):
            for ch in HALVES:
                self.sib_copy(slot, ch, SEND).wait_send()


class Scatter:
    def __init__(self, at, pbuf, sibr, rcv, sems):
        self.at, self.pbuf, self.sibr, self.rcv = at, pbuf, sibr, rcv
        self.rsend, self.rrecv, self.ssend, self.srecv = sems
        self.batch, self.n_loc = sibr.shape[1], sibr.shape[2]
        self.hb = self.batch // 2

    def slot_of(self, way, s):
        return 0 if s == 0 else (2 * s - 1 if way == UP else 2 * s)

    def rows(self, slot):
        at = self.at
        away = at.half - (slot + 1) // 2
        zz = at.wrap(at.chip + (2 * lax.rem(slot, 2) - 1) * away)
        return pl.ds(pl.multiple_of(zz * 2 * self.n_loc, 2 * self.n_loc), 2 * self.n_loc)

    def put(self, slot, value):
        self.pbuf[slot] = value.astype(BF16).reshape(self.batch, 2 * self.n_loc, value.shape[-1])
        self.sib_copy(slot).start()

    def ring_copy(self, way, s, ch):
        part = pl.ds(ch * self.hb, self.hb)
        return pltpu.make_async_remote_copy(
            src_ref=self.sibr.at[self.slot_of(way, s), part], dst_ref=self.rcv.at[way, s, part],
            send_sem=self.rsend.at[way, s, ch], recv_sem=self.rrecv.at[way, s, ch],
            device_id=self.at.ahead(1 if way == UP else -1), device_id_type=MESH)

    def sib_copy(self, slot):
        rows = pl.ds(pl.multiple_of((1 - self.at.core) * self.n_loc, self.n_loc), self.n_loc)
        return pltpu.make_async_remote_copy(
            src_ref=self.pbuf.at[slot, :, rows, :], dst_ref=self.sibr.at[slot],
            send_sem=self.ssend.at[slot], recv_sem=self.srecv.at[slot],
            device_id=self.at.sibling(), device_id_type=MESH)

    def own_sum(self, slot, part):
        rows = pl.ds(pl.multiple_of(self.at.core * self.n_loc, self.n_loc), self.n_loc)
        return self.pbuf[slot, part, rows, :].astype(F32) + self.sibr[slot, part].astype(F32)

    def starts_at(self, way, ch):
        return 0 if ch == way else 1

    def pass_on(self, way, s, ch):
        slot, part = self.slot_of(way, s), pl.ds(ch * self.hb, self.hb)
        total = self.own_sum(slot, part)
        if s > self.starts_at(way, ch):
            self.ring_copy(way, s - 1, ch).wait_recv()
            total = total + self.rcv[way, s - 1, part].astype(F32)
        self.sibr[slot, part] = total.astype(BF16)
        self.ring_copy(way, s, ch).start()

    def step(self, s):
        if s == 0:
            self.sib_copy(0).wait_recv()
            self.pass_on(UP, 0, 0)
            self.pass_on(DOWN, 0, 1)
            return
        self.sib_copy(2 * s - 1).wait_recv()
        self.pass_on(UP, s, 1)
        self.sib_copy(2 * s).wait_recv()
        self.pass_on(DOWN, s, 0)
        self.pass_on(UP, s, 0)
        self.pass_on(DOWN, s, 1)

    def final(self, use):
        last = self.at.ring - 1
        self.sib_copy(last).wait_recv()
        for ch, order in ((1, (UP, DOWN)), (0, (DOWN, UP))):
            part = pl.ds(ch * self.hb, self.hb)
            total = self.own_sum(last, part)
            for way in order:
                self.ring_copy(way, self.at.half - 1, ch).wait_recv()
                total = total + self.rcv[way, self.at.half - 1, part].astype(F32)
            use(part, total)

    def finish(self):
        for way in WAYS:
            for s in range(self.at.half):
                for ch in HALVES:
                    if s >= self.starts_at(way, ch):
                        self.ring_copy(way, s, ch).wait_send()
        for slot in range(self.at.ring):
            self.sib_copy(slot).wait_send()


def loop_slots(n, hooks, body):
    def step(slot):
        for s in range(n):
            @pl.when(slot == s)
            def _():
                hooks(s)
        body(slot)
    each(n, step)


def gather_sems(tp_size):
    ring, half = tp_size // 2, tp_size // 4
    return [pltpu.SemaphoreType.DMA(s) for s in ((2, half, 2), (2, half, 2), (ring, 2), (ring, 2))]


def scatter_sems(tp_size):
    ring, half = tp_size // 2, tp_size // 4
    return [pltpu.SemaphoreType.DMA(s) for s in ((2, half, 2), (2, half, 2), (ring,), (ring,))]


def pad_rows(dest, source, head_dim):
    parts = source.shape[0] // head_dim
    head_pad = dest.shape[0] // parts
    width = dest.shape[1]
    for i in range(parts):
        dest[i * head_pad:i * head_pad + head_dim, :] = source[i * head_dim:(i + 1) * head_dim, :]
        dest[i * head_pad + head_dim:(i + 1) * head_pad, :] = jnp.zeros((head_pad - head_dim, width), dest.dtype)


def at_sample(mod, b):
    return [mod[i, pl.ds(b, 1), :] for i in range(mod.shape[0])]


def fill_mod(mod, t_ref, table_ref, rows):
    for i, row in enumerate(rows):
        mod[i] = mod_row(t_ref, table_ref, row)


def mod_row(t_ref, table_ref, i):
    width = table_ref.shape[1]
    return table_ref[i:i + 1, :].astype(F32) + t_ref[:, i * width:(i + 1) * width].astype(F32)


def rows_of(ref, rows):
    block = ref[:, rows, :]
    return block.reshape(block.shape[0] * block.shape[1], block.shape[2])


def put_rows(ref, rows, value):
    ref[:, rows, :] = value.astype(ref.dtype).reshape(ref.shape[0], rows.size, ref.shape[2])


def row_sum(value):
    return jnp.sum(value, axis=0, keepdims=True)


def gelu_pair(hidden):
    c0, c1 = 0.7978845608028654, 0.044715
    square = hidden * hidden
    tanh = jnp.tanh(c0 * hidden * (1.0 + c1 * square))
    half_up = 0.5 * (1.0 + tanh)
    slope = half_up + 0.5 * hidden * (1.0 - tanh * tanh) * (c0 * (1.0 + 3.0 * c1 * square))
    return hidden * half_up, slope


def normalize(rows):
    rows = rows.astype(F32)
    centered = rows - jnp.mean(rows, axis=-1, keepdims=True)
    inv_std = lax.rsqrt(jnp.mean(centered * centered, axis=-1, keepdims=True) + LN_EPS)
    return centered * inv_std, inv_std


def normalize_back(normed, inv_std, g_normed):
    mean_g = jnp.mean(g_normed, axis=-1, keepdims=True)
    mean_gn = jnp.mean(g_normed * normed, axis=-1, keepdims=True)
    return inv_std * (g_normed - mean_g - normed * mean_gn)


def softmax_of(scores):
    top = jnp.max(scores, axis=-1, keepdims=True)
    powers = jnp.exp(scores - top)
    return powers * (1.0 / jnp.sum(powers, axis=-1, keepdims=True))


def forward_body(tp_size, head_dim, *refs):
    at = Place(tp_size)
    take = cutter(refs)
    x, y, g, t_emb, table, lens, *bias_in = take(11)
    wqkv_in, wkv_in, wq_in, wo_in, wco_in = take(5)
    h1_out, y_out, x1_out, g_out = take(4)
    outs, scratch = take(9), take(9)
    qkv, kv, q_c, val, cval, prob, cprob, atot, x2 = scratch
    h1, x1, gm, mod, fh, fy, fx, fg, pbuf, sibr1, rcv1, sibr2, rcv2, wqkv, wkv, wq, wo, wco = take(18)
    gather_h, gather_y, gather_x, gather_g = [Gather(at, own, full, take(4)) for own, full in ((h1, fh), (y, fy), (x1, fx), (gm, fg))]
    scat_o, scat_c = [Scatter(at, pbuf, sibr, rcv, take(4)) for sibr, rcv in ((sibr1, rcv1), (sibr2, rcv2))]
    saves, out_sem = take(4), refs[-1]
    batch = x.shape[0]
    head_pad = wq.shape[0]
    bqkv, bkv, bq = [padded_bias(ref, head_dim, head_pad) for ref in bias_in[:3]]
    bo, bco = [row_of(ref) for ref in bias_in[3:]]
    scale = head_dim ** -0.5

    def out_copy(i):
        return pltpu.make_async_copy(scratch[i], outs[i], out_sem.at[i])

    at.greet_near()
    gather_y.start()
    fill_mod(mod, t_emb, table, (SHIFT1, SCALE1, GATE1, GATE2))

    def norm_one(b):
        shift, scale, _, gate = at_sample(mod, b)
        normed, _ = normalize(x[b])
        h1[b] = (normed * (1.0 + scale) + shift).astype(BF16)
        gm[b] = (g[b].astype(F32) * gate).astype(BF16)

    each(batch, norm_one)
    gather_h.start()
    for dest, source in ((wqkv, wqkv_in), (wkv, wkv_in), (wq, wq_in), (wo, wo_in), (wco, wco_in)):
        pad_rows(dest, source, head_dim)

    def hooks(s):
        for g in gather_h.groups_before(s):
            gather_h.group(g)
        gather_h.ready(s)
        if s in (3, 5):
            gather_y.group(s // 2 - 1)

    def project(slot):
        rows = gather_h.rows(slot)
        gather_h.save_copy(h1_out, saves[0], slot).start()
        put_rows(qkv, rows, dot(rows_of(fh, rows), wqkv, NT) + bqkv)

    loop_slots(at.ring, hooks, project)

    def hooks(b):
        if b == batch // 2:
            gather_y.group(2)
        if b == batch - 1:
            gather_y.group(3)

    def attend_self(b):
        q_b, k_b, v_b = [qkv[b, :, i * head_pad:(i + 1) * head_pad] for i in range(3)]
        p_b = softmax_of(dot(q_b, k_b, NT) * scale).astype(BF16)
        prob[b] = p_b
        val[b] = dot(p_b, v_b).astype(BF16)

    loop_slots(batch, hooks, attend_self)
    for i in (0, 3, 5):
        out_copy(i).start()

    def hooks(s):
        if s >= 2 and s % 2 == 0:
            scat_o.step(s // 2 - 1)
            gather_y.group(s // 2 + 3)
        if s == at.ring - 1:
            gather_g.start()

    def project_o(slot):
        scat_o.put(slot, dot(rows_of(val, scat_o.rows(slot)), wo))

    loop_slots(at.ring, hooks, project_o)
    scat_o.step(at.half - 1)

    def take_o(part, total):
        atot[part] = total + bo

    scat_o.final(take_o)
    out_copy(7).start()

    def x1_one(b):
        _, _, gate, _ = at_sample(mod, b)
        x1[b] = (x[b].astype(F32) + gate * atot[b]).astype(BF16)

    each(batch, x1_one)

    gather_x.start()

    def hooks(s):
        for g in gather_x.groups_before(s):
            gather_x.group(g)
        gather_y.ready(s)
        gather_x.ready(s)
        if s >= 2 and s % 2 == 0:
            gather_g.group(s // 2 - 1)

    def project(slot):
        rows = gather_x.rows(slot)
        gather_y.save_copy(y_out, saves[1], slot).start()
        gather_x.save_copy(x1_out, saves[2], slot).start()
        put_rows(kv, rows, dot(rows_of(fy, rows), wkv, NT) + bkv)
        put_rows(q_c, rows, dot(rows_of(fx, rows), wq, NT) + bq)

    loop_slots(at.ring, hooks, project)
    scat_o.finish()

    def hooks(b):
        if b == batch // 2:
            gather_g.group(3)
        if b == batch - 1:
            gather_g.group(4)

    def attend_cross(b):
        k_b, v_b = [kv[b, :, i * head_pad:(i + 1) * head_pad] for i in range(2)]
        scores = dot(q_c[b], k_b, NT) * scale
        slots = lax.broadcasted_iota(jnp.int32, scores.shape, 1)
        p_b = softmax_of(jnp.where(slots < lens[b], scores, MASK_FILL)).astype(BF16)
        cprob[b] = p_b
        cval[b] = dot(p_b, v_b).astype(BF16)

    loop_slots(batch, hooks, attend_cross)
    for i in (1, 2, 4, 6):
        out_copy(i).start()

    def save_g(slots):
        for slot in slots:
            gather_g.ready(slot)
            gather_g.save_copy(g_out, saves[3], slot).start()

    def hooks(s):
        if s >= 2 and s % 2 == 0:
            scat_c.step(s // 2 - 1)
        if s == 3:
            gather_g.group(5)
            save_g(range(3))
        if s == 5:
            gather_g.group(6)
            save_g((3, 4))

    def project_c(slot):
        scat_c.put(slot, dot(rows_of(cval, scat_c.rows(slot)), wco))

    loop_slots(at.ring, hooks, project_c)
    scat_c.step(at.half - 1)
    save_g(range(5, at.ring))

    def take_c(part, total):
        x2[part] = (x1[part].astype(F32) + total + bco).astype(BF16)

    scat_c.final(take_c)
    out_copy(8).start()
    for stream in (gather_h, gather_y, gather_x, gather_g, scat_c):
        stream.finish()
    for slot in range(at.ring):
        gather_h.save_copy(h1_out, saves[0], slot).wait()
        gather_y.save_copy(y_out, saves[1], slot).wait()
        gather_x.save_copy(x1_out, saves[2], slot).wait()
        gather_g.save_copy(g_out, saves[3], slot).wait()
    for i in range(9):
        out_copy(i).wait()


def forward_call(tp_size, cid, head_dim, head_pad, *ins):
    batch, n_loc, width = ins[0].shape
    n_tok = n_loc * tp_size
    ring, half = tp_size // 2, tp_size // 4
    tokens = lambda last: (batch, n_tok, last)
    local = (batch, n_loc, width)
    kept = [(tokens(3 * head_pad), BF16), (tokens(2 * head_pad), BF16), (tokens(head_pad), BF16), (tokens(head_pad), BF16),
            (tokens(head_pad), BF16), (tokens(n_tok), BF16), (tokens(n_tok), BF16), (local, F32), (local, BF16)]
    sib, rcv = (ring, *local), (2, half, *local)
    return pl.pallas_call(
        functools.partial(forward_body, tp_size, head_dim),
        out_shape=[jax.ShapeDtypeStruct(tokens(width), BF16)] * 4 + [jax.ShapeDtypeStruct(*k) for k in kept],
        in_specs=[VMEM] * 5 + [pl.BlockSpec(memory_space=pltpu.SMEM)] + [VMEM] * (len(ins) - 6),
        out_specs=[ANY] * (4 + len(kept)),
        scratch_shapes=[pltpu.VMEM(*k) for k in kept] + [
            *[pltpu.VMEM(local, BF16)] * 3, pltpu.VMEM((4, batch, width), F32), *[pltpu.VMEM(tokens(width), BF16)] * 4,
            pltpu.VMEM((ring, batch, 2 * n_loc, width), BF16),
            pltpu.VMEM(sib, BF16), pltpu.VMEM(rcv, BF16), pltpu.VMEM(sib, BF16), pltpu.VMEM(rcv, BF16)]
        + [pltpu.VMEM((n * head_pad, width), BF16) for n in (3, 2, 1, 1, 1)]
        + gather_sems(tp_size) * 4 + scatter_sems(tp_size) * 2
        + [pltpu.SemaphoreType.DMA((ring,))] * 4 + [pltpu.SemaphoreType.DMA((len(kept),))],
        compiler_params=KERNEL(collective_id=cid),
        name='attention_forward',
    )(*ins)


class RowFeed:
    def __init__(self, source, buf, sem, rows):
        self.source, self.buf, self.sem, self.rows = source, buf, sem, rows

    def copy(self, slot):
        side = lax.rem(slot, 2)
        return pltpu.make_async_copy(self.source.at[:, self.rows(slot), :], self.buf.at[side], self.sem.at[side])

    def take(self, slot, n):
        @pl.when(slot + 1 < n)
        def _():
            self.copy(slot + 1).start()
        self.copy(slot).wait()
        block = self.buf[lax.rem(slot, 2)]
        return block.reshape(block.shape[0] * block.shape[1], block.shape[2])


def small_total(at, src, got, mine, out, sems):
    send1, recv1, send2, recv2 = sems
    tiles = src.shape[1] // LANES

    def lanes(i):
        return pl.ds(i * LANES, LANES)

    def first(tile, peer_slot):
        return pltpu.make_async_remote_copy(
            src_ref=src.at[:, lanes(tile)], dst_ref=got.at[peer_slot], send_sem=send1.at[tile], recv_sem=recv1.at[peer_slot],
            device_id={'tp': tile}, device_id_type=MESH)

    def second(tile, d):
        return pltpu.make_async_remote_copy(
            src_ref=mine, dst_ref=out.at[:, lanes(tile)], send_sem=send2.at[d - 1], recv_sem=recv2.at[tile],
            device_id=at.other(d), device_id_type=MESH)

    for tile in range(tiles):
        @pl.when(at.me != tile)
        def _():
            first(tile, lax.rem(at.me - tile + at.tp_size, at.tp_size) - 1).start()
    for tile in range(tiles):
        @pl.when(at.me == tile)
        def _():
            total = src[:, tile * LANES:(tile + 1) * LANES]
            for d in range(1, at.tp_size):
                first(tile, d - 1).wait_recv()
                total = total + got[d - 1]
            mine[...] = total
            for d in range(1, at.tp_size):
                second(tile, d).start()
            out[:, tile * LANES:(tile + 1) * LANES] = total
            for d in range(1, at.tp_size):
                second(tile, d).wait_send()
    for tile in range(tiles):
        @pl.when(at.me != tile)
        def _():
            second(tile, 1).wait_recv()
            first(tile, 0).wait_send()


def backward_body(tp_size, head_dim, *refs):
    at = Place(tp_size)
    take = cutter(refs)
    g_cross, g_x2, x, x2, g, atot, t_emb, table, b2_in, w2, wqkv_in, wkv_in, wq_in, wo_in, wco_in, sums_in = take(16)
    b2 = row_of(b2_in)
    loads, feeds = take(8), take(3)
    x_out, g_x, g_y, sums_out = take(4)
    accs = take(8)
    gw_qkv, gw_kv, gw_q, gw_o, gw_co, gb_qkv, gb_kv, gb_q = accs
    held = take(8)
    qkv, kv, q_c, val, cval, prob, cprob, act_all = held
    full, pbuf, sibr1, rcv1, pbufy, sibr2, rcv2, wqkv, wkv, wq, wo, wco = take(12)
    g_val, g_qkv, g_kv, g_q, g_x1, g_h1, g_attn, mod, sums, got, mine, feed_a, feed_y = take(13)
    gather_c, gather_a = [Gather(at, own, full, take(4)) for own in (g_cross, g_attn)]
    near, far = (pbuf, sibr1, rcv1), (pbufy, sibr2, rcv2)
    scat_m, scat_q, scat_y, scat_h = [Scatter(at, *bufs, take(4)) for bufs in (far, near, far, near)]
    load_sem, *feed_sems = take(4)
    feed_h, feed_x, feed_yy = [
        RowFeed(source, buf, sem, scat.rows)
        for source, buf, sem, scat in zip(feeds, (feed_a, feed_a, feed_y), feed_sems, (scat_h, scat_q, scat_y))]
    batch, n_loc, width = x.shape
    ring, half = at.ring, at.half
    head_pad = wq.shape[0]
    scale = head_dim ** -0.5

    def load_copy(i):
        return pltpu.make_async_copy(loads[i], held[i], load_sem.at[i])

    for i in range(len(held)):
        load_copy(i).start()
    at.greet_all()
    gather_c.start()
    feed_x.copy(0).start()
    feed_yy.copy(0).start()
    fill_mod(mod, t_emb, table, (SHIFT1, SCALE1, GATE1, GATE2))
    for dest, source in ((wqkv, wqkv_in), (wkv, wkv_in), (wq, wq_in), (wo, wo_in), (wco, wco_in)):
        pad_rows(dest, source, head_dim)
    sums[...] = sums_in[...]
    clear(accs)
    for i in range(len(held)):
        load_copy(i).wait()

    def put_m(slot):
        scat_m.put(slot, dot(rows_of(act_all, scat_m.rows(slot)), w2))

    def out_back(gather, value, weight, acc, beside):
        def body(slot):
            rows = gather.rows(slot)
            block = rows_of(full, rows)
            put_rows(g_val, rows, dot(block, weight, NT))
            add_to(acc, dot(rows_of(value, rows), block, TN))
            beside(slot)
        return body

    def hooks(s):
        for g in gather_c.groups_before(s):
            gather_c.group(g)
        if s >= 2 and s % 2 == 0:
            scat_m.step(s // 2 - 1)
        gather_c.ready(s)

    loop_slots(ring, hooks, out_back(gather_c, cval, wco, gw_co, put_m))
    gather_c.finish()

    def back_one(q_b, k_b, v_b, p_b, g_b):
        g_p = dot(g_b, v_b, NT)
        p_f = p_b.astype(F32)
        row_dot = jnp.sum(g_p * p_f, axis=-1, keepdims=True)
        g_s = (p_f * (g_p - row_dot) * scale).astype(BF16)
        return dot(g_s, k_b).astype(BF16), dot(g_s, q_b, TN).astype(BF16), dot(p_b, g_b, TN).astype(BF16)

    def hooks(b):
        if b == batch // 2:
            scat_m.step(half - 1)

    def cross_back(b):
        parts = back_one(q_c[b], kv[b, :, :head_pad], kv[b, :, head_pad:], cprob[b], g_val[b])
        g_q[b] = parts[0]
        g_kv[b, :, :head_pad] = parts[1]
        g_kv[b, :, head_pad:] = parts[2]

    loop_slots(batch, hooks, cross_back)

    def hooks(s):
        if s >= 2 and s % 2 == 0:
            scat_q.step(s // 2 - 1)
        if s == 3:
            scat_m.final(take_m)
            scat_m.finish()

    def take_m(part, total):
        g_h1[part] = total + b2

    def put_q(slot):
        block = rows_of(g_q, scat_q.rows(slot))
        scat_q.put(slot, dot(block, wq))
        add_to(gw_q, dot(block, feed_x.take(slot, ring), TN))
        add_to(gb_q, row_sum(block.astype(F32)))

    def put_y(slot):
        block = rows_of(g_kv, scat_y.rows(slot))
        scat_y.put(slot, dot(block, wkv))
        add_to(gw_kv, dot(block, feed_yy.take(slot, ring), TN))
        add_to(gb_kv, row_sum(block.astype(F32)))

    loop_slots(ring, hooks, put_q)
    scat_q.step(half - 1)

    def out_one(b, gate_sum):
        gate, g_out, total = at_sample(mod, b)[-1], g[b].astype(F32), g_h1[b]
        x_out[b] = (x2[b].astype(F32) + gate * total).astype(BF16)
        return gate_sum + row_sum(g_out * total)

    zero = jnp.zeros((1, width), F32)
    sums[GATE2:GATE2 + 1, :] = lax.fori_loop(0, batch, out_one, zero)

    def take_q(part, total):
        g_x1[part] = g_x2[part] + total

    scat_q.final(take_q)
    feed_h.copy(0).start()

    def x1_back(b, carry):
        gate_sum, bias_sum = carry
        rows = g_x1[b]
        block = (rows * mod[2, pl.ds(b, 1), :]).astype(BF16)
        g_attn[b] = block
        return gate_sum + row_sum(rows * atot[b]), bias_sum + row_sum(block.astype(F32))

    gate_sum, bias_sum = lax.fori_loop(0, batch, x1_back, (zero, zero))
    for row, value in ((GATE1, gate_sum), (B_O, bias_sum)):
        sums[row:row + 1, :] = value

    scat_q.finish()
    gather_a.start()

    def hooks(s):
        for g in gather_a.groups_before(s):
            gather_a.group(g)
        if s >= 2 and s % 2 == 0:
            scat_y.step(s // 2 - 1)
        gather_a.ready(s)

    loop_slots(ring, hooks, out_back(gather_a, val, wo, gw_o, put_y))

    def hooks(b):
        if b == batch // 4:
            scat_y.step(half - 1)

    def self_back(b):
        parts = back_one(*[qkv[b, :, i * head_pad:(i + 1) * head_pad] for i in range(3)], prob[b], g_val[b])
        for i in range(3):
            g_qkv[b, :, i * head_pad:(i + 1) * head_pad] = parts[i]

    loop_slots(batch, hooks, self_back)

    def take_y(part, total):
        g_y[part] = total.astype(BF16)

    def hooks(s):
        if s >= 2 and s % 2 == 0:
            scat_h.step(s // 2 - 1)
        if s == 5:
            scat_y.final(take_y)

    def put_h(slot):
        block = rows_of(g_qkv, scat_h.rows(slot))
        scat_h.put(slot, dot(block, wqkv))
        add_to(gw_qkv, dot(block, feed_h.take(slot, ring), TN))
        add_to(gb_qkv, row_sum(block.astype(F32)))

    loop_slots(ring, hooks, put_h)
    scat_h.step(half - 1)
    def take_h(part, total):
        g_h1[part] = total

    scat_h.final(take_h)

    def x_back(b, carry):
        shift_sum, scale_sum = carry
        normed, inv_std = normalize(x[b])
        grad = g_h1[b]
        back = normalize_back(normed, inv_std, grad * (1.0 + mod[1, pl.ds(b, 1), :]))
        g_x[b] = (g_x1[b] + back).astype(BF16)
        return shift_sum + row_sum(grad), scale_sum + row_sum(grad * normed)

    shift_sum, scale_sum = lax.fori_loop(0, batch, x_back, (zero, zero))
    for row, value in ((SHIFT1, shift_sum), (SCALE1, scale_sum)):
        sums[row:row + 1, :] = value
    small_total(at, sums, got, mine, sums_out, take(4))
    for stream in (gather_a, scat_y, scat_h):
        stream.finish()


def backward_call(tp_size, cid, head_dim, head_pad, ins, loads, feeds):
    batch, n_loc, width = ins[0].shape
    n_tok = n_loc * tp_size
    ring, half = tp_size // 2, tp_size // 4
    n_sum = ins[-1].shape[0]
    tokens = lambda last: (batch, n_tok, last)
    local = (batch, n_loc, width)
    sib, rcv, pbuf = (ring, *local), (2, half, *local), (ring, batch, 2 * n_loc, width)
    outs = [(local, BF16)] * 3 + [((n_sum, width), F32)]
    outs += [((n * head_pad, width), F32) for n in (3, 2, 1, 1, 1)] + [((1, n * head_pad), F32) for n in (3, 2, 1)]
    return pl.pallas_call(
        functools.partial(backward_body, tp_size, head_dim),
        out_shape=[jax.ShapeDtypeStruct(*o) for o in outs],
        in_specs=[VMEM] * len(ins) + [ANY] * (len(loads) + len(feeds)),
        out_specs=[VMEM] * len(outs),
        scratch_shapes=[pltpu.VMEM(a.shape, a.dtype) for a in loads]
        + [pltpu.VMEM(s, BF16) for s in (tokens(width), pbuf, sib, rcv, pbuf, sib, rcv)]
        + [pltpu.VMEM((n * head_pad, width), BF16) for n in (3, 2, 1, 1, 1)]
        + [pltpu.VMEM(tokens(n * head_pad), BF16) for n in (1, 3, 2, 1)]
        + [pltpu.VMEM(local, F32), pltpu.VMEM(local, F32), pltpu.VMEM(local, BF16), pltpu.VMEM((4, batch, width), F32), pltpu.VMEM((n_sum, width), F32),
           pltpu.VMEM((tp_size - 1, n_sum, LANES), F32), pltpu.VMEM((n_sum, LANES), F32)]
        + [pltpu.VMEM((2, batch, 2 * n_loc, width), BF16)] * 2
        + gather_sems(tp_size) * 2 + scatter_sems(tp_size) * 4
        + [pltpu.SemaphoreType.DMA((len(loads),))] + [pltpu.SemaphoreType.DMA((2,))] * 3
        + [pltpu.SemaphoreType.DMA((n,)) for n in (width // LANES, tp_size - 1, tp_size - 1, width // LANES)],
        compiler_params=KERNEL(collective_id=cid),
        name='attention_backward',
    )(*ins, *loads, *feeds)


def mlp_body(tp_size, *refs):
    at = Place(tp_size)
    take = cutter(refs)
    x2, g, t_emb, table, b1_in, w1, w2, g_all = take(8)
    b1 = row_of(b1_in)
    act_all, g_x2, g_cross, sums, gw_1, gw_2, gb_1 = take(7)
    h2, mod, fh, hid_all, g_h2, feed, *bufs = take(9)
    gather_h, scat_h = Gather(at, h2, fh, take(4)), Scatter(at, *bufs, take(4))
    feed_g, feed_again = [RowFeed(g_all, feed, refs[-1], stream.rows) for stream in (gather_h, scat_h)]
    batch = x2.shape[0]

    feed_g.copy(0).start()
    at.greet_near()
    fill_mod(mod, t_emb, table, (SHIFT2, SCALE2, GATE2))

    def norm_one(b):
        shift, scale, _ = at_sample(mod, b)
        normed, _ = normalize(x2[b])
        h2[b] = (normed * (1.0 + scale) + shift).astype(BF16)

    each(batch, norm_one)
    gather_h.start()
    clear((gw_1, gw_2, gb_1, sums))

    def hooks(s):
        for group in gather_h.groups_before(s):
            gather_h.group(group)
        gather_h.ready(s)

    def mlp(slot):
        rows = gather_h.rows(slot)
        h2_blk, g_blk = rows_of(fh, rows), feed_g.take(slot, at.ring)
        act, slope = gelu_pair(dot(h2_blk, w1) + b1)
        act = act.astype(BF16)
        put_rows(act_all, rows, act)
        g_hidden = dot(g_blk, w2, NT) * slope
        add_to(gb_1, row_sum(g_hidden))
        g_hidden = g_hidden.astype(BF16)
        put_rows(hid_all, rows, g_hidden)

    loop_slots(at.ring, hooks, mlp)
    feed_again.copy(0).start()

    def hooks(s):
        if s >= 2 and s % 2 == 0:
            scat_h.step(s // 2 - 1)

    def put_h(slot):
        rows = scat_h.rows(slot)
        g_hidden = rows_of(hid_all, rows)
        scat_h.put(slot, dot(g_hidden, w1, NT))
        add_to(gw_1, dot(rows_of(fh, rows), g_hidden, TN))
        add_to(gw_2, dot(rows_of(act_all, rows), feed_again.take(slot, at.ring), TN))

    loop_slots(at.ring, hooks, put_h)
    scat_h.step(at.half - 1)

    def take_h(part, value):
        g_h2[part] = value

    scat_h.final(take_h)

    def back_one(b, carry):
        _, scale, gate = at_sample(mod, b)
        g_out, grad = g[b].astype(F32), g_h2[b]
        normed, inv_std = normalize(x2[b])
        back = g_out + normalize_back(normed, inv_std, grad * (1.0 + scale))
        g_x2[b] = back
        g_cross[b] = back.astype(BF16)
        terms = grad, grad * normed, back.astype(BF16).astype(F32), (g_out * gate).astype(BF16).astype(F32)
        return tuple(c + row_sum(t) for c, t in zip(carry, terms))

    zero = jnp.zeros((1, x2.shape[-1]), F32)
    found = lax.fori_loop(0, batch, back_one, (zero,) * 4)
    for row, value in zip((SHIFT2, SCALE2, B_CO, B_2), found):
        sums[row:row + 1, :] = value
    gather_h.finish()
    scat_h.finish()


def mlp_call(tp_size, cid, *ins):
    batch, n_loc, width = ins[0].shape
    ffn = ins[-2].shape[0]
    n_tok = n_loc * tp_size
    ring, half = tp_size // 2, tp_size // 4
    local, tokens, hidden = (batch, n_loc, width), (batch, n_tok, width), (batch, n_tok, ffn)
    chip = batch, 2 * n_loc, width
    outs = [(hidden, BF16), (local, F32), (local, BF16), ((SUM_ROWS, width), F32), ((width, ffn), F32), ((ffn, width), F32), ((1, ffn), F32)]
    scratch = [(local, BF16), ((3, batch, width), F32), (tokens, BF16), (hidden, BF16), (local, F32), ((2, *chip), BF16),
               ((ring, *chip), BF16), ((ring, *local), BF16), ((2, half, *local), BF16)]
    return pl.pallas_call(
        functools.partial(mlp_body, tp_size),
        out_shape=[jax.ShapeDtypeStruct(*o) for o in outs],
        in_specs=[VMEM] * (len(ins) - 1) + [ANY],
        out_specs=[VMEM] * len(outs),
        scratch_shapes=[pltpu.VMEM(*k) for k in scratch] + gather_sems(tp_size) + scatter_sems(tp_size) + [pltpu.SemaphoreType.DMA((2,))],
        compiler_params=KERNEL(collective_id=cid),
        name='mlp_both_ways',
    )(*ins)


def finish_body(head_dim, head_pad, n_head, n_bias, *refs):
    sources, results = refs[:len(refs) // 2], refs[len(refs) // 2:]
    for i, (source, result) in enumerate(zip(sources, results)):
        if i < n_head:
            for p in range(result.shape[0] // head_dim):
                result[p * head_dim:(p + 1) * head_dim, :] = source[p * head_pad:p * head_pad + head_dim, :].astype(result.dtype)
        elif i < n_head + n_bias:
            parts = [source[:, p:p + head_dim] for p in range(0, source.shape[1], head_pad)]
            result[...] = jnp.concatenate(parts, axis=1).astype(result.dtype)
        else:
            result[...] = source[...].astype(result.dtype)


def finish_call(head_dim, head_pad, padded, biases, plain):
    shapes = [(a.shape[0] // head_pad * head_dim, a.shape[1]) for a in padded]
    shapes += [(1, b.shape[1] // head_pad * head_dim) for b in biases] + [a.shape for a in plain]
    return pl.pallas_call(
        functools.partial(finish_body, head_dim, head_pad, len(padded), len(biases)),
        out_shape=[jax.ShapeDtypeStruct(shape, BF16) for shape in shapes],
        in_specs=[VMEM] * len(shapes),
        out_specs=[VMEM] * len(shapes),
        compiler_params=pltpu.CompilerParams(vmem_limit_bytes=60 * 1000 * 1000),
        name='results',
    )(*padded, *biases, *plain)


def device_block(tp_size, x_loc, y_loc, t_loc, len_loc, mod_table, w_qkv, b_qkv, w_o, b_o, w_q, b_q, w_kv, b_kv, w_co, b_co, w_1, b_1, w_2, b_2, g_loc):
    head_dim = w_q.shape[2]
    head_pad = -(-head_dim // LANES) * LANES
    wqkv, wq, wkv = [w.transpose(1, 2, 0)[0] for w in (w_qkv, w_q, w_kv)]
    wo, wco = w_o[0], w_co[0]

    h1_all, y_all, x1_all, g_all, qkv, kv, q_cross, attn_val, cross_val, attn_prob, cross_prob, attn_total, x2_loc = forward_call(
        tp_size, 0, head_dim, head_pad, x_loc, y_loc, g_loc, t_loc, mod_table, len_loc,
        b_qkv, b_kv, b_q, b_o, b_co, wqkv, wkv, wq, wo, wco)
    gelu_out, g_x2, g_cross, sums, g_w_1, g_w_2, g_b_1 = mlp_call(
        tp_size, 1, x2_loc, g_loc, t_loc, mod_table, b_1, w_1, w_2, g_all)
    x_out, g_x, g_y, sums, g_w_qkv, g_w_kv, g_w_q, g_w_o, g_w_co, g_b_qkv, g_b_kv, g_b_q = backward_call(
        tp_size, 2, head_dim, head_pad,
        [g_cross, g_x2, x_loc, x2_loc, g_loc, attn_total, t_loc, mod_table, b_2, w_2, wqkv, wkv, wq, wo, wco, sums],
        [qkv, kv, q_cross, attn_val, cross_val, attn_prob, cross_prob, gelu_out], [h1_all, x1_all, y_all])

    g_w_qkv, g_w_kv, g_w_q, g_w_o, g_w_co, g_b_qkv, g_b_kv, g_b_q, g_w_1, g_b_1, g_w_2, x_out, g_x, g_y = finish_call(
        head_dim, head_pad, [g_w_qkv, g_w_kv, g_w_q, g_w_o, g_w_co], [g_b_qkv, g_b_kv, g_b_q], [g_w_1, g_b_1, g_w_2, x_out, g_x, g_y])
    g_w_qkv, g_w_kv, g_w_q = [grad[None].transpose(2, 0, 1) for grad in (g_w_qkv, g_w_kv, g_w_q)]
    vectors = sums.astype(BF16)
    return (x_out, g_x, g_y, sums[:6], g_w_qkv, g_b_qkv, g_w_o[None], vectors[B_O], g_w_q, g_b_q, g_w_kv, g_b_kv,
            g_w_co[None], vectors[B_CO], g_w_1, g_b_1[0], g_w_2, vectors[B_2])


def solution(mesh):
    token, heads, rows, whole = P('dp', 'tp'), P(None, 'tp'), P('tp'), P()
    group, group_rows, group_heads = P('dp'), P(('dp', 'tp')), P('dp', 'tp')
    in_specs = (token, token, group, group, whole, heads, rows, rows, whole, heads, rows, heads, rows, rows, whole, heads, rows, rows, whole, token)
    out_specs = (token, token, token, group, group_heads, group_rows, group_rows, group, group_heads, group_rows, group_heads, group_rows,
                 group_rows, group, group_heads, group_rows, group_rows, group)
    return jax.shard_map(functools.partial(device_block, mesh.shape['tp']), mesh=mesh, in_specs=in_specs, out_specs=out_specs, check_vma=False)
```

```python
import functools
import itertools

import jax
import jax.numpy as jnp
from jax import lax
from jax.experimental import pallas as pl
from jax.experimental.pallas import tpu as pltpu
from jax.sharding import PartitionSpec as P

LN_EPS = 1e-6
MASK_FILL = -1e30
LANES = 128
MESH = pl.DeviceIdType.MESH
BF16 = jnp.bfloat16
F32 = jnp.float32
NN = (((1,), (0,)), ((), ()))
NT = (((1,), (1,)), ((), ()))
TN = (((0,), (0,)), ((), ()))
SHIFT1, SCALE1, GATE1, SHIFT2, SCALE2, GATE2, B_O, B_CO, B_2 = range(9)
SUM_ROWS = 16
LOADED = 19
UP, DOWN = HALVES = WAYS = 0, 1
SEND, TAKE = True, False
KERNEL = functools.partial(pltpu.CompilerParams, has_side_effects=True, vmem_limit_bytes=67 * 1000 * 1000)
VMEM, ANY = pl.BlockSpec(memory_space=pltpu.VMEM), pl.BlockSpec(memory_space=pl.ANY)


def dot(lhs, rhs, dims=NN):
    return lax.dot_general(lhs, rhs[...], dims, preferred_element_type=F32)


def add_to(acc, value):
    acc[...] += value


def clear(refs):
    for ref in refs:
        ref[...] = jnp.zeros_like(ref)


def each(n, body):
    def step(i, carry):
        body(i)
        return carry
    lax.fori_loop(0, n, step, None)


def cutter(refs):
    left = iter(refs)
    return lambda n: list(itertools.islice(left, n))


def padded_bias(ref, head_dim, head_pad):
    gap = jnp.zeros((1, head_pad - head_dim), F32)
    parts = [ref[:, p:p + head_dim].astype(F32) for p in range(0, ref.shape[1], head_dim)]
    return jnp.concatenate([piece for part in parts for piece in (part, gap)], axis=1)


def row_of(ref):
    return ref[...].astype(F32).reshape(1, -1)


class Place:
    def __init__(self, tp_size):
        self.tp_size = tp_size
        self.me = lax.axis_index('tp')
        self.ring, self.chip, self.core = tp_size // 2, self.me // 2, lax.rem(self.me, 2)
        self.half = self.ring // 2

    def wrap(self, zz):
        return lax.rem(zz + self.ring, self.ring)

    def sibling(self):
        return {'tp': self.chip * 2 + 1 - self.core}

    def ahead(self, sign):
        return {'tp': self.wrap(self.chip + sign) * 2 + self.core}

    def other(self, d):
        return {'tp': lax.rem(self.me + d, self.tp_size)}

    def greet(self, peers):
        barrier = pltpu.get_barrier_semaphore()
        for peer in peers:
            pl.semaphore_signal(barrier, device_id=peer, device_id_type=MESH)
        pl.semaphore_wait(barrier, len(peers))

    def greet_all(self):
        self.greet([self.other(d) for d in range(1, self.tp_size)])

    def greet_near(self):
        self.greet([self.ahead(1), self.ahead(-1), self.sibling()])


class Gather:
    def __init__(self, at, own, full, sems):
        self.at, self.own_ref, self.full = at, own, full
        self.rsend, self.rrecv, self.ssend, self.srecv = sems
        self.batch, self.n_loc = own.shape[0], own.shape[1]
        self.hb = self.batch // 2

    def part(self, zz, cc, ch):
        row = pl.multiple_of((zz * 2 + cc) * self.n_loc, self.n_loc)
        return self.full.at[pl.ds(ch * self.hb, self.hb), pl.ds(row, self.n_loc), :]

    def own(self, ch):
        return self.own_ref.at[pl.ds(ch * self.hb, self.hb)]

    def ring_copy(self, way, k, ch, sending):
        at = self.at
        sign = -1 if way == UP else 1
        zb = at.wrap(at.chip + sign * (k - 1 if sending else k))
        src = self.own(ch) if (sending and k == 1) else self.part(zb, at.core, ch)
        return pltpu.make_async_remote_copy(
            src_ref=src, dst_ref=self.part(zb, at.core, ch),
            send_sem=self.rsend.at[way, k - 1, ch], recv_sem=self.rrecv.at[way, k - 1, ch],
            device_id=at.ahead(-sign), device_id_type=MESH)

    def chip_at(self, slot):
        k = (slot + 1) // 2
        return self.at.wrap(self.at.chip - k) if slot % 2 else self.at.wrap(self.at.chip + k)

    def sib_copy(self, slot, ch, sending):
        at = self.at
        cc = at.core if sending else 1 - at.core
        zb = self.chip_at(slot)
        src = self.own(ch) if (sending and slot == 0) else self.part(zb, cc, ch)
        return pltpu.make_async_remote_copy(
            src_ref=src, dst_ref=self.part(zb, cc, ch),
            send_sem=self.ssend.at[slot, ch], recv_sem=self.srecv.at[slot, ch],
            device_id=at.sibling(), device_id_type=MESH)

    def carries(self, way, k, ch):
        return k < self.at.half or (k == self.at.half and ch == way)

    def slot_of(self, way, k):
        half = self.at.half
        return 2 * half - 1 if k == half else (2 * k - 1 if way == UP else 2 * k)

    def start(self):
        for way, ch in ((UP, 0), (DOWN, 1), (UP, 1), (DOWN, 0)):
            self.ring_copy(way, 1, ch, SEND).start()
        for ch in HALVES:
            self.sib_copy(0, ch, SEND).start()
        row = pl.multiple_of(self.at.me * self.n_loc, self.n_loc)
        self.full[:, pl.ds(row, self.n_loc), :] = self.own_ref[...]

    def arrive(self, way, k, ch):
        self.ring_copy(way, k, ch, TAKE).wait_recv()
        if self.carries(way, k + 1, ch):
            self.ring_copy(way, k + 1, ch, SEND).start()
        self.sib_copy(self.slot_of(way, k), ch, SEND).start()

    def group(self, g):
        k = g // 2 + 1
        first, second = ((UP, 0), (DOWN, 1)) if g % 2 == 0 else ((UP, 1), (DOWN, 0))
        self.arrive(first[0], k, first[1])
        self.arrive(second[0], k, second[1])

    def groups_before(self, slot):
        last = self.at.ring - 1
        return () if slot == last - 1 else ((last - 1,) if slot == last else (slot,))

    def ready(self, slot):
        for ch in HALVES:
            self.sib_copy(slot, ch, TAKE).wait_recv()

    def rows(self, slot):
        k = (slot + 1) // 2
        zz = self.at.wrap(self.at.chip + (1 - 2 * lax.rem(slot, 2)) * k)
        return pl.ds(pl.multiple_of(zz * 2 * self.n_loc, 2 * self.n_loc), 2 * self.n_loc)

    def save_copy(self, dest, sem, slot):
        rows = self.rows(slot)
        return pltpu.make_async_copy(self.full.at[:, rows, :], dest.at[:, rows, :], sem.at[slot])

    def finish(self):
        for way in WAYS:
            for k in range(1, self.at.half + 1):
                for ch in HALVES:
                    if self.carries(way, k, ch):
                        self.ring_copy(way, k, ch, SEND).wait_send()
        for slot in range(self.at.ring):
            for ch in HALVES:
                self.sib_copy(slot, ch, SEND).wait_send()


class Scatter:
    def __init__(self, at, pbuf, sibr, rcv, sems):
        self.at, self.pbuf, self.sibr, self.rcv = at, pbuf, sibr, rcv
        self.rsend, self.rrecv, self.ssend, self.srecv = sems
        self.batch, self.n_loc = sibr.shape[1], sibr.shape[2]
        self.hb = self.batch // 2

    def slot_of(self, way, s):
        return 0 if s == 0 else (2 * s - 1 if way == UP else 2 * s)

    def rows(self, slot):
        at = self.at
        away = at.half - (slot + 1) // 2
        zz = at.wrap(at.chip + (2 * lax.rem(slot, 2) - 1) * away)
        return pl.ds(pl.multiple_of(zz * 2 * self.n_loc, 2 * self.n_loc), 2 * self.n_loc)

    def put(self, slot, value):
        self.pbuf[slot] = value.astype(BF16).reshape(self.batch, 2 * self.n_loc, value.shape[-1])
        self.sib_copy(slot).start()

    def ring_copy(self, way, s, ch):
        part = pl.ds(ch * self.hb, self.hb)
        return pltpu.make_async_remote_copy(
            src_ref=self.sibr.at[self.slot_of(way, s), part], dst_ref=self.rcv.at[way, s, part],
            send_sem=self.rsend.at[way, s, ch], recv_sem=self.rrecv.at[way, s, ch],
            device_id=self.at.ahead(1 if way == UP else -1), device_id_type=MESH)

    def sib_copy(self, slot):
        rows = pl.ds(pl.multiple_of((1 - self.at.core) * self.n_loc, self.n_loc), self.n_loc)
        return pltpu.make_async_remote_copy(
            src_ref=self.pbuf.at[slot, :, rows, :], dst_ref=self.sibr.at[slot],
            send_sem=self.ssend.at[slot], recv_sem=self.srecv.at[slot],
            device_id=self.at.sibling(), device_id_type=MESH)

    def own_sum(self, slot, part):
        rows = pl.ds(pl.multiple_of(self.at.core * self.n_loc, self.n_loc), self.n_loc)
        return self.pbuf[slot, part, rows, :].astype(F32) + self.sibr[slot, part].astype(F32)

    def starts_at(self, way, ch):
        return 0 if ch == way else 1

    def pass_on(self, way, s, ch):
        slot, part = self.slot_of(way, s), pl.ds(ch * self.hb, self.hb)
        total = self.own_sum(slot, part)
        if s > self.starts_at(way, ch):
            self.ring_copy(way, s - 1, ch).wait_recv()
            total = total + self.rcv[way, s - 1, part].astype(F32)
        self.sibr[slot, part] = total.astype(BF16)
        self.ring_copy(way, s, ch).start()

    def step(self, s):
        if s == 0:
            self.sib_copy(0).wait_recv()
            self.pass_on(UP, 0, 0)
            self.pass_on(DOWN, 0, 1)
            return
        self.sib_copy(2 * s - 1).wait_recv()
        self.pass_on(UP, s, 1)
        self.sib_copy(2 * s).wait_recv()
        self.pass_on(DOWN, s, 0)
        self.pass_on(UP, s, 0)
        self.pass_on(DOWN, s, 1)

    def final(self, use):
        last = self.at.ring - 1
        self.sib_copy(last).wait_recv()
        for ch, order in ((1, (UP, DOWN)), (0, (DOWN, UP))):
            part = pl.ds(ch * self.hb, self.hb)
            total = self.own_sum(last, part)
            for way in order:
                self.ring_copy(way, self.at.half - 1, ch).wait_recv()
                total = total + self.rcv[way, self.at.half - 1, part].astype(F32)
            use(part, total)

    def finish(self):
        for way in WAYS:
            for s in range(self.at.half):
                for ch in HALVES:
                    if s >= self.starts_at(way, ch):
                        self.ring_copy(way, s, ch).wait_send()
        for slot in range(self.at.ring):
            self.sib_copy(slot).wait_send()


def loop_slots(n, hooks, body):
    def step(slot):
        for s in range(n):
            @pl.when(slot == s)
            def _():
                hooks(s)
        body(slot)
    each(n, step)


def gather_sems(tp_size):
    ring, half = tp_size // 2, tp_size // 4
    return [pltpu.SemaphoreType.DMA(s) for s in ((2, half, 2), (2, half, 2), (ring, 2), (ring, 2))]


def scatter_sems(tp_size):
    ring, half = tp_size // 2, tp_size // 4
    return [pltpu.SemaphoreType.DMA(s) for s in ((2, half, 2), (2, half, 2), (ring,), (ring,))]


def pad_rows(dest, source, head_dim):
    parts = source.shape[0] // head_dim
    head_pad = dest.shape[0] // parts
    width = dest.shape[1]
    for i in range(parts):
        dest[i * head_pad:i * head_pad + head_dim, :] = source[i * head_dim:(i + 1) * head_dim, :]
        dest[i * head_pad + head_dim:(i + 1) * head_pad, :] = jnp.zeros((head_pad - head_dim, width), dest.dtype)


def at_sample(mod, b):
    return [mod[i, pl.ds(b, 1), :] for i in range(mod.shape[0])]


def fill_mod(mod, t_ref, table_ref, rows):
    for i, row in enumerate(rows):
        mod[i] = mod_row(t_ref, table_ref, row)


def mod_row(t_ref, table_ref, i):
    width = table_ref.shape[1]
    return table_ref[i:i + 1, :].astype(F32) + t_ref[:, i * width:(i + 1) * width].astype(F32)


def rows_of(ref, rows):
    block = ref[:, rows, :]
    return block.reshape(block.shape[0] * block.shape[1], block.shape[2])


def put_rows(ref, rows, value):
    ref[:, rows, :] = value.astype(ref.dtype).reshape(ref.shape[0], rows.size, ref.shape[2])


def row_sum(value):
    return jnp.sum(value, axis=0, keepdims=True)


def gelu_pair(hidden):
    c0, c1 = 0.7978845608028654, 0.044715
    square = hidden * hidden
    tanh = jnp.tanh(c0 * hidden * (1.0 + c1 * square))
    half_up = 0.5 * (1.0 + tanh)
    slope = half_up + 0.5 * hidden * (1.0 - tanh * tanh) * (c0 * (1.0 + 3.0 * c1 * square))
    return hidden * half_up, slope


def normalize(rows):
    rows = rows.astype(F32)
    centered = rows - jnp.mean(rows, axis=-1, keepdims=True)
    inv_std = lax.rsqrt(jnp.mean(centered * centered, axis=-1, keepdims=True) + LN_EPS)
    return centered * inv_std, inv_std


def normalize_back(normed, inv_std, g_normed):
    mean_g = jnp.mean(g_normed, axis=-1, keepdims=True)
    mean_gn = jnp.mean(g_normed * normed, axis=-1, keepdims=True)
    return inv_std * (g_normed - mean_g - normed * mean_gn)


def softmax_of(scores):
    top = jnp.max(scores, axis=-1, keepdims=True)
    powers = jnp.exp(scores - top)
    return powers * (1.0 / jnp.sum(powers, axis=-1, keepdims=True))


def forward_body(tp_size, head_dim, *refs):
    at = Place(tp_size)
    take = cutter(refs)
    x, y, g, t_emb, table, lens, *bias_in = take(11)
    wqkv_in, wkv_in, wq_in, wo_in, wco_in = take(5)
    h1_out, y_out, x1_out, g_out = take(4)
    outs, scratch = take(9), take(9)
    qkv, kv, q_c, val, cval, prob, cprob, atot, x2 = scratch
    h1, x1, gm, mod, fh, fy, fx, fg, pbuf, sibr1, rcv1, sibr2, rcv2, wqkv, wkv, wq, wo, wco = take(18)
    gather_h, gather_y, gather_x, gather_g = [Gather(at, own, full, take(4)) for own, full in ((h1, fh), (y, fy), (x1, fx), (gm, fg))]
    scat_o, scat_c = [Scatter(at, pbuf, sibr, rcv, take(4)) for sibr, rcv in ((sibr1, rcv1), (sibr2, rcv2))]
    saves, out_sem = take(4), refs[-1]
    batch = x.shape[0]
    head_pad = wq.shape[0]
    bqkv, bkv, bq = [padded_bias(ref, head_dim, head_pad) for ref in bias_in[:3]]
    bo, bco = [row_of(ref) for ref in bias_in[3:]]
    scale = head_dim ** -0.5

    def out_copy(i):
        return pltpu.make_async_copy(scratch[i], outs[i], out_sem.at[i])

    at.greet_near()
    gather_y.start()
    fill_mod(mod, t_emb, table, (SHIFT1, SCALE1, GATE1, GATE2))

    def norm_one(b):
        shift, scale, _, gate = at_sample(mod, b)
        normed, _ = normalize(x[b])
        h1[b] = (normed * (1.0 + scale) + shift).astype(BF16)
        gm[b] = (g[b].astype(F32) * gate).astype(BF16)

    each(batch, norm_one)
    gather_h.start()
    for dest, source in ((wqkv, wqkv_in), (wkv, wkv_in), (wq, wq_in), (wo, wo_in), (wco, wco_in)):
        pad_rows(dest, source, head_dim)

    def hooks(s):
        for g in gather_h.groups_before(s):
            gather_h.group(g)
        gather_h.ready(s)
        if s in (3, 5):
            gather_y.group(s // 2 - 1)

    def project(slot):
        rows = gather_h.rows(slot)
        gather_h.save_copy(h1_out, saves[0], slot).start()
        put_rows(qkv, rows, dot(rows_of(fh, rows), wqkv, NT) + bqkv)

    loop_slots(at.ring, hooks, project)

    def hooks(b):
        if b == batch // 2:
            gather_y.group(2)
        if b == batch - 1:
            gather_y.group(3)

    def attend_self(b):
        q_b, k_b, v_b = [qkv[b, :, i * head_pad:(i + 1) * head_pad] for i in range(3)]
        p_b = softmax_of(dot(q_b, k_b, NT) * scale).astype(BF16)
        prob[b] = p_b
        val[b] = dot(p_b, v_b).astype(BF16)

    loop_slots(batch, hooks, attend_self)
    for i in (0, 3, 5):
        out_copy(i).start()

    def hooks(s):
        if s >= 2 and s % 2 == 0:
            scat_o.step(s // 2 - 1)
            gather_y.group(s // 2 + 3)
        if s == at.ring - 1:
            gather_g.start()

    def project_o(slot):
        scat_o.put(slot, dot(rows_of(val, scat_o.rows(slot)), wo))

    loop_slots(at.ring, hooks, project_o)
    scat_o.step(at.half - 1)

    def take_o(part, total):
        atot[part] = total + bo

    scat_o.final(take_o)
    out_copy(7).start()

    def x1_one(b):
        _, _, gate, _ = at_sample(mod, b)
        x1[b] = (x[b].astype(F32) + gate * atot[b]).astype(BF16)

    each(batch, x1_one)

    gather_x.start()

    def hooks(s):
        for g in gather_x.groups_before(s):
            gather_x.group(g)
        gather_y.ready(s)
        gather_x.ready(s)
        if s >= 2 and s % 2 == 0:
            gather_g.group(s // 2 - 1)

    def project(slot):
        rows = gather_x.rows(slot)
        gather_y.save_copy(y_out, saves[1], slot).start()
        gather_x.save_copy(x1_out, saves[2], slot).start()
        put_rows(kv, rows, dot(rows_of(fy, rows), wkv, NT) + bkv)
        put_rows(q_c, rows, dot(rows_of(fx, rows), wq, NT) + bq)

    loop_slots(at.ring, hooks, project)
    scat_o.finish()

    def hooks(b):
        if b == batch // 2:
            gather_g.group(3)
        if b == batch - 1:
            gather_g.group(4)

    def attend_cross(b):
        k_b, v_b = [kv[b, :, i * head_pad:(i + 1) * head_pad] for i in range(2)]
        scores = dot(q_c[b], k_b, NT) * scale
        slots = lax.broadcasted_iota(jnp.int32, scores.shape, 1)
        p_b = softmax_of(jnp.where(slots < lens[b], scores, MASK_FILL)).astype(BF16)
        cprob[b] = p_b
        cval[b] = dot(p_b, v_b).astype(BF16)

    loop_slots(batch, hooks, attend_cross)
    for i in (1, 2, 4, 6):
        out_copy(i).start()

    def save_g(slots):
        for slot in slots:
            gather_g.ready(slot)
            gather_g.save_copy(g_out, saves[3], slot).start()

    def hooks(s):
        if s >= 2 and s % 2 == 0:
            scat_c.step(s // 2 - 1)
        if s == 3:
            gather_g.group(5)
            save_g(range(3))
        if s == 5:
            gather_g.group(6)
            save_g((3, 4))

    def project_c(slot):
        scat_c.put(slot, dot(rows_of(cval, scat_c.rows(slot)), wco))

    loop_slots(at.ring, hooks, project_c)
    scat_c.step(at.half - 1)
    save_g(range(5, at.ring))

    def take_c(part, total):
        x2[part] = (x1[part].astype(F32) + total + bco).astype(BF16)

    scat_c.final(take_c)
    out_copy(8).start()
    for stream in (gather_h, gather_y, gather_x, gather_g, scat_c):
        stream.finish()
    for slot in range(at.ring):
        gather_h.save_copy(h1_out, saves[0], slot).wait()
        gather_y.save_copy(y_out, saves[1], slot).wait()
        gather_x.save_copy(x1_out, saves[2], slot).wait()
        gather_g.save_copy(g_out, saves[3], slot).wait()
    for i in range(9):
        out_copy(i).wait()


def forward_call(tp_size, cid, head_dim, head_pad, *ins):
    batch, n_loc, width = ins[0].shape
    n_tok = n_loc * tp_size
    ring, half = tp_size // 2, tp_size // 4
    tokens = lambda last: (batch, n_tok, last)
    local = (batch, n_loc, width)
    kept = [(tokens(3 * head_pad), BF16), (tokens(2 * head_pad), BF16), (tokens(head_pad), BF16), (tokens(head_pad), BF16),
            (tokens(head_pad), BF16), (tokens(n_tok), BF16), (tokens(n_tok), BF16), (local, F32), (local, BF16)]
    sib, rcv = (ring, *local), (2, half, *local)
    return pl.pallas_call(
        functools.partial(forward_body, tp_size, head_dim),
        out_shape=[jax.ShapeDtypeStruct(tokens(width), BF16)] * 4 + [jax.ShapeDtypeStruct(*k) for k in kept],
        in_specs=[VMEM] * 5 + [pl.BlockSpec(memory_space=pltpu.SMEM)] + [VMEM] * (len(ins) - 6),
        out_specs=[ANY] * (4 + len(kept)),
        scratch_shapes=[pltpu.VMEM(*k) for k in kept] + [
            *[pltpu.VMEM(local, BF16)] * 3, pltpu.VMEM((4, batch, width), F32), *[pltpu.VMEM(tokens(width), BF16)] * 4,
            pltpu.VMEM((ring, batch, 2 * n_loc, width), BF16),
            pltpu.VMEM(sib, BF16), pltpu.VMEM(rcv, BF16), pltpu.VMEM(sib, BF16), pltpu.VMEM(rcv, BF16)]
        + [pltpu.VMEM((n * head_pad, width), BF16) for n in (3, 2, 1, 1, 1)]
        + gather_sems(tp_size) * 4 + scatter_sems(tp_size) * 2
        + [pltpu.SemaphoreType.DMA((ring,))] * 4 + [pltpu.SemaphoreType.DMA((len(kept),))],
        compiler_params=KERNEL(collective_id=cid),
        name='attention_forward',
    )(*ins)


class Emit:
    def __init__(self, acc, stage, dest, sem):
        self.acc, self.stage = acc, stage
        self.copy = pltpu.make_async_copy(stage, dest, sem)

    def start(self, head_dim, head_pad):
        for p in range(self.stage.shape[0] // head_dim):
            self.stage[p * head_dim:(p + 1) * head_dim, :] = self.acc[p * head_pad:p * head_pad + head_dim, :].astype(BF16)
        self.copy.start()


class RowFeed:
    def __init__(self, source, buf, sem, rows):
        self.source, self.buf, self.sem, self.rows = source, buf, sem, rows

    def copy(self, slot):
        side = lax.rem(slot, 2)
        return pltpu.make_async_copy(self.source.at[:, self.rows(slot), :], self.buf.at[side], self.sem.at[side])

    def take(self, slot, n):
        @pl.when(slot + 1 < n)
        def _():
            self.copy(slot + 1).start()
        self.copy(slot).wait()
        block = self.buf[lax.rem(slot, 2)]
        return block.reshape(block.shape[0] * block.shape[1], block.shape[2])


def small_total(at, src, got, mine, out, sems, between):
    send1, recv1, send2, recv2 = sems
    tiles = src.shape[1] // LANES

    def lanes(i):
        return pl.ds(i * LANES, LANES)

    def first(tile, peer_slot):
        return pltpu.make_async_remote_copy(
            src_ref=src.at[:, lanes(tile)], dst_ref=got.at[peer_slot], send_sem=send1.at[tile], recv_sem=recv1.at[peer_slot],
            device_id={'tp': tile}, device_id_type=MESH)

    def second(tile, d):
        return pltpu.make_async_remote_copy(
            src_ref=mine, dst_ref=out.at[:, lanes(tile)], send_sem=send2.at[d - 1], recv_sem=recv2.at[tile],
            device_id=at.other(d), device_id_type=MESH)

    for tile in range(tiles):
        @pl.when(at.me != tile)
        def _():
            first(tile, lax.rem(at.me - tile + at.tp_size, at.tp_size) - 1).start()
    between()
    for tile in range(tiles):
        @pl.when(at.me == tile)
        def _():
            total = src[:, tile * LANES:(tile + 1) * LANES]
            for d in range(1, at.tp_size):
                first(tile, d - 1).wait_recv()
                total = total + got[d - 1]
            mine[...] = total
            for d in range(1, at.tp_size):
                second(tile, d).start()
            out[:, tile * LANES:(tile + 1) * LANES] = total
            for d in range(1, at.tp_size):
                second(tile, d).wait_send()
    for tile in range(tiles):
        @pl.when(at.me != tile)
        def _():
            second(tile, 1).wait_recv()
            first(tile, 0).wait_send()


def backward_body(tp_size, head_dim, *refs):
    at = Place(tp_size)
    take = cutter(refs)
    g_cross, t_emb, table, b2_in, sums_in = take(5)
    b2 = row_of(b2_in)
    loads, feeds = take(LOADED), take(3)
    x_out, g_x, g_y, sums_out, gb_qkv, gb_kv, gb_q = take(7)
    dests, held = take(5), take(LOADED)
    wqkv_in, wkv_in, wq_in, wo_in, wco_in, w2, act_all, cval, q_c, kv, cprob, g_x2, x, x2, g, atot, val, qkv, prob = held
    accs, stages = take(5), take(5)
    gw_qkv, gw_kv, gw_q, gw_o, gw_co = accs
    full, pbuf, sibr1, rcv1, pbufy, sibr2, rcv2, wqkv, wkv, wq, wo, wco = take(12)
    g_val, g_qkv, g_kv, g_q, g_x1, g_h1, g_attn, mod, sums, got, mine, feed_a, feed_y = take(13)
    gather_c, gather_a = [Gather(at, own, full, take(4)) for own in (g_cross, g_attn)]
    near, far = (pbuf, sibr1, rcv1), (pbufy, sibr2, rcv2)
    scat_m, scat_q, scat_y, scat_h = [Scatter(at, *bufs, take(4)) for bufs in (far, near, far, near)]
    load_sem, emit_sem, *feed_sems = take(5)
    emits = [Emit(*e, emit_sem.at[i]) for i, e in enumerate(zip(accs, stages, dests))]
    emit_qkv, emit_kv, emit_q, emit_o, emit_co = [functools.partial(e.start, head_dim, wq.shape[0]) for e in emits]
    feed_h, feed_x, feed_yy = [
        RowFeed(source, buf, sem, scat.rows)
        for source, buf, sem, scat in zip(feeds, (feed_a, feed_a, feed_y), feed_sems, (scat_h, scat_q, scat_y))]
    batch, _, width = x.shape
    ring, half = at.ring, at.half
    head_pad = wq.shape[0]
    scale = head_dim ** -0.5

    def load_copy(i):
        return pltpu.make_async_copy(loads[i], held[i], load_sem.at[i])

    for i in range(len(held)):
        load_copy(i).start()
    at.greet_all()
    gather_c.start()
    feed_x.copy(0).start()
    feed_yy.copy(0).start()
    fill_mod(mod, t_emb, table, (SHIFT1, SCALE1, GATE1, GATE2))
    sums[...] = sums_in[...]
    clear((*accs, gb_qkv, gb_kv, gb_q))
    for i in range(len(held)):
        load_copy(i).wait()
    for dest, source in zip((wqkv, wkv, wq, wo, wco), held):
        pad_rows(dest, source, head_dim)

    def put_m(slot):
        scat_m.put(slot, dot(rows_of(act_all, scat_m.rows(slot)), w2))

    def out_back(gather, value, weight, acc, beside):
        def body(slot):
            rows = gather.rows(slot)
            block = rows_of(full, rows)
            put_rows(g_val, rows, dot(block, weight, NT))
            add_to(acc, dot(rows_of(value, rows), block, TN))
            beside(slot)
        return body

    def hooks(s):
        for g in gather_c.groups_before(s):
            gather_c.group(g)
        if s >= 2 and s % 2 == 0:
            scat_m.step(s // 2 - 1)
        gather_c.ready(s)

    loop_slots(ring, hooks, out_back(gather_c, cval, wco, gw_co, put_m))
    gather_c.finish()
    emit_co()

    def back_one(q_b, k_b, v_b, p_b, g_b):
        g_p = dot(g_b, v_b, NT)
        p_f = p_b.astype(F32)
        row_dot = jnp.sum(g_p * p_f, axis=-1, keepdims=True)
        g_s = (p_f * (g_p - row_dot) * scale).astype(BF16)
        return dot(g_s, k_b).astype(BF16), dot(g_s, q_b, TN).astype(BF16), dot(p_b, g_b, TN).astype(BF16)

    def hooks(b):
        if b == batch // 2:
            scat_m.step(half - 1)

    def cross_back(b):
        parts = back_one(q_c[b], kv[b, :, :head_pad], kv[b, :, head_pad:], cprob[b], g_val[b])
        g_q[b] = parts[0]
        g_kv[b, :, :head_pad] = parts[1]
        g_kv[b, :, head_pad:] = parts[2]

    loop_slots(batch, hooks, cross_back)

    def hooks(s):
        if s >= 2 and s % 2 == 0:
            scat_q.step(s // 2 - 1)
        if s == 3:
            scat_m.final(take_m)
            scat_m.finish()

    def take_m(part, total):
        g_h1[part] = total + b2

    def put_q(slot):
        block = rows_of(g_q, scat_q.rows(slot))
        scat_q.put(slot, dot(block, wq))
        add_to(gw_q, dot(block, feed_x.take(slot, ring), TN))
        add_to(gb_q, row_sum(block.astype(F32)))

    def put_y(slot):
        block = rows_of(g_kv, scat_y.rows(slot))
        scat_y.put(slot, dot(block, wkv))
        add_to(gw_kv, dot(block, feed_yy.take(slot, ring), TN))
        add_to(gb_kv, row_sum(block.astype(F32)))

    loop_slots(ring, hooks, put_q)
    scat_q.step(half - 1)
    emit_q()

    def out_one(b, gate_sum):
        gate, g_out, total = at_sample(mod, b)[-1], g[b].astype(F32), g_h1[b]
        x_out[b] = (x2[b].astype(F32) + gate * total).astype(BF16)
        return gate_sum + row_sum(g_out * total)

    zero = jnp.zeros((1, width), F32)
    sums[GATE2:GATE2 + 1, :] = lax.fori_loop(0, batch, out_one, zero)

    def take_q(part, total):
        g_x1[part] = g_x2[part] + total

    scat_q.final(take_q)
    feed_h.copy(0).start()

    def x1_back(b, carry):
        gate_sum, bias_sum = carry
        rows = g_x1[b]
        block = (rows * mod[2, pl.ds(b, 1), :]).astype(BF16)
        g_attn[b] = block
        return gate_sum + row_sum(rows * atot[b]), bias_sum + row_sum(block.astype(F32))

    gate_sum, bias_sum = lax.fori_loop(0, batch, x1_back, (zero, zero))
    for row, value in ((GATE1, gate_sum), (B_O, bias_sum)):
        sums[row:row + 1, :] = value

    scat_q.finish()
    gather_a.start()

    def hooks(s):
        for g in gather_a.groups_before(s):
            gather_a.group(g)
        if s >= 2 and s % 2 == 0:
            scat_y.step(s // 2 - 1)
        gather_a.ready(s)

    loop_slots(ring, hooks, out_back(gather_a, val, wo, gw_o, put_y))

    def hooks(b):
        if b == batch // 4:
            scat_y.step(half - 1)

    def self_back(b):
        parts = back_one(*[qkv[b, :, i * head_pad:(i + 1) * head_pad] for i in range(3)], prob[b], g_val[b])
        for i in range(3):
            g_qkv[b, :, i * head_pad:(i + 1) * head_pad] = parts[i]

    loop_slots(batch, hooks, self_back)
    emit_kv()
    emit_o()

    def take_y(part, total):
        g_y[part] = total.astype(BF16)

    def hooks(s):
        if s >= 2 and s % 2 == 0:
            scat_h.step(s // 2 - 1)
        if s == 5:
            scat_y.final(take_y)

    def put_h(slot):
        block = rows_of(g_qkv, scat_h.rows(slot))
        scat_h.put(slot, dot(block, wqkv))
        add_to(gw_qkv, dot(block, feed_h.take(slot, ring), TN))
        add_to(gb_qkv, row_sum(block.astype(F32)))

    loop_slots(ring, hooks, put_h)
    scat_h.step(half - 1)
    emit_qkv()

    def take_h(part, total):
        g_h1[part] = total

    scat_h.final(take_h)

    def sums_one(b, carry):
        shift_sum, scale_sum = carry
        normed, _ = normalize(x[b])
        return shift_sum + row_sum(g_h1[b]), scale_sum + row_sum(g_h1[b] * normed)

    def x_one(b):
        normed, inv_std = normalize(x[b])
        _, scale, *_ = at_sample(mod, b)
        back = normalize_back(normed, inv_std, g_h1[b] * (1.0 + scale))
        g_x[b] = (g_x1[b] + back).astype(BF16)

    shift_sum, scale_sum = lax.fori_loop(0, batch, sums_one, (zero, zero))
    for row, value in ((SHIFT1, shift_sum), (SCALE1, scale_sum)):
        sums[row:row + 1, :] = value
    small_total(at, sums, got, mine, sums_out, take(4), lambda: each(batch, x_one))
    for stream in (gather_a, scat_y, scat_h):
        stream.finish()
    for emit in emits:
        emit.copy.wait()


def backward_call(tp_size, cid, head_dim, head_pad, ins, loads, feeds):
    batch, n_loc, width = ins[0].shape
    n_tok = n_loc * tp_size
    ring, half = tp_size // 2, tp_size // 4
    tokens = lambda last: (batch, n_tok, last)
    local = (batch, n_loc, width)
    sib, rcv, pbuf = (ring, *local), (2, half, *local), (ring, batch, 2 * n_loc, width)
    parts = 3, 2, 1, 1, 1
    outs = [(local, BF16)] * 3 + [((SUM_ROWS, width), F32)] + [((1, n * head_pad), F32) for n in parts[:3]]
    grads = [((n * head_dim, width), BF16) for n in parts]
    return pl.pallas_call(
        functools.partial(backward_body, tp_size, head_dim),
        out_shape=[jax.ShapeDtypeStruct(*o) for o in outs + grads],
        in_specs=[VMEM] * len(ins) + [ANY] * (len(loads) + len(feeds)),
        out_specs=[VMEM] * len(outs) + [ANY] * len(grads),
        scratch_shapes=[pltpu.VMEM(a.shape, a.dtype) for a in loads]
        + [pltpu.VMEM((n * head_pad, width), F32) for n in parts] + [pltpu.VMEM(*g) for g in grads]
        + [pltpu.VMEM(s, BF16) for s in (tokens(width), pbuf, sib, rcv, pbuf, sib, rcv)]
        + [pltpu.VMEM((n * head_pad, width), BF16) for n in parts]
        + [pltpu.VMEM(tokens(n * head_pad), BF16) for n in (1, 3, 2, 1)]
        + [pltpu.VMEM(local, F32), pltpu.VMEM(local, F32), pltpu.VMEM(local, BF16), pltpu.VMEM((4, batch, width), F32), pltpu.VMEM((SUM_ROWS, width), F32),
           pltpu.VMEM((tp_size - 1, SUM_ROWS, LANES), F32), pltpu.VMEM((SUM_ROWS, LANES), F32)]
        + [pltpu.VMEM((2, batch, 2 * n_loc, width), BF16)] * 2
        + gather_sems(tp_size) * 2 + scatter_sems(tp_size) * 4
        + [pltpu.SemaphoreType.DMA((len(loads),)), pltpu.SemaphoreType.DMA((len(grads),))] + [pltpu.SemaphoreType.DMA((2,))] * 3
        + [pltpu.SemaphoreType.DMA((n,)) for n in (width // LANES, tp_size - 1, tp_size - 1, width // LANES)],
        compiler_params=KERNEL(collective_id=cid),
        name='attention_backward',
    )(*ins, *loads, *feeds)


def mlp_body(tp_size, *refs):
    at = Place(tp_size)
    take = cutter(refs)
    x2, g, t_emb, table, b1_in, w1, w2, g_all = take(8)
    b1 = row_of(b1_in)
    g_x2, g_cross, sums, gb_1, act_out, *dests = take(7)
    h2, mod, fh, hid_all, g_h2, feed, act_all, gw_1, gw_2, *stages = take(11)
    bufs = take(3)
    gather_h, scat_h = Gather(at, h2, fh, take(4)), Scatter(at, *bufs, take(4))
    act_sem, *emit_sems = take(3)
    act_copy = pltpu.make_async_copy(act_all, act_out, act_sem)
    emits = [Emit(*e) for e in zip((gw_1, gw_2), stages, dests, emit_sems)]
    feed_g, feed_again = [RowFeed(g_all, feed, refs[-1], stream.rows) for stream in (gather_h, scat_h)]
    batch = x2.shape[0]

    feed_g.copy(0).start()
    at.greet_near()
    fill_mod(mod, t_emb, table, (SHIFT2, SCALE2, GATE2))

    def norm_one(b):
        shift, scale, _ = at_sample(mod, b)
        normed, _ = normalize(x2[b])
        h2[b] = (normed * (1.0 + scale) + shift).astype(BF16)

    each(batch, norm_one)
    gather_h.start()
    clear((gw_1, gw_2, gb_1, sums))

    def hooks(s):
        for group in gather_h.groups_before(s):
            gather_h.group(group)
        gather_h.ready(s)

    def mlp(slot):
        rows = gather_h.rows(slot)
        h2_blk, g_blk = rows_of(fh, rows), feed_g.take(slot, at.ring)
        act, slope = gelu_pair(dot(h2_blk, w1) + b1)
        act = act.astype(BF16)
        put_rows(act_all, rows, act)
        g_hidden = dot(g_blk, w2, NT) * slope
        add_to(gb_1, row_sum(g_hidden))
        g_hidden = g_hidden.astype(BF16)
        put_rows(hid_all, rows, g_hidden)

    loop_slots(at.ring, hooks, mlp)
    act_copy.start()
    feed_again.copy(0).start()

    def hooks(s):
        if s >= 2 and s % 2 == 0:
            scat_h.step(s // 2 - 1)

    def put_h(slot):
        rows = scat_h.rows(slot)
        g_hidden = rows_of(hid_all, rows)
        scat_h.put(slot, dot(g_hidden, w1, NT))
        add_to(gw_1, dot(rows_of(fh, rows), g_hidden, TN))
        add_to(gw_2, dot(rows_of(act_all, rows), feed_again.take(slot, at.ring), TN))

    loop_slots(at.ring, hooks, put_h)
    scat_h.step(at.half - 1)
    for emit in emits:
        rows = emit.acc.shape[0]
        emit.start(rows, rows)

    def take_h(part, value):
        g_h2[part] = value

    scat_h.final(take_h)

    def back_one(b, carry):
        _, scale, gate = at_sample(mod, b)
        g_out, grad = g[b].astype(F32), g_h2[b]
        normed, inv_std = normalize(x2[b])
        back = g_out + normalize_back(normed, inv_std, grad * (1.0 + scale))
        g_x2[b] = back
        g_cross[b] = back.astype(BF16)
        terms = grad, grad * normed, back.astype(BF16).astype(F32), (g_out * gate).astype(BF16).astype(F32)
        return tuple(c + row_sum(t) for c, t in zip(carry, terms))

    zero = jnp.zeros((1, x2.shape[-1]), F32)
    found = lax.fori_loop(0, batch, back_one, (zero,) * 4)
    for row, value in zip((SHIFT2, SCALE2, B_CO, B_2), found):
        sums[row:row + 1, :] = value
    gather_h.finish()
    scat_h.finish()
    for copy in (act_copy, *[emit.copy for emit in emits]):
        copy.wait()


def mlp_call(tp_size, cid, *ins):
    batch, n_loc, width = ins[0].shape
    ffn = ins[-2].shape[0]
    n_tok = n_loc * tp_size
    ring, half = tp_size // 2, tp_size // 4
    local, tokens, hidden = (batch, n_loc, width), (batch, n_tok, width), (batch, n_tok, ffn)
    chip = batch, 2 * n_loc, width
    outs = [(local, F32), (local, BF16), ((SUM_ROWS, width), F32), ((1, ffn), F32)]
    late = [(hidden, BF16), ((width, ffn), BF16), ((ffn, width), BF16)]
    scratch = [(local, BF16), ((3, batch, width), F32), (tokens, BF16), (hidden, BF16), (local, F32), ((2, *chip), BF16),
               (hidden, BF16), ((width, ffn), F32), ((ffn, width), F32), *late[1:],
               ((ring, *chip), BF16), ((ring, *local), BF16), ((2, half, *local), BF16)]
    return pl.pallas_call(
        functools.partial(mlp_body, tp_size),
        out_shape=[jax.ShapeDtypeStruct(*o) for o in outs + late],
        in_specs=[VMEM] * (len(ins) - 1) + [ANY],
        out_specs=[VMEM] * len(outs) + [ANY] * len(late),
        scratch_shapes=[pltpu.VMEM(*k) for k in scratch] + gather_sems(tp_size) + scatter_sems(tp_size)
        + [pltpu.SemaphoreType.DMA] * len(late) + [pltpu.SemaphoreType.DMA((2,))],
        compiler_params=KERNEL(collective_id=cid),
        name='mlp_both_ways',
    )(*ins)


def finish_body(head_dim, head_pad, n_big, *refs):
    take = cutter(refs)
    sources, biases, (b_1, sums) = take(n_big), take(3), take(2)
    results, bias_outs, vectors = take(n_big), take(3), take(4)
    table, stages, (sem_in, sem_out) = take(1)[0], take(n_big), take(2)
    copies_in = [pltpu.make_async_copy(*ends, sem_in.at[i]) for i, ends in enumerate(zip(sources, stages))]
    copies_out = [pltpu.make_async_copy(*ends, sem_out.at[i]) for i, ends in enumerate(zip(stages, results))]
    for copy in copies_in:
        copy.start()
    for source, result in zip(biases, bias_outs):
        parts = [source[:, p:p + head_dim] for p in range(0, source.shape[1], head_pad)]
        result[...] = jnp.concatenate(parts, axis=1).astype(BF16)
    rows = [b_1[...]] + [sums[row:row + 1, :] for row in (B_O, B_CO, B_2)]
    for row, result in zip(rows, vectors):
        result[...] = row.astype(BF16).reshape(result.shape)
    table[...] = sums[:B_O, :]
    for arrived, leave in zip(copies_in, copies_out):
        arrived.wait()
        leave.start()
    for copy in copies_out:
        copy.wait()


def finish_call(head_dim, head_pad, big, biases, b_1, sums):
    width = sums.shape[1]
    shapes = [a.shape for a in big] + [(1, b.shape[1] // head_pad * head_dim) for b in biases] + [(b_1.shape[1],)] + [(width,)] * 3
    return pl.pallas_call(
        functools.partial(finish_body, head_dim, head_pad, len(big)),
        out_shape=[jax.ShapeDtypeStruct(shape, BF16) for shape in shapes] + [jax.ShapeDtypeStruct((B_O, width), F32)],
        in_specs=[ANY] * len(big) + [VMEM] * (len(biases) + 2),
        out_specs=[ANY] * len(big) + [VMEM] * (len(biases) + 5),
        scratch_shapes=[pltpu.VMEM(a.shape, BF16) for a in big] + [pltpu.SemaphoreType.DMA((len(big),))] * 2,
        compiler_params=pltpu.CompilerParams(vmem_limit_bytes=60 * 1000 * 1000),
        name='results',
    )(*big, *biases, b_1, sums)


def device_block(tp_size, x_loc, y_loc, t_loc, len_loc, mod_table, w_qkv, b_qkv, w_o, b_o, w_q, b_q, w_kv, b_kv, w_co, b_co, w_1, b_1, w_2, b_2, g_loc):
    head_dim = w_q.shape[2]
    head_pad = -(-head_dim // LANES) * LANES
    wqkv, wq, wkv = [w.transpose(1, 2, 0)[0] for w in (w_qkv, w_q, w_kv)]
    wo, wco = w_o[0], w_co[0]

    h1_all, y_all, x1_all, g_all, qkv, kv, q_cross, attn_val, cross_val, attn_prob, cross_prob, attn_total, x2_loc = forward_call(
        tp_size, 0, head_dim, head_pad, x_loc, y_loc, g_loc, t_loc, mod_table, len_loc,
        b_qkv, b_kv, b_q, b_o, b_co, wqkv, wkv, wq, wo, wco)
    g_x2, g_cross, sums, g_b_1, gelu_out, g_w_1, g_w_2 = mlp_call(
        tp_size, 1, x2_loc, g_loc, t_loc, mod_table, b_1, w_1, w_2, g_all)
    x_out, g_x, g_y, sums, *rest = backward_call(
        tp_size, 2, head_dim, head_pad, [g_cross, t_loc, mod_table, b_2, sums],
        [wqkv, wkv, wq, wo, wco, w_2, gelu_out, cross_val, q_cross, kv, cross_prob, g_x2, x_loc, x2_loc, g_loc, attn_total,
         attn_val, qkv, attn_prob], [h1_all, x1_all, y_all])
    bias_grads, weight_grads = rest[:3], rest[3:]

    results = finish_call(head_dim, head_pad, [x_out, g_x, g_y, g_w_1, g_w_2, *weight_grads], bias_grads, g_b_1, sums)
    x_out, g_x, g_y, g_w_1, g_w_2, *results = results
    g_w_qkv, g_w_kv, g_w_q, g_w_o, g_w_co, g_b_qkv, g_b_kv, g_b_q, g_b_1, g_b_o, g_b_co, g_b_2, g_table = results
    g_w_qkv, g_w_kv, g_w_q = [grad[None].transpose(2, 0, 1) for grad in (g_w_qkv, g_w_kv, g_w_q)]
    return (x_out, g_x, g_y, g_table, g_w_qkv, g_b_qkv, g_w_o[None], g_b_o, g_w_q, g_b_q, g_w_kv, g_b_kv,
            g_w_co[None], g_b_co, g_w_1, g_b_1, g_w_2, g_b_2)


def solution(mesh):
    token, heads, rows, whole = P('dp', 'tp'), P(None, 'tp'), P('tp'), P()
    group, group_rows, group_heads = P('dp'), P(('dp', 'tp')), P('dp', 'tp')
    in_specs = (token, token, group, group, whole, heads, rows, rows, whole, heads, rows, heads, rows, rows, whole, heads, rows, rows, whole, token)
    out_specs = (token, token, token, group, group_heads, group_rows, group_rows, group, group_heads, group_rows, group_heads, group_rows,
                 group_rows, group, group_heads, group_rows, group_rows, group)
    return jax.shard_map(functools.partial(device_block, mesh.shape['tp']), mesh=mesh, in_specs=in_specs, out_specs=out_specs, check_vma=False)
```

```python
import functools
import itertools

import jax
import jax.numpy as jnp
from jax import lax
from jax.experimental import pallas as pl
from jax.experimental.pallas import tpu as pltpu
from jax.sharding import PartitionSpec as P

LN_EPS = 1e-6
MASK_FILL = -1e30
LANES = 128
MESH = pl.DeviceIdType.MESH
BF16 = jnp.bfloat16
F32 = jnp.float32
NN = (((1,), (0,)), ((), ()))
NT = (((1,), (1,)), ((), ()))
TN = (((0,), (0,)), ((), ()))
SHIFT1, SCALE1, GATE1, SHIFT2, SCALE2, GATE2, B_O, B_CO, B_2 = range(9)
SUM_ROWS = 16
LOADED = 19
UP, DOWN = HALVES = WAYS = 0, 1
SEND, TAKE = True, False
KERNEL = functools.partial(pltpu.CompilerParams, has_side_effects=True, vmem_limit_bytes=67 * 1000 * 1000)
VMEM, ANY = pl.BlockSpec(memory_space=pltpu.VMEM), pl.BlockSpec(memory_space=pl.ANY)


def dot(lhs, rhs, dims=NN):
    return lax.dot_general(lhs, rhs[...], dims, preferred_element_type=F32)


def add_to(acc, value):
    acc[...] += value


def clear(refs):
    for ref in refs:
        ref[...] = jnp.zeros_like(ref)


def each(n, body):
    def step(i, carry):
        body(i)
        return carry
    lax.fori_loop(0, n, step, None)


def cutter(refs):
    left = iter(refs)
    return lambda n: list(itertools.islice(left, n))


def padded_bias(ref, head_dim, head_pad):
    gap = jnp.zeros((1, head_pad - head_dim), F32)
    parts = [ref[:, p:p + head_dim].astype(F32) for p in range(0, ref.shape[1], head_dim)]
    return jnp.concatenate([piece for part in parts for piece in (part, gap)], axis=1)


def row_of(ref):
    return ref[...].astype(F32).reshape(1, -1)


class Place:
    def __init__(self, tp_size):
        self.tp_size = tp_size
        self.me = lax.axis_index('tp')
        self.ring, self.chip, self.core = tp_size // 2, self.me // 2, lax.rem(self.me, 2)
        self.half = self.ring // 2

    def wrap(self, zz):
        return lax.rem(zz + self.ring, self.ring)

    def sibling(self):
        return {'tp': self.chip * 2 + 1 - self.core}

    def ahead(self, sign):
        return {'tp': self.wrap(self.chip + sign) * 2 + self.core}

    def other(self, d):
        return {'tp': lax.rem(self.me + d, self.tp_size)}

    def greet(self, peers):
        barrier = pltpu.get_barrier_semaphore()
        for peer in peers:
            pl.semaphore_signal(barrier, device_id=peer, device_id_type=MESH)
        pl.semaphore_wait(barrier, len(peers))

    def greet_all(self):
        self.greet([self.other(d) for d in range(1, self.tp_size)])

    def greet_near(self):
        self.greet([self.ahead(1), self.ahead(-1), self.sibling()])


class Gather:
    def __init__(self, at, own, full, sems):
        self.at, self.own_ref, self.full = at, own, full
        self.rsend, self.rrecv, self.ssend, self.srecv = sems
        self.batch, self.n_loc = own.shape[0], own.shape[1]
        self.hb = self.batch // 2

    def part(self, zz, cc, ch):
        row = pl.multiple_of((zz * 2 + cc) * self.n_loc, self.n_loc)
        return self.full.at[pl.ds(ch * self.hb, self.hb), pl.ds(row, self.n_loc), :]

    def own(self, ch):
        return self.own_ref.at[pl.ds(ch * self.hb, self.hb)]

    def ring_copy(self, way, k, ch, sending):
        at = self.at
        sign = -1 if way == UP else 1
        zb = at.wrap(at.chip + sign * (k - 1 if sending else k))
        src = self.own(ch) if (sending and k == 1) else self.part(zb, at.core, ch)
        return pltpu.make_async_remote_copy(
            src_ref=src, dst_ref=self.part(zb, at.core, ch),
            send_sem=self.rsend.at[way, k - 1, ch], recv_sem=self.rrecv.at[way, k - 1, ch],
            device_id=at.ahead(-sign), device_id_type=MESH)

    def chip_at(self, slot):
        k = (slot + 1) // 2
        return self.at.wrap(self.at.chip - k) if slot % 2 else self.at.wrap(self.at.chip + k)

    def sib_copy(self, slot, ch, sending):
        at = self.at
        cc = at.core if sending else 1 - at.core
        zb = self.chip_at(slot)
        src = self.own(ch) if (sending and slot == 0) else self.part(zb, cc, ch)
        return pltpu.make_async_remote_copy(
            src_ref=src, dst_ref=self.part(zb, cc, ch),
            send_sem=self.ssend.at[slot, ch], recv_sem=self.srecv.at[slot, ch],
            device_id=at.sibling(), device_id_type=MESH)

    def carries(self, way, k, ch):
        return k < self.at.half or (k == self.at.half and ch == way)

    def slot_of(self, way, k):
        half = self.at.half
        return 2 * half - 1 if k == half else (2 * k - 1 if way == UP else 2 * k)

    def start(self):
        for way, ch in ((UP, 0), (DOWN, 1), (UP, 1), (DOWN, 0)):
            self.ring_copy(way, 1, ch, SEND).start()
        for ch in HALVES:
            self.sib_copy(0, ch, SEND).start()
        row = pl.multiple_of(self.at.me * self.n_loc, self.n_loc)
        self.full[:, pl.ds(row, self.n_loc), :] = self.own_ref[...]

    def arrive(self, way, k, ch):
        self.ring_copy(way, k, ch, TAKE).wait_recv()
        if self.carries(way, k + 1, ch):
            self.ring_copy(way, k + 1, ch, SEND).start()
        self.sib_copy(self.slot_of(way, k), ch, SEND).start()

    def group(self, g):
        k = g // 2 + 1
        first, second = ((UP, 0), (DOWN, 1)) if g % 2 == 0 else ((UP, 1), (DOWN, 0))
        self.arrive(first[0], k, first[1])
        self.arrive(second[0], k, second[1])

    def groups_before(self, slot):
        last = self.at.ring - 1
        return () if slot == last - 1 else ((last - 1,) if slot == last else (slot,))

    def ready(self, slot):
        for ch in HALVES:
            self.sib_copy(slot, ch, TAKE).wait_recv()

    def rows(self, slot):
        k = (slot + 1) // 2
        zz = self.at.wrap(self.at.chip + (1 - 2 * lax.rem(slot, 2)) * k)
        return pl.ds(pl.multiple_of(zz * 2 * self.n_loc, 2 * self.n_loc), 2 * self.n_loc)

    def save_copy(self, dest, sem, slot):
        rows = self.rows(slot)
        return pltpu.make_async_copy(self.full.at[:, rows, :], dest.at[:, rows, :], sem.at[slot])

    def finish(self):
        for way in WAYS:
            for k in range(1, self.at.half + 1):
                for ch in HALVES:
                    if self.carries(way, k, ch):
                        self.ring_copy(way, k, ch, SEND).wait_send()
        for slot in range(self.at.ring):
            for ch in HALVES:
                self.sib_copy(slot, ch, SEND).wait_send()


class Scatter:
    def __init__(self, at, pbuf, sibr, rcv, sems):
        self.at, self.pbuf, self.sibr, self.rcv = at, pbuf, sibr, rcv
        self.rsend, self.rrecv, self.ssend, self.srecv = sems
        self.batch, self.n_loc = sibr.shape[1], sibr.shape[2]
        self.hb = self.batch // 2

    def slot_of(self, way, s):
        return 0 if s == 0 else (2 * s - 1 if way == UP else 2 * s)

    def rows(self, slot):
        at = self.at
        away = at.half - (slot + 1) // 2
        zz = at.wrap(at.chip + (2 * lax.rem(slot, 2) - 1) * away)
        return pl.ds(pl.multiple_of(zz * 2 * self.n_loc, 2 * self.n_loc), 2 * self.n_loc)

    def put(self, slot, value):
        self.pbuf[slot] = value.astype(BF16).reshape(self.batch, 2 * self.n_loc, value.shape[-1])
        self.sib_copy(slot).start()

    def ring_copy(self, way, s, ch):
        part = pl.ds(ch * self.hb, self.hb)
        return pltpu.make_async_remote_copy(
            src_ref=self.sibr.at[self.slot_of(way, s), part], dst_ref=self.rcv.at[way, s, part],
            send_sem=self.rsend.at[way, s, ch], recv_sem=self.rrecv.at[way, s, ch],
            device_id=self.at.ahead(1 if way == UP else -1), device_id_type=MESH)

    def sib_copy(self, slot):
        rows = pl.ds(pl.multiple_of((1 - self.at.core) * self.n_loc, self.n_loc), self.n_loc)
        return pltpu.make_async_remote_copy(
            src_ref=self.pbuf.at[slot, :, rows, :], dst_ref=self.sibr.at[slot],
            send_sem=self.ssend.at[slot], recv_sem=self.srecv.at[slot],
            device_id=self.at.sibling(), device_id_type=MESH)

    def own_sum(self, slot, part):
        rows = pl.ds(pl.multiple_of(self.at.core * self.n_loc, self.n_loc), self.n_loc)
        return self.pbuf[slot, part, rows, :].astype(F32) + self.sibr[slot, part].astype(F32)

    def starts_at(self, way, ch):
        return 0 if ch == way else 1

    def pass_on(self, way, s, ch):
        slot, part = self.slot_of(way, s), pl.ds(ch * self.hb, self.hb)
        total = self.own_sum(slot, part)
        if s > self.starts_at(way, ch):
            self.ring_copy(way, s - 1, ch).wait_recv()
            total = total + self.rcv[way, s - 1, part].astype(F32)
        self.sibr[slot, part] = total.astype(BF16)
        self.ring_copy(way, s, ch).start()

    def step(self, s):
        if s == 0:
            self.sib_copy(0).wait_recv()
            self.pass_on(UP, 0, 0)
            self.pass_on(DOWN, 0, 1)
            return
        self.sib_copy(2 * s - 1).wait_recv()
        self.pass_on(UP, s, 1)
        self.sib_copy(2 * s).wait_recv()
        self.pass_on(DOWN, s, 0)
        self.pass_on(UP, s, 0)
        self.pass_on(DOWN, s, 1)

    def final(self, use):
        last = self.at.ring - 1
        self.sib_copy(last).wait_recv()
        for ch, order in ((1, (UP, DOWN)), (0, (DOWN, UP))):
            part = pl.ds(ch * self.hb, self.hb)
            total = self.own_sum(last, part)
            for way in order:
                self.ring_copy(way, self.at.half - 1, ch).wait_recv()
                total = total + self.rcv[way, self.at.half - 1, part].astype(F32)
            use(part, total)

    def finish(self):
        for way in WAYS:
            for s in range(self.at.half):
                for ch in HALVES:
                    if s >= self.starts_at(way, ch):
                        self.ring_copy(way, s, ch).wait_send()
        for slot in range(self.at.ring):
            self.sib_copy(slot).wait_send()


def loop_slots(n, hooks, body):
    def step(slot):
        for s in range(n):
            @pl.when(slot == s)
            def _():
                hooks(s)
        body(slot)
    each(n, step)


def gather_sems(tp_size):
    ring, half = tp_size // 2, tp_size // 4
    return [pltpu.SemaphoreType.DMA(s) for s in ((2, half, 2), (2, half, 2), (ring, 2), (ring, 2))]


def scatter_sems(tp_size):
    ring, half = tp_size // 2, tp_size // 4
    return [pltpu.SemaphoreType.DMA(s) for s in ((2, half, 2), (2, half, 2), (ring,), (ring,))]


def pad_rows(dest, source, head_dim):
    parts = source.shape[0] // head_dim
    head_pad = dest.shape[0] // parts
    width = dest.shape[1]
    for i in range(parts):
        dest[i * head_pad:i * head_pad + head_dim, :] = source[i * head_dim:(i + 1) * head_dim, :]
        dest[i * head_pad + head_dim:(i + 1) * head_pad, :] = jnp.zeros((head_pad - head_dim, width), dest.dtype)


def at_sample(mod, b):
    return [mod[i, pl.ds(b, 1), :] for i in range(mod.shape[0])]


def fill_mod(mod, t_ref, table_ref, rows):
    for i, row in enumerate(rows):
        mod[i] = mod_row(t_ref, table_ref, row)


def mod_row(t_ref, table_ref, i):
    width = table_ref.shape[1]
    return table_ref[i:i + 1, :].astype(F32) + t_ref[:, i * width:(i + 1) * width].astype(F32)


def rows_of(ref, rows):
    block = ref[:, rows, :]
    return block.reshape(block.shape[0] * block.shape[1], block.shape[2])


def put_rows(ref, rows, value):
    ref[:, rows, :] = value.astype(ref.dtype).reshape(ref.shape[0], rows.size, ref.shape[2])


def row_sum(value):
    return jnp.sum(value, axis=0, keepdims=True)


def gelu_pair(hidden):
    c0, c1 = 0.7978845608028654, 0.044715
    square = hidden * hidden
    tanh = jnp.tanh(c0 * hidden * (1.0 + c1 * square))
    half_up = 0.5 * (1.0 + tanh)
    slope = half_up + 0.5 * hidden * (1.0 - tanh * tanh) * (c0 * (1.0 + 3.0 * c1 * square))
    return hidden * half_up, slope


def normalize(rows):
    rows = rows.astype(F32)
    centered = rows - jnp.mean(rows, axis=-1, keepdims=True)
    inv_std = lax.rsqrt(jnp.mean(centered * centered, axis=-1, keepdims=True) + LN_EPS)
    return centered * inv_std, inv_std


def normalize_back(normed, inv_std, g_normed):
    mean_g = jnp.mean(g_normed, axis=-1, keepdims=True)
    mean_gn = jnp.mean(g_normed * normed, axis=-1, keepdims=True)
    return inv_std * (g_normed - mean_g - normed * mean_gn)


def softmax_of(scores):
    top = jnp.max(scores, axis=-1, keepdims=True)
    powers = jnp.exp(scores - top)
    return powers * (1.0 / jnp.sum(powers, axis=-1, keepdims=True))


def forward_body(tp_size, head_dim, *refs):
    at = Place(tp_size)
    take = cutter(refs)
    x, y, g, t_emb, table, lens, *bias_in = take(11)
    sources = take(5)
    h1_out, y_out, x1_out, g_out = take(4)
    outs, scratch = take(9), take(9)
    qkv, kv, q_c, val, cval, prob, cprob, atot, x2 = scratch
    h1, x1, gm, mod, fh, fy, fx, fg, pbuf, sibr1, rcv1, sibr2, rcv2, wqkv, wkv, wq, wo, wco = take(18)
    raws = take(5)
    gather_h, gather_y, gather_x, gather_g = [Gather(at, own, full, take(4)) for own, full in ((h1, fh), (y, fy), (x1, fx), (gm, fg))]
    scat_o, scat_c = [Scatter(at, pbuf, sibr, rcv, take(4)) for sibr, rcv in ((sibr1, rcv1), (sibr2, rcv2))]
    *saves, raw_sem = take(5)
    out_sem = refs[-1]
    raw_copies = [pltpu.make_async_copy(*ends, raw_sem.at[i]) for i, ends in enumerate(zip(sources, raws))]
    for copy in raw_copies:
        copy.start()
    batch = x.shape[0]
    head_pad = wq.shape[0]
    bqkv, bkv, bq = [padded_bias(ref, head_dim, head_pad) for ref in bias_in[:3]]
    bo, bco = [row_of(ref) for ref in bias_in[3:]]
    scale = head_dim ** -0.5

    def out_copy(i):
        return pltpu.make_async_copy(scratch[i], outs[i], out_sem.at[i])

    at.greet_near()
    gather_y.start()
    fill_mod(mod, t_emb, table, (SHIFT1, SCALE1, GATE1, GATE2))

    def norm_one(b):
        shift, scale, _, gate = at_sample(mod, b)
        normed, _ = normalize(x[b])
        h1[b] = (normed * (1.0 + scale) + shift).astype(BF16)
        gm[b] = (g[b].astype(F32) * gate).astype(BF16)

    each(batch, norm_one)
    gather_h.start()
    for copy, dest, source in zip(raw_copies, (wqkv, wkv, wq, wo, wco), raws):
        copy.wait()
        pad_rows(dest, source, head_dim)

    def hooks(s):
        for g in gather_h.groups_before(s):
            gather_h.group(g)
        gather_h.ready(s)
        if s in (3, 5):
            gather_y.group(s // 2 - 1)

    def project(slot):
        rows = gather_h.rows(slot)
        gather_h.save_copy(h1_out, saves[0], slot).start()
        put_rows(qkv, rows, dot(rows_of(fh, rows), wqkv, NT) + bqkv)

    loop_slots(at.ring, hooks, project)

    def hooks(b):
        if b == batch // 2:
            gather_y.group(2)
        if b == batch - 1:
            gather_y.group(3)

    def attend_self(b):
        q_b, k_b, v_b = [qkv[b, :, i * head_pad:(i + 1) * head_pad] for i in range(3)]
        p_b = softmax_of(dot(q_b, k_b, NT) * scale).astype(BF16)
        prob[b] = p_b
        val[b] = dot(p_b, v_b).astype(BF16)

    loop_slots(batch, hooks, attend_self)
    for i in (0, 3, 5):
        out_copy(i).start()

    def hooks(s):
        if s % 2:
            scat_o.step(s // 2)
        elif s:
            gather_y.group(s // 2 + 3)
        if s == at.ring - 1:
            gather_g.start()

    def project_o(slot):
        scat_o.put(slot, dot(rows_of(val, scat_o.rows(slot)), wo))

    loop_slots(at.ring, hooks, project_o)

    def take_o(part, total):
        atot[part] = total + bo

    scat_o.final(take_o)
    out_copy(7).start()

    def x1_one(b):
        _, _, gate, _ = at_sample(mod, b)
        x1[b] = (x[b].astype(F32) + gate * atot[b]).astype(BF16)

    each(batch, x1_one)

    gather_x.start()

    def hooks(s):
        for g in gather_x.groups_before(s):
            gather_x.group(g)
        gather_y.ready(s)
        gather_x.ready(s)
        if s >= 2 and s % 2 == 0:
            gather_g.group(s // 2 - 1)

    def project(slot):
        rows = gather_x.rows(slot)
        gather_y.save_copy(y_out, saves[1], slot).start()
        gather_x.save_copy(x1_out, saves[2], slot).start()
        put_rows(kv, rows, dot(rows_of(fy, rows), wkv, NT) + bkv)
        put_rows(q_c, rows, dot(rows_of(fx, rows), wq, NT) + bq)

    loop_slots(at.ring, hooks, project)
    scat_o.finish()

    def hooks(b):
        if b == batch // 2:
            gather_g.group(3)
        if b == batch - 1:
            gather_g.group(4)

    def attend_cross(b):
        k_b, v_b = [kv[b, :, i * head_pad:(i + 1) * head_pad] for i in range(2)]
        scores = dot(q_c[b], k_b, NT) * scale
        slots = lax.broadcasted_iota(jnp.int32, scores.shape, 1)
        p_b = softmax_of(jnp.where(slots < lens[b], scores, MASK_FILL)).astype(BF16)
        cprob[b] = p_b
        cval[b] = dot(p_b, v_b).astype(BF16)

    loop_slots(batch, hooks, attend_cross)
    for i in (1, 2, 4, 6):
        out_copy(i).start()

    def save_g(slots):
        for slot in slots:
            gather_g.ready(slot)
            gather_g.save_copy(g_out, saves[3], slot).start()

    def hooks(s):
        if s % 2:
            scat_c.step(s // 2)
        if s == 3:
            gather_g.group(5)
            save_g(range(3))
        if s == 5:
            gather_g.group(6)
            save_g((3, 4))

    def project_c(slot):
        scat_c.put(slot, dot(rows_of(cval, scat_c.rows(slot)), wco))

    loop_slots(at.ring, hooks, project_c)
    save_g(range(5, at.ring))

    def take_c(part, total):
        x2[part] = (x1[part].astype(F32) + total + bco).astype(BF16)

    scat_c.final(take_c)
    out_copy(8).start()
    for stream in (gather_h, gather_y, gather_x, gather_g, scat_c):
        stream.finish()
    for slot in range(at.ring):
        gather_h.save_copy(h1_out, saves[0], slot).wait()
        gather_y.save_copy(y_out, saves[1], slot).wait()
        gather_x.save_copy(x1_out, saves[2], slot).wait()
        gather_g.save_copy(g_out, saves[3], slot).wait()
    for i in range(9):
        out_copy(i).wait()


def forward_call(tp_size, cid, head_dim, head_pad, *ins):
    batch, n_loc, width = ins[0].shape
    n_tok = n_loc * tp_size
    ring, half = tp_size // 2, tp_size // 4
    tokens = lambda last: (batch, n_tok, last)
    local = (batch, n_loc, width)
    kept = [(tokens(3 * head_pad), BF16), (tokens(2 * head_pad), BF16), (tokens(head_pad), BF16), (tokens(head_pad), BF16),
            (tokens(head_pad), BF16), (tokens(n_tok), BF16), (tokens(n_tok), BF16), (local, F32), (local, BF16)]
    sib, rcv = (ring, *local), (2, half, *local)
    return pl.pallas_call(
        functools.partial(forward_body, tp_size, head_dim),
        out_shape=[jax.ShapeDtypeStruct(tokens(width), BF16)] * 4 + [jax.ShapeDtypeStruct(*k) for k in kept],
        in_specs=[VMEM] * 5 + [pl.BlockSpec(memory_space=pltpu.SMEM)] + [VMEM] * (len(ins) - 11) + [ANY] * 5,
        out_specs=[ANY] * (4 + len(kept)),
        scratch_shapes=[pltpu.VMEM(*k) for k in kept] + [
            *[pltpu.VMEM(local, BF16)] * 3, pltpu.VMEM((4, batch, width), F32), *[pltpu.VMEM(tokens(width), BF16)] * 4,
            pltpu.VMEM((ring, batch, 2 * n_loc, width), BF16),
            pltpu.VMEM(sib, BF16), pltpu.VMEM(rcv, BF16), pltpu.VMEM(sib, BF16), pltpu.VMEM(rcv, BF16)]
        + [pltpu.VMEM((n * head_pad, width), BF16) for n in (3, 2, 1, 1, 1)] + [pltpu.VMEM(w.shape, BF16) for w in ins[-5:]]
        + gather_sems(tp_size) * 4 + scatter_sems(tp_size) * 2
        + [pltpu.SemaphoreType.DMA((ring,))] * 4 + [pltpu.SemaphoreType.DMA((5,))] + [pltpu.SemaphoreType.DMA((len(kept),))],
        compiler_params=KERNEL(collective_id=cid),
        name='attention_forward',
    )(*ins)


class Emit:
    def __init__(self, acc, stage, dest, sem):
        self.acc, self.stage = acc, stage
        self.copy = pltpu.make_async_copy(stage, dest, sem)

    def start(self, head_dim, head_pad):
        for p in range(self.stage.shape[0] // head_dim):
            self.stage[p * head_dim:(p + 1) * head_dim, :] = self.acc[p * head_pad:p * head_pad + head_dim, :].astype(BF16)
        self.copy.start()


class RowFeed:
    def __init__(self, source, buf, sem, rows):
        self.source, self.buf, self.sem, self.rows = source, buf, sem, rows

    def copy(self, slot):
        side = lax.rem(slot, 2)
        return pltpu.make_async_copy(self.source.at[:, self.rows(slot), :], self.buf.at[side], self.sem.at[side])

    def take(self, slot, n):
        @pl.when(slot + 1 < n)
        def _():
            self.copy(slot + 1).start()
        self.copy(slot).wait()
        block = self.buf[lax.rem(slot, 2)]
        return block.reshape(block.shape[0] * block.shape[1], block.shape[2])


def small_total(at, src, got, mine, out, sems, between):
    send1, recv1, send2, recv2 = sems
    tiles = src.shape[1] // LANES

    def lanes(i):
        return pl.ds(i * LANES, LANES)

    def first(tile, peer_slot):
        return pltpu.make_async_remote_copy(
            src_ref=src.at[:, lanes(tile)], dst_ref=got.at[peer_slot], send_sem=send1.at[tile], recv_sem=recv1.at[peer_slot],
            device_id={'tp': tile}, device_id_type=MESH)

    def second(tile, d):
        return pltpu.make_async_remote_copy(
            src_ref=mine, dst_ref=out.at[:, lanes(tile)], send_sem=send2.at[d - 1], recv_sem=recv2.at[tile],
            device_id=at.other(d), device_id_type=MESH)

    for tile in range(tiles):
        @pl.when(at.me != tile)
        def _():
            first(tile, lax.rem(at.me - tile + at.tp_size, at.tp_size) - 1).start()
    between()
    for tile in range(tiles):
        @pl.when(at.me == tile)
        def _():
            total = src[:, tile * LANES:(tile + 1) * LANES]
            for d in range(1, at.tp_size):
                first(tile, d - 1).wait_recv()
                total = total + got[d - 1]
            mine[...] = total
            for d in range(1, at.tp_size):
                second(tile, d).start()
            out[:, tile * LANES:(tile + 1) * LANES] = total
            for d in range(1, at.tp_size):
                second(tile, d).wait_send()
    for tile in range(tiles):
        @pl.when(at.me != tile)
        def _():
            second(tile, 1).wait_recv()
            first(tile, 0).wait_send()


def backward_body(tp_size, head_dim, *refs):
    at = Place(tp_size)
    take = cutter(refs)
    g_cross, t_emb, table, b2_in, sums_in = take(5)
    b2 = row_of(b2_in)
    loads, feeds = take(LOADED), take(3)
    x_out, g_x, g_y, sums_out, gb_qkv, gb_kv, gb_q = take(7)
    dests, held = take(5), take(LOADED)
    wqkv_in, wkv_in, wq_in, wo_in, wco_in, w2, act_all, cval, q_c, kv, cprob, g_x2, x, x2, g, atot, val, qkv, prob = held
    accs, stages = take(5), take(5)
    gw_qkv, gw_kv, gw_q, gw_o, gw_co = accs
    full, pbuf, sibr1, rcv1, pbufy, sibr2, rcv2, wqkv, wkv, wq, wo, wco = take(12)
    g_val, g_qkv, g_kv, g_q, g_x1, g_h1, g_attn, mod, sums, got, mine, feed_a, feed_y = take(13)
    gather_c, gather_a = [Gather(at, own, full, take(4)) for own in (g_cross, g_attn)]
    near, far = (pbuf, sibr1, rcv1), (pbufy, sibr2, rcv2)
    scat_m, scat_q, scat_y, scat_h = [Scatter(at, *bufs, take(4)) for bufs in (far, near, far, near)]
    load_sem, emit_sem, *feed_sems = take(5)
    emits = [Emit(*e, emit_sem.at[i]) for i, e in enumerate(zip(accs, stages, dests))]
    emit_qkv, emit_kv, emit_q, emit_o, emit_co = [functools.partial(e.start, head_dim, wq.shape[0]) for e in emits]
    feed_h, feed_x, feed_yy = [
        RowFeed(source, buf, sem, scat.rows)
        for source, buf, sem, scat in zip(feeds, (feed_a, feed_a, feed_y), feed_sems, (scat_h, scat_q, scat_y))]
    batch, _, width = x.shape
    ring, half = at.ring, at.half
    head_pad = wq.shape[0]
    scale = head_dim ** -0.5

    def load_copy(i):
        return pltpu.make_async_copy(loads[i], held[i], load_sem.at[i])

    for i in range(len(held)):
        load_copy(i).start()
    at.greet_all()
    gather_c.start()
    feed_x.copy(0).start()
    feed_yy.copy(0).start()
    fill_mod(mod, t_emb, table, (SHIFT1, SCALE1, GATE1, GATE2))
    sums[...] = sums_in[...]
    clear((*accs, gb_qkv, gb_kv, gb_q))
    for i in range(len(held)):
        load_copy(i).wait()
    for dest, source in zip((wqkv, wkv, wq, wo, wco), held):
        pad_rows(dest, source, head_dim)

    def put_m(slot):
        scat_m.put(slot, dot(rows_of(act_all, scat_m.rows(slot)), w2))

    def out_back(gather, value, weight, acc, beside):
        def body(slot):
            rows = gather.rows(slot)
            block = rows_of(full, rows)
            put_rows(g_val, rows, dot(block, weight, NT))
            add_to(acc, dot(rows_of(value, rows), block, TN))
            beside(slot)
        return body

    def hooks(s):
        for g in gather_c.groups_before(s):
            gather_c.group(g)
        if s >= 2 and s % 2 == 0:
            scat_m.step(s // 2 - 1)
        gather_c.ready(s)

    loop_slots(ring, hooks, out_back(gather_c, cval, wco, gw_co, put_m))
    gather_c.finish()
    emit_co()

    def back_one(q_b, k_b, v_b, p_b, g_b):
        g_p = dot(g_b, v_b, NT)
        p_f = p_b.astype(F32)
        row_dot = jnp.sum(g_p * p_f, axis=-1, keepdims=True)
        g_s = (p_f * (g_p - row_dot) * scale).astype(BF16)
        return dot(g_s, k_b).astype(BF16), dot(g_s, q_b, TN).astype(BF16), dot(p_b, g_b, TN).astype(BF16)

    def hooks(b):
        if b == batch // 2:
            scat_m.step(half - 1)

    def cross_back(b):
        parts = back_one(q_c[b], kv[b, :, :head_pad], kv[b, :, head_pad:], cprob[b], g_val[b])
        g_q[b] = parts[0]
        g_kv[b, :, :head_pad] = parts[1]
        g_kv[b, :, head_pad:] = parts[2]

    loop_slots(batch, hooks, cross_back)

    def hooks(s):
        if s % 2:
            scat_q.step(s // 2)
        if s == 3:
            scat_m.final(take_m)
            scat_m.finish()

    def take_m(part, total):
        g_h1[part] = total + b2

    def put_q(slot):
        block = rows_of(g_q, scat_q.rows(slot))
        scat_q.put(slot, dot(block, wq))
        add_to(gw_q, dot(block, feed_x.take(slot, ring), TN))
        add_to(gb_q, row_sum(block.astype(F32)))

    def put_y(slot):
        block = rows_of(g_kv, scat_y.rows(slot))
        scat_y.put(slot, dot(block, wkv))
        add_to(gw_kv, dot(block, feed_yy.take(slot, ring), TN))
        add_to(gb_kv, row_sum(block.astype(F32)))

    loop_slots(ring, hooks, put_q)
    emit_q()

    def out_one(b, gate_sum):
        gate, g_out, total = at_sample(mod, b)[-1], g[b].astype(F32), g_h1[b]
        x_out[b] = (x2[b].astype(F32) + gate * total).astype(BF16)
        return gate_sum + row_sum(g_out * total)

    zero = jnp.zeros((1, width), F32)
    sums[GATE2:GATE2 + 1, :] = lax.fori_loop(0, batch, out_one, zero)

    def take_q(part, total):
        g_x1[part] = g_x2[part] + total

    scat_q.final(take_q)
    feed_h.copy(0).start()

    def x1_back(b, carry):
        gate_sum, bias_sum = carry
        rows = g_x1[b]
        block = (rows * mod[2, pl.ds(b, 1), :]).astype(BF16)
        g_attn[b] = block
        return gate_sum + row_sum(rows * atot[b]), bias_sum + row_sum(block.astype(F32))

    gate_sum, bias_sum = lax.fori_loop(0, batch, x1_back, (zero, zero))
    for row, value in ((GATE1, gate_sum), (B_O, bias_sum)):
        sums[row:row + 1, :] = value

    scat_q.finish()
    gather_a.start()

    def hooks(s):
        for g in gather_a.groups_before(s):
            gather_a.group(g)
        if s >= 2 and s % 2 == 0:
            scat_y.step(s // 2 - 1)
        gather_a.ready(s)

    loop_slots(ring, hooks, out_back(gather_a, val, wo, gw_o, put_y))

    def hooks(b):
        if b == batch // 4:
            scat_y.step(half - 1)

    def self_back(b):
        parts = back_one(*[qkv[b, :, i * head_pad:(i + 1) * head_pad] for i in range(3)], prob[b], g_val[b])
        for i in range(3):
            g_qkv[b, :, i * head_pad:(i + 1) * head_pad] = parts[i]

    loop_slots(batch, hooks, self_back)
    emit_kv()
    emit_o()

    def take_y(part, total):
        g_y[part] = total.astype(BF16)

    def hooks(s):
        if s % 2:
            scat_h.step(s // 2)
        if s == 5:
            scat_y.final(take_y)

    def put_h(slot):
        block = rows_of(g_qkv, scat_h.rows(slot))
        scat_h.put(slot, dot(block, wqkv))
        add_to(gw_qkv, dot(block, feed_h.take(slot, ring), TN))
        add_to(gb_qkv, row_sum(block.astype(F32)))

    loop_slots(ring, hooks, put_h)
    emit_qkv()

    def take_h(part, total):
        g_h1[part] = total

    scat_h.final(take_h)

    def sums_one(b, carry):
        shift_sum, scale_sum = carry
        normed, _ = normalize(x[b])
        return shift_sum + row_sum(g_h1[b]), scale_sum + row_sum(g_h1[b] * normed)

    def x_one(b):
        normed, inv_std = normalize(x[b])
        _, scale, *_ = at_sample(mod, b)
        back = normalize_back(normed, inv_std, g_h1[b] * (1.0 + scale))
        g_x[b] = (g_x1[b] + back).astype(BF16)

    shift_sum, scale_sum = lax.fori_loop(0, batch, sums_one, (zero, zero))
    for row, value in ((SHIFT1, shift_sum), (SCALE1, scale_sum)):
        sums[row:row + 1, :] = value
    small_total(at, sums, got, mine, sums_out, take(4), lambda: each(batch, x_one))
    for stream in (gather_a, scat_y, scat_h):
        stream.finish()
    for emit in emits:
        emit.copy.wait()


def backward_call(tp_size, cid, head_dim, head_pad, ins, loads, feeds):
    batch, n_loc, width = ins[0].shape
    n_tok = n_loc * tp_size
    ring, half = tp_size // 2, tp_size // 4
    tokens = lambda last: (batch, n_tok, last)
    local = (batch, n_loc, width)
    sib, rcv, pbuf = (ring, *local), (2, half, *local), (ring, batch, 2 * n_loc, width)
    parts = 3, 2, 1, 1, 1
    outs = [(local, BF16)] * 3 + [((SUM_ROWS, width), F32)] + [((1, n * head_pad), F32) for n in parts[:3]]
    grads = [((n * head_dim, width), BF16) for n in parts]
    return pl.pallas_call(
        functools.partial(backward_body, tp_size, head_dim),
        out_shape=[jax.ShapeDtypeStruct(*o) for o in outs + grads],
        in_specs=[VMEM] * len(ins) + [ANY] * (len(loads) + len(feeds)),
        out_specs=[VMEM] * len(outs) + [ANY] * len(grads),
        scratch_shapes=[pltpu.VMEM(a.shape, a.dtype) for a in loads]
        + [pltpu.VMEM((n * head_pad, width), F32) for n in parts] + [pltpu.VMEM(*g) for g in grads]
        + [pltpu.VMEM(s, BF16) for s in (tokens(width), pbuf, sib, rcv, pbuf, sib, rcv)]
        + [pltpu.VMEM((n * head_pad, width), BF16) for n in parts]
        + [pltpu.VMEM(tokens(n * head_pad), BF16) for n in (1, 3, 2, 1)]
        + [pltpu.VMEM(local, F32), pltpu.VMEM(local, F32), pltpu.VMEM(local, BF16), pltpu.VMEM((4, batch, width), F32), pltpu.VMEM((SUM_ROWS, width), F32),
           pltpu.VMEM((tp_size - 1, SUM_ROWS, LANES), F32), pltpu.VMEM((SUM_ROWS, LANES), F32)]
        + [pltpu.VMEM((2, batch, 2 * n_loc, width), BF16)] * 2
        + gather_sems(tp_size) * 2 + scatter_sems(tp_size) * 4
        + [pltpu.SemaphoreType.DMA((len(loads),)), pltpu.SemaphoreType.DMA((len(grads),))] + [pltpu.SemaphoreType.DMA((2,))] * 3
        + [pltpu.SemaphoreType.DMA((n,)) for n in (width // LANES, tp_size - 1, tp_size - 1, width // LANES)],
        compiler_params=KERNEL(collective_id=cid),
        name='attention_backward',
    )(*ins, *loads, *feeds)


def mlp_body(tp_size, *refs):
    at = Place(tp_size)
    take = cutter(refs)
    x2, g, t_emb, table, b1_in, *sources, g_all = take(8)
    b1 = row_of(b1_in)
    g_x2, g_cross, sums, gb_1, act_out, *dests = take(7)
    h2, mod, fh, hid_all, g_h2, feed, w1, w2, act_all, gw_1, gw_2, *stages = take(13)
    bufs = take(3)
    gather_h, scat_h = Gather(at, h2, fh, take(4)), Scatter(at, *bufs, take(4))
    act_sem, *emit_sems = take(3)
    weight_copies = [pltpu.make_async_copy(*ends) for ends in zip(sources, (w1, w2), take(2))]
    for copy in weight_copies:
        copy.start()
    act_copy = pltpu.make_async_copy(act_all, act_out, act_sem)
    emits = [Emit(*e) for e in zip((gw_1, gw_2), stages, dests, emit_sems)]
    feed_g, feed_again = [RowFeed(g_all, feed, refs[-1], stream.rows) for stream in (gather_h, scat_h)]
    batch = x2.shape[0]

    feed_g.copy(0).start()
    at.greet_near()
    fill_mod(mod, t_emb, table, (SHIFT2, SCALE2, GATE2))

    def norm_one(b):
        shift, scale, _ = at_sample(mod, b)
        normed, _ = normalize(x2[b])
        h2[b] = (normed * (1.0 + scale) + shift).astype(BF16)

    each(batch, norm_one)
    gather_h.start()
    clear((gw_1, gw_2, gb_1, sums))
    for copy in weight_copies:
        copy.wait()

    def hooks(s):
        for group in gather_h.groups_before(s):
            gather_h.group(group)
        gather_h.ready(s)

    def mlp(slot):
        rows = gather_h.rows(slot)
        h2_blk, g_blk = rows_of(fh, rows), feed_g.take(slot, at.ring)
        act, slope = gelu_pair(dot(h2_blk, w1) + b1)
        act = act.astype(BF16)
        put_rows(act_all, rows, act)
        g_hidden = dot(g_blk, w2, NT) * slope
        add_to(gb_1, row_sum(g_hidden))
        g_hidden = g_hidden.astype(BF16)
        put_rows(hid_all, rows, g_hidden)

    loop_slots(at.ring, hooks, mlp)
    act_copy.start()
    feed_again.copy(0).start()

    def hooks(s):
        if s % 2:
            scat_h.step(s // 2)

    def put_h(slot):
        rows = scat_h.rows(slot)
        g_hidden = rows_of(hid_all, rows)
        scat_h.put(slot, dot(g_hidden, w1, NT))
        add_to(gw_1, dot(rows_of(fh, rows), g_hidden, TN))
        add_to(gw_2, dot(rows_of(act_all, rows), feed_again.take(slot, at.ring), TN))

    loop_slots(at.ring, hooks, put_h)
    for emit in emits:
        rows = emit.acc.shape[0]
        emit.start(rows, rows)

    def take_h(part, value):
        g_h2[part] = value

    scat_h.final(take_h)

    def back_one(b, carry):
        _, scale, gate = at_sample(mod, b)
        g_out, grad = g[b].astype(F32), g_h2[b]
        normed, inv_std = normalize(x2[b])
        back = g_out + normalize_back(normed, inv_std, grad * (1.0 + scale))
        g_x2[b] = back
        g_cross[b] = back.astype(BF16)
        terms = grad, grad * normed, back.astype(BF16).astype(F32), (g_out * gate).astype(BF16).astype(F32)
        return tuple(c + row_sum(t) for c, t in zip(carry, terms))

    zero = jnp.zeros((1, x2.shape[-1]), F32)
    found = lax.fori_loop(0, batch, back_one, (zero,) * 4)
    for row, value in zip((SHIFT2, SCALE2, B_CO, B_2), found):
        sums[row:row + 1, :] = value
    gather_h.finish()
    scat_h.finish()
    for copy in (act_copy, *[emit.copy for emit in emits]):
        copy.wait()


def mlp_call(tp_size, cid, *ins):
    batch, n_loc, width = ins[0].shape
    ffn = ins[-2].shape[0]
    n_tok = n_loc * tp_size
    ring, half = tp_size // 2, tp_size // 4
    local, tokens, hidden = (batch, n_loc, width), (batch, n_tok, width), (batch, n_tok, ffn)
    chip = batch, 2 * n_loc, width
    outs = [(local, F32), (local, BF16), ((SUM_ROWS, width), F32), ((1, ffn), F32)]
    late = [(hidden, BF16), ((width, ffn), BF16), ((ffn, width), BF16)]
    scratch = [(local, BF16), ((3, batch, width), F32), (tokens, BF16), (hidden, BF16), (local, F32), ((2, *chip), BF16), *late[1:],
               (hidden, BF16), ((width, ffn), F32), ((ffn, width), F32), *late[1:],
               ((ring, *chip), BF16), ((ring, *local), BF16), ((2, half, *local), BF16)]
    return pl.pallas_call(
        functools.partial(mlp_body, tp_size),
        out_shape=[jax.ShapeDtypeStruct(*o) for o in outs + late],
        in_specs=[VMEM] * (len(ins) - 3) + [ANY] * 3,
        out_specs=[VMEM] * len(outs) + [ANY] * len(late),
        scratch_shapes=[pltpu.VMEM(*k) for k in scratch] + gather_sems(tp_size) + scatter_sems(tp_size)
        + [pltpu.SemaphoreType.DMA] * 5 + [pltpu.SemaphoreType.DMA((2,))],
        compiler_params=KERNEL(collective_id=cid),
        name='mlp_both_ways',
    )(*ins)


def finish_body(head_dim, head_pad, n_big, *refs):
    take = cutter(refs)
    sources, biases, (b_1, sums) = take(n_big), take(3), take(2)
    results, bias_outs, vectors = take(n_big), take(3), take(4)
    table, stages, (sem_in, sem_out) = take(1)[0], take(n_big), take(2)
    copies_in = [pltpu.make_async_copy(*ends, sem_in.at[i]) for i, ends in enumerate(zip(sources, stages))]
    copies_out = [pltpu.make_async_copy(*ends, sem_out.at[i]) for i, ends in enumerate(zip(stages, results))]
    for copy in copies_in:
        copy.start()
    for source, result in zip(biases, bias_outs):
        parts = [source[:, p:p + head_dim] for p in range(0, source.shape[1], head_pad)]
        result[...] = jnp.concatenate(parts, axis=1).astype(BF16)
    rows = [b_1[...]] + [sums[row:row + 1, :] for row in (B_O, B_CO, B_2)]
    for row, result in zip(rows, vectors):
        result[...] = row.astype(BF16).reshape(result.shape)
    table[...] = sums[:B_O, :]
    for arrived, leave in zip(copies_in, copies_out):
        arrived.wait()
        leave.start()
    for copy in copies_out:
        copy.wait()


def finish_call(head_dim, head_pad, big, biases, b_1, sums):
    width = sums.shape[1]
    shapes = [a.shape for a in big] + [(1, b.shape[1] // head_pad * head_dim) for b in biases] + [(b_1.shape[1],)] + [(width,)] * 3
    return pl.pallas_call(
        functools.partial(finish_body, head_dim, head_pad, len(big)),
        out_shape=[jax.ShapeDtypeStruct(shape, BF16) for shape in shapes] + [jax.ShapeDtypeStruct((B_O, width), F32)],
        in_specs=[ANY] * len(big) + [VMEM] * (len(biases) + 2),
        out_specs=[ANY] * len(big) + [VMEM] * (len(biases) + 5),
        scratch_shapes=[pltpu.VMEM(a.shape, BF16) for a in big] + [pltpu.SemaphoreType.DMA((len(big),))] * 2,
        compiler_params=pltpu.CompilerParams(vmem_limit_bytes=60 * 1000 * 1000),
        name='results',
    )(*big, *biases, b_1, sums)


def device_block(tp_size, x_loc, y_loc, t_loc, len_loc, mod_table, w_qkv, b_qkv, w_o, b_o, w_q, b_q, w_kv, b_kv, w_co, b_co, w_1, b_1, w_2, b_2, g_loc):
    head_dim = w_q.shape[2]
    head_pad = -(-head_dim // LANES) * LANES
    wqkv, wq, wkv = [w.transpose(1, 2, 0)[0] for w in (w_qkv, w_q, w_kv)]
    wo, wco = w_o[0], w_co[0]

    h1_all, y_all, x1_all, g_all, qkv, kv, q_cross, attn_val, cross_val, attn_prob, cross_prob, attn_total, x2_loc = forward_call(
        tp_size, 0, head_dim, head_pad, x_loc, y_loc, g_loc, t_loc, mod_table, len_loc,
        b_qkv, b_kv, b_q, b_o, b_co, wqkv, wkv, wq, wo, wco)
    g_x2, g_cross, sums, g_b_1, gelu_out, g_w_1, g_w_2 = mlp_call(
        tp_size, 1, x2_loc, g_loc, t_loc, mod_table, b_1, w_1, w_2, g_all)
    x_out, g_x, g_y, sums, *rest = backward_call(
        tp_size, 2, head_dim, head_pad, [g_cross, t_loc, mod_table, b_2, sums],
        [wqkv, wkv, wq, wo, wco, w_2, gelu_out, cross_val, q_cross, kv, cross_prob, g_x2, x_loc, x2_loc, g_loc, attn_total,
         attn_val, qkv, attn_prob], [h1_all, x1_all, y_all])
    bias_grads, weight_grads = rest[:3], rest[3:]

    results = finish_call(head_dim, head_pad, [x_out, g_x, g_y, g_w_1, g_w_2, *weight_grads], bias_grads, g_b_1, sums)
    x_out, g_x, g_y, g_w_1, g_w_2, *results = results
    g_w_qkv, g_w_kv, g_w_q, g_w_o, g_w_co, g_b_qkv, g_b_kv, g_b_q, g_b_1, g_b_o, g_b_co, g_b_2, g_table = results
    g_w_qkv, g_w_kv, g_w_q = [grad[None].transpose(2, 0, 1) for grad in (g_w_qkv, g_w_kv, g_w_q)]
    return (x_out, g_x, g_y, g_table, g_w_qkv, g_b_qkv, g_w_o[None], g_b_o, g_w_q, g_b_q, g_w_kv, g_b_kv,
            g_w_co[None], g_b_co, g_w_1, g_b_1, g_w_2, g_b_2)


def solution(mesh):
    token, heads, rows, whole = P('dp', 'tp'), P(None, 'tp'), P('tp'), P()
    group, group_rows, group_heads = P('dp'), P(('dp', 'tp')), P('dp', 'tp')
    in_specs = (token, token, group, group, whole, heads, rows, rows, whole, heads, rows, heads, rows, rows, whole, heads, rows, rows, whole, token)
    out_specs = (token, token, token, group, group_heads, group_rows, group_rows, group, group_heads, group_rows, group_heads, group_rows,
                 group_rows, group, group_heads, group_rows, group_rows, group)
    return jax.shard_map(functools.partial(device_block, mesh.shape['tp']), mesh=mesh, in_specs=in_specs, out_specs=out_specs, check_vma=False)
```
